256 devices in a mesh: lat: 32 (over y, x, core), lev: 8 (over z).
Axes of the slice: x: 4, y: 4, z: 8, core: 2. Of those that a mesh axis runs over, the one named last changes fastest.
Arguments:
- fields: float32 [12, 128, 256, 1024], P(None, 'lev', 'lat'), may hold values from -6 to 6
- legendre: bfloat16 [256, 256, 256], P('lat'), as said below
- owner_counts: int32 [32], replicated, may hold values from 1 to 16, 256 in all
Outputs:
- covariance: float32 [512, 128, 128], P('lat', 'lev')
The draws below stay inside these ranges and needn't reach their ends.
Inputs may be any that keep to these rules, and one draw needn't show every extreme that they name: `owner_counts`: each owner holds 1 to 16 total wavenumbers, the counts sum to 256, and some owner holds exactly 16. legendre[lat, m, n] is zero where n < m.
All inputs are finite; a program needn't handle non-finite values.
Results may differ from the reference program's by a relative error of at most 0.0038.
Values may be sent and summed in bfloat16 or wider, within the bound.
No kernel may reach another device: no remote copies, remote signals or barrier semaphores. Data moves between devices by JAX's collectives and lax.ppermute only.
A program may use at most 128 MiB of HBM per device.

```python
import math
import jax
import jax.numpy as jnp
import numpy as np
from jax import lax

NLON = 1024
NLAT = 256
MTRUNC = 256
LEV = 128
MEM = 12
NCAP = 16
OWNERS = 32


def draw_legendre(key, part):
    values = jax.random.normal(key, (NLAT, MTRUNC, MTRUNC), jnp.float32) * NLAT ** (-0.5)
    order = jnp.arange(MTRUNC, dtype=jnp.int32)
    keeper = order[None, :] >= order[:, None]
    return jnp.where(keeper[None, :, :], values, jnp.zeros_like(values)).astype(jnp.bfloat16)


def levels(key, extent, shards, smallest, top_value):
    level = 1.0
    for position, parts in shards:
        draws = jax.random.uniform(jax.random.fold_in(jax.random.fold_in(key, 6), position), (parts,), jnp.float32, smallest / len(shards), top_value / len(shards))
        level = level * jnp.repeat(jnp.exp(draws), extent[position] // parts).reshape((-1,) + (1,) * (len(extent) - 1 - position))
    return level


def split_up(number_of, total, reach, slope):
    portions = [(1 << 20) // math.isqrt(rank ** slope) + 1 for rank in range(2, number_of + 1)]
    rest, given = total - reach - (number_of - 1), [1] * (number_of - 1)
    while rest > 0:
        candidates = [i for i in range(number_of - 1) if given[i] < reach]
        mass, remaining = sum([portions[i] for i in candidates]), rest
        for i in candidates:
            addition = min(reach - given[i], max(1, remaining * portions[i] // mass), rest)
            given[i] = given[i] + addition
            rest = rest - addition
    return np.array([reach] + given)


def ragged_sizes(key, number_of, total, most, skew):
    if number_of == 2:
        one = jax.random.randint(key, (), max(1, total - most), min(most, total - 1) + 1)
        return jnp.stack([one, total - one])
    lengths = jnp.asarray(split_up(number_of, total, most, skew), jnp.int32)
    couples = (number_of - 1) // 2
    giver, taker = lengths[1:1 + 2 * couples:2], lengths[2:2 + 2 * couples:2]
    room = jnp.minimum(giver - 1, most - taker)
    moved = jax.random.randint(jax.random.fold_in(key, 1), (couples,), 0, 1 << 20) % (room + 1)
    lengths = lengths.at[1:1 + 2 * couples:2].set(giver - moved).at[2:2 + 2 * couples:2].set(taker + moved)
    return lengths[jax.random.permutation(jax.random.fold_in(key, 2), number_of)]


def normal_values(key, shape, scale, most, split=(), kind=jnp.bfloat16):
    factor_of = levels(key, shape, split, -0.22, 0.18) if split else 1.0
    entries = jax.random.normal(key, shape, jnp.float32) * scale * factor_of
    return jnp.minimum(jnp.maximum(entries, -most), most).astype(kind)


def setup_inputs(seed: int = 0) -> dict:
    splits = jax.random.split(jax.random.key(seed), 4)
    return {
        "fields": normal_values(splits[0], (MEM, LEV, NLAT, NLON), 1.0, 6.0, ((1, 8), (2, 32)), jnp.float32),
        "legendre": draw_legendre(jax.random.fold_in(splits[3], 71), 0),
        "owner_counts": ragged_sizes(splits[2], OWNERS, MTRUNC, NCAP, 2).astype(jnp.int32),
    }


def reference(fields, legendre, owner_counts):
    transform = jnp.fft.rfft(fields, axis=-1)[..., :MTRUNC] * (NLON ** -0.5)
    stacked = jnp.stack([jnp.real(transform), jnp.imag(transform)], axis=0).astype(jnp.float32)
    spectra = jnp.transpose(stacked, (3, 4, 0, 1, 2)).astype(jnp.bfloat16)
    block_size = 32

    def add_block(running, block_id):
        spec_block = lax.dynamic_slice_in_dim(spectra, block_id * block_size, block_size, 1).astype(jnp.float32)
        transform_table_block = lax.dynamic_slice_in_dim(legendre, block_id * block_size, block_size, 1).astype(jnp.float32)
        wavenumber_rows = jnp.einsum('lmqbe,lmn->nmqbe', spec_block, transform_table_block)
        anomaly = (wavenumber_rows - jnp.mean(wavenumber_rows, axis=3, keepdims=True)).astype(jnp.bfloat16)
        anomaly = lax.optimization_barrier(anomaly).astype(jnp.float32)
        return running + jnp.einsum('nmqbe,nmqbk->nek', anomaly, anomaly), None

    blocks_all = jnp.arange(MTRUNC // block_size, dtype=jnp.int32)
    start_sum = jnp.zeros((MTRUNC, LEV, LEV), jnp.float32)
    full, unused = lax.scan(add_block, start_sum, blocks_all)
    wavenumber = jnp.arange(MTRUNC, dtype=jnp.int32)
    divisor = ((MEM - 1) * (2 * wavenumber + 2)).astype(jnp.float32)
    full = full / divisor[:, None, None]
    starts = (jnp.cumsum(owner_counts) - owner_counts).astype(jnp.int32)
    offset = jnp.arange(NCAP, dtype=jnp.int32)
    active_flag = offset[None, :] < owner_counts[:, None]
    slot_index = jnp.where(active_flag, starts[:, None] + offset[None, :], 0).reshape(-1).astype(jnp.int32)
    selected_entries = jnp.take(full, slot_index, axis=0)
    return jnp.where(active_flag.reshape(-1)[:, None, None], selected_entries, jnp.zeros_like(selected_entries))
```

```python
import functools
import math

import jax
import jax.numpy as jnp
import ml_dtypes
import numpy as np
from jax import lax
from jax.experimental import pallas as pl
from jax.experimental.pallas import tpu as pltpu
from jax.sharding import PartitionSpec as P

F32, BF16 = jnp.float32, jnp.bfloat16
LATS, LEVS = 32, 8
STRIDE = 32
BLOCKS = 8
SPEC_ROWS, LEG_ROWS = 64, 24
ROWS = SPEC_ROWS + LEG_ROWS
SLOT_ROWS, USED_ROWS = 16, 14
VMEM = pltpu.VMEM


def fourier_tables(points, modes):
    half = points // 2
    j = np.arange(half)
    tables = []
    for parity in range(2):
        d = 2 * np.arange(LATS // 2) + parity
        m = (d[:, None] + STRIDE * np.arange(BLOCKS)[None, :]).reshape(-1)
        angle = (m[:, None] * j[None, :] % points) * (2.0 * math.pi / points)
        tables.append(np.concatenate([np.cos(angle), -np.sin(angle)]) * points**-0.5)
    table = np.stack(tables)
    high = table.astype(np.float32).astype(ml_dtypes.bfloat16)
    low = (table - high.astype(np.float64)).astype(np.float32).astype(ml_dtypes.bfloat16)
    return high, low


def dot_nt(a, b):
    return lax.dot_general(a, b, (((1,), (1,)), ((), ())), preferred_element_type=F32)


def dot_tn(a, b):
    return lax.dot_general(a, b, (((0,), (0,)), ((), ())), preferred_element_type=F32)


def dot_nn(a, b):
    return lax.dot_general(a, b, (((1,), (0,)), ((), ())), preferred_element_type=F32)


def fourier_kernel(members, lev_rows, lat_rows, pieces, *refs):
    f_refs, (leg_ref, hi_ref, lo_ref, out_ref, uhi, ulo, t_ref) = refs[:pieces], refs[pieces:]
    b = pl.program_id(0)
    rows = pl.ds(pl.multiple_of(b * lev_rows, lev_rows), lev_rows)
    for piece in range(pieces // 2):
        lanes = slice(piece * 128, (piece + 1) * 128)
        for lat in range(lat_rows):
            every = pl.ds(lat, lev_rows, stride=lat_rows)
            left, right = f_refs[piece][0, every, :], f_refs[piece + pieces // 2][0, every, :]
            for parity, u in enumerate((left + right, left - right)):
                high = u.astype(BF16)
                uhi[parity, lat, rows, lanes] = high
                ulo[parity, lat, rows, lanes] = (u - high.astype(F32)).astype(BF16)

    @pl.when(b < lat_rows)
    def _():
        table = leg_ref[0].astype(F32)
        lane = lax.broadcasted_iota(jnp.int32, (STRIDE, 2 * 128), 1)

        def block(i):
            return table[STRIDE * i : STRIDE * (i + 1), :]

        tiles = [block(0)[:, :128], block(0)[:, 128:]]
        for p in range(1, BLOCKS // 2):
            other = pltpu.roll(block(BLOCKS - p), STRIDE * p, 1)
            packed = jnp.where(lane >= STRIDE * p, block(p), other)
            tiles += [packed[:, :128], packed[:, 128:]]
        tiles.append(block(BLOCKS // 2)[:, 128:])
        for t, tile in enumerate(tiles):
            first = SPEC_ROWS + (t // 3) * lat_rows
            t_ref[t % 3, pl.ds(first + b, LATS, stride=ROWS), :] = tile

    @pl.when(b == members - 1)
    def _():
        count = LATS // 2 * BLOCKS
        for lat in range(lat_rows):
            for parity in range(2):
                h, l = uhi[parity, lat], ulo[parity, lat]
                acc = dot_nt(hi_ref[parity], h) + (dot_nt(hi_ref[parity], l) + dot_nt(lo_ref[parity], h))
                both = jnp.concatenate([acc[:count], acc[count:]], axis=1)
                for pair in range(LATS // 2):
                    start = (2 * pair + parity) * ROWS + lat
                    for t in range(3):
                        t_ref[t, pl.ds(start, BLOCKS, stride=lat_rows), :] = both[
                            pair * BLOCKS : (pair + 1) * BLOCKS, t * 128 : (t + 1) * 128
                        ]
        for t in range(3):
            for d in range(LATS):
                rows = slice(d * ROWS, (d + 1) * ROWS)
                out_ref[rows, t * 128 : (t + 1) * 128] = t_ref[t, rows, :].astype(BF16)


def fourier(fields, legendre):
    members, lev_rows, lat_rows, points = fields.shape
    modes = legendre.shape[1]
    columns, pieces = 2 * members * lev_rows, points // 128
    rows = fields.reshape(members, lev_rows * lat_rows, points)
    high, low = fourier_tables(points, modes)
    whole = lambda *shape: pl.BlockSpec(shape, lambda b: (0,) * len(shape))
    return pl.pallas_call(
        functools.partial(fourier_kernel, members, lev_rows, lat_rows, pieces),
        grid=(members,),
        in_specs=[
            pl.BlockSpec((1, lev_rows * lat_rows, 128), lambda b, piece=piece: (b, 0, piece))
            for piece in range(pieces)
        ]
        + [
            pl.BlockSpec((1, modes, modes), lambda b: (jnp.minimum(b, lat_rows - 1), 0, 0)),
            whole(*high.shape),
            whole(*low.shape),
        ],
        out_specs=whole(LATS * ROWS, columns),
        out_shape=jax.ShapeDtypeStruct((LATS * ROWS, columns), BF16),
        scratch_shapes=[
            VMEM((2, lat_rows, members * lev_rows, points // 2), BF16),
            VMEM((2, lat_rows, members * lev_rows, points // 2), BF16),
            VMEM((3, LATS * ROWS, 128), F32),
        ],
        compiler_params=pltpu.CompilerParams(vmem_limit_bytes=40 << 20),
        cost_estimate=pl.CostEstimate(flops=5 * 10**9, bytes_accessed=10**7, transcendentals=0),
        name="fourier",
    )(*[rows] * pieces, legendre, jnp.asarray(high), jnp.asarray(low))


def place(i, j):
    p = min(j, BLOCKS - 1 - j)
    base = 3 * i if j < BLOCKS // 2 else 3 * (p + 1) + 3 * i
    return [(2 * p + (base + t) // USED_ROWS, (base + t) % USED_ROWS) for t in range(3)]


def legendre_kernel(members, lev_rows, lat_rows, r_ref, out_ref, t_ref):
    columns = r_ref.shape[2]
    lats = LATS * lat_rows

    def rows_of(first, lanes):
        x = r_ref[:, first : first + lat_rows, lanes].astype(F32)
        return x.reshape(lats, -1).astype(BF16)

    def table(t):
        return rows_of(SPEC_ROWS + (t // 3) * lat_rows, slice((t % 3) * 128, (t % 3 + 1) * 128))

    def spectra(i):
        return rows_of(i * lat_rows, slice(0, columns))

    row = lax.broadcasted_iota(jnp.int32, (columns, columns), 0)
    col = lax.broadcasted_iota(jnp.int32, (columns, columns), 1)
    half = members * lev_rows
    same = ((row >= half) == (col >= half)) & (row % lev_rows == col % lev_rows)
    ones = jnp.where(same, 1.0, 0.0).astype(BF16)

    zero = jnp.zeros((LATS, 128), F32)
    for k in range(2 * BLOCKS // 2):
        for r in range(USED_ROWS - (k % 2), SLOT_ROWS):
            t_ref[pl.ds(k * SLOT_ROWS + r, LATS, stride=LEVS * SLOT_ROWS), :] = zero

    def finish(waves, units):
        high = waves.astype(BF16)
        low = (waves - high.astype(F32)).astype(BF16)
        total = dot_nn(high, ones) + dot_nn(low, ones)
        anomaly = waves - total * (1.0 / members)
        for u, (i, j) in enumerate(units):
            for t, (k, r) in enumerate(place(i, j)):
                t_ref[pl.ds(k * SLOT_ROWS + r, LATS, stride=LEVS * SLOT_ROWS), :] = anomaly[
                    u * STRIDE : (u + 1) * STRIDE, t * 128 : (t + 1) * 128
                ]

    for p in range(BLOCKS // 2):
        first, second = table(2 * p), table(2 * p + 1)
        mine = spectra(p)
        lower, upper = dot_tn(first, mine), dot_tn(second, mine)
        units = [(p, j) for j in range(p, BLOCKS)]
        if p:
            other = dot_tn(first, spectra(BLOCKS - p))
            lower = jnp.concatenate([other[: STRIDE * p], lower[STRIDE * p :]], axis=0)
            units = [(BLOCKS - p, BLOCKS - p + g) for g in range(p)] + units
        finish(lower, units[:4])
        finish(upper, units[4:])
    p = BLOCKS // 2
    finish(dot_tn(table(2 * p), spectra(p)), [(p, j) for j in range(p, BLOCKS)])
    step = LEVS * SLOT_ROWS
    for c in range(LATS):
        out_ref[c * step : (c + 1) * step, :] = t_ref[c * step : (c + 1) * step, :].astype(BF16)


def legendre_stage(received, members, lev_rows, lat_rows):
    rows = LATS * LEVS * SLOT_ROWS
    return pl.pallas_call(
        functools.partial(legendre_kernel, members, lev_rows, lat_rows),
        in_specs=[pl.BlockSpec(memory_space=VMEM)],
        out_specs=pl.BlockSpec(memory_space=VMEM),
        out_shape=jax.ShapeDtypeStruct((rows, 128), BF16),
        scratch_shapes=[VMEM((rows, 128), F32)],
        compiler_params=pltpu.CompilerParams(vmem_limit_bytes=40 << 20),
        cost_estimate=pl.CostEstimate(flops=2 * 10**9, bytes_accessed=4 * 10**6, transcendentals=0),
        name="legendre",
    )(received)


def home(lev):
    p, h = lev // 2, lev % 2
    return p, h


def covariance_kernel(members, lev_rows, y_ref, out_ref):
    levels = LEVS * lev_rows
    count = LATS * SLOT_ROWS
    lev, lat = lax.axis_index("lev"), lax.axis_index("lat")
    p, h = home(lev)
    parts = [y_ref[:, v].reshape(count, 128) for v in range(LEVS)]
    lane = lax.broadcasted_iota(jnp.int32, (count, 128), 1)
    for bit in (1, 2, 4):
        shift = bit * lev_rows
        low = (lane // shift) % 2 == 0
        swapped = list(parts)
        for v in range(LEVS):
            if v & bit:
                continue
            a, b = parts[v], parts[v | bit]
            swapped[v] = jnp.where(low, a, pltpu.roll(b, shift, 1))
            swapped[v | bit] = jnp.where(low, pltpu.roll(a, 128 - shift, 1), b)
        parts = swapped
    first_rows = jnp.where(h == 0, 3 * (p + 1), 0)
    slot = lax.broadcasted_iota(jnp.int32, (levels, count), 1) % SLOT_ROWS
    is_first = slot < first_rows
    one = jnp.zeros((levels, levels), F32)
    two = jnp.zeros((levels, levels), F32)
    for part in parts:
        part = part.astype(BF16)
        turned = part.astype(F32).T
        zero = jnp.zeros_like(turned)
        one += dot_nn(jnp.where(is_first, turned, zero).astype(BF16), part)
        two += dot_nn(jnp.where(is_first, zero, turned).astype(BF16), part)
    for s, (total, n) in enumerate(((one, lat + STRIDE * p), (two, lat + STRIDE * (BLOCKS - 1 - p)))):
        divisor = ((members - 1) * (2 * n + 2)).astype(F32)
        scaled = total / jnp.full((levels, levels), divisor, F32)
        for v in range(LEVS):
            out_ref[v, s * lev_rows : (s + 1) * lev_rows, :] = scaled[v * lev_rows : (v + 1) * lev_rows]


def covariance_stage(received, members, lev_rows):
    return pl.pallas_call(
        functools.partial(covariance_kernel, members, lev_rows),
        in_specs=[pl.BlockSpec(memory_space=VMEM)],
        out_specs=pl.BlockSpec(memory_space=VMEM),
        out_shape=jax.ShapeDtypeStruct((LEVS, 2 * lev_rows, 128), F32),
        compiler_params=pltpu.CompilerParams(vmem_limit_bytes=40 << 20),
        cost_estimate=pl.CostEstimate(flops=10**9, bytes_accessed=2 * 10**6, transcendentals=0),
        name="covariance",
    )(received)


def route_kernel(lev_rows, counts_ref, g_ref, out_ref, f_ref):
    lat = lax.axis_index("lat")
    half = BLOCKS // 2
    for j in range(BLOCKS):
        p, s = min(j, BLOCKS - 1 - j), int(j >= half)
        rows = slice(s * lev_rows, (s + 1) * lev_rows)
        f_ref[j] = g_ref[2 * p, rows, :] + g_ref[2 * p + 1, rows, :]

    def step(owner, start):
        j = jnp.maximum(start - lat + (STRIDE - 1), 0) // STRIDE
        out_ref[owner] = f_ref[jnp.minimum(j, BLOCKS - 1)]
        return start + counts_ref[owner]

    lax.fori_loop(0, LATS, step, jnp.int32(0))


def route_stage(parts, owner_counts, lev_rows):
    return pl.pallas_call(
        functools.partial(route_kernel, lev_rows),
        in_specs=[pl.BlockSpec(memory_space=pltpu.SMEM), pl.BlockSpec(memory_space=VMEM)],
        out_specs=pl.BlockSpec(memory_space=VMEM),
        out_shape=jax.ShapeDtypeStruct((LATS, lev_rows, 128), F32),
        scratch_shapes=[VMEM((BLOCKS, lev_rows, 128), F32)],
        name="route",
    )(owner_counts, parts)


def collect_kernel(counts_ref, r_ref, out_ref):
    lat = lax.axis_index("lat")
    start = lax.fori_loop(0, lat, lambda k, s: s + counts_ref[k], jnp.int32(0))
    count = counts_ref[lat]
    for slot in range(out_ref.shape[0]):
        block = r_ref[(start + slot) % STRIDE]
        out_ref[slot] = jnp.where(slot < count, block, jnp.zeros_like(block))


def collect_stage(routed, owner_counts, capacity, lev_rows):
    return pl.pallas_call(
        collect_kernel,
        in_specs=[pl.BlockSpec(memory_space=pltpu.SMEM), pl.BlockSpec(memory_space=VMEM)],
        out_specs=pl.BlockSpec(memory_space=VMEM),
        out_shape=jax.ShapeDtypeStruct((capacity, lev_rows, 128), F32),
        name="collect",
    )(owner_counts, routed)


def exchange(x, axis):
    return lax.all_to_all(x, axis, split_axis=0, concat_axis=0, tiled=True)


def on_device(fields, legendre, owner_counts):
    members, lev_rows, lat_rows, _ = fields.shape
    modes = legendre.shape[1]
    capacity = 2 * modes // owner_counts.shape[0]
    first = fourier(fields, legendre)
    first = exchange(first.reshape(LATS, ROWS, -1), "lat")
    second = legendre_stage(first, members, lev_rows, lat_rows)
    second = exchange(second.reshape(LATS * LEVS, SLOT_ROWS, 128), ("lat", "lev"))
    third = covariance_stage(second.reshape(LATS, LEVS, SLOT_ROWS, 128), members, lev_rows)
    third = exchange(third, "lev")
    fourth = route_stage(third, owner_counts, lev_rows)
    fourth = exchange(fourth, "lat")
    return collect_stage(fourth, owner_counts, capacity, lev_rows)


def solution(mesh):
    return jax.shard_map(
        on_device,
        mesh=mesh,
        in_specs=(P(None, "lev", "lat", None), P("lat", None, None), P()),
        out_specs=P("lat", "lev", None),
        check_vma=False,
    )
```

```python
import functools
import math

import jax
import jax.numpy as jnp
import ml_dtypes
import numpy as np
from jax import lax
from jax.experimental import pallas as pl
from jax.experimental.pallas import tpu as pltpu
from jax.sharding import PartitionSpec as P

F32, BF16 = jnp.float32, jnp.bfloat16
LATS, LEVS = 32, 8
STRIDE = 32
BLOCKS = 8
SPEC_ROWS, LEG_ROWS = 64, 24
ROWS = SPEC_ROWS + LEG_ROWS
SLOT_ROWS, USED_ROWS = 16, 14
VMEM = pltpu.VMEM


def fourier_tables(points, modes):
    half = points // 2
    j = np.arange(half)
    tables = []
    for parity in range(2):
        d = 2 * np.arange(LATS // 2) + parity
        m = (d[:, None] + STRIDE * np.arange(BLOCKS)[None, :]).reshape(-1)
        angle = (m[:, None] * j[None, :] % points) * (2.0 * math.pi / points)
        tables.append(np.concatenate([np.cos(angle), -np.sin(angle)]) * points**-0.5)
    table = np.stack(tables)
    high = table.astype(np.float32).astype(ml_dtypes.bfloat16)
    low = (table - high.astype(np.float64)).astype(np.float32).astype(ml_dtypes.bfloat16)
    return np.stack([high, low])


def dot_nt(a, b):
    return lax.dot_general(a, b, (((1,), (1,)), ((), ())), preferred_element_type=F32)


def dot_tn(a, b):
    return lax.dot_general(a, b, (((0,), (0,)), ((), ())), preferred_element_type=F32)


def dot_nn(a, b):
    return lax.dot_general(a, b, (((1,), (0,)), ((), ())), preferred_element_type=F32)


def fourier_kernel(members, lev_rows, lat_rows, f_hbm, leg_hbm, tab_hbm, out_ref, f_ref, leg_ref, tab_ref, uhi, ulo, t_ref, f_sem, sem):
    pieces = f_ref.shape[0]
    block_rows = lev_rows * lat_rows

    def fetch(b, piece):
        rows = pl.ds(pl.multiple_of(b * block_rows, block_rows), block_rows)
        source = f_hbm.at[b, :, piece * 128 : (piece + 1) * 128]
        return pltpu.make_async_copy(source, f_ref.at[piece, rows, :], f_sem.at[b, piece])

    leg_copy = pltpu.make_async_copy(leg_hbm, leg_ref, sem.at[0])
    tab_copy = pltpu.make_async_copy(tab_hbm, tab_ref, sem.at[1])
    leg_copy.start()
    for b in range(members):
        for piece in range(pieces):
            fetch(b, piece).start()
    tab_copy.start()
    leg_copy.wait()

    def pack(lat, carry):
        table = leg_ref[lat].astype(F32)
        lane = lax.broadcasted_iota(jnp.int32, (STRIDE, 2 * 128), 1)

        def block(i):
            return table[STRIDE * i : STRIDE * (i + 1), :]

        tiles = [block(0)[:, :128], block(0)[:, 128:]]
        for p in range(1, BLOCKS // 2):
            other = pltpu.roll(block(BLOCKS - p), STRIDE * p, 1)
            packed = jnp.where(lane >= STRIDE * p, block(p), other)
            tiles += [packed[:, :128], packed[:, 128:]]
        tiles.append(block(BLOCKS // 2)[:, 128:])
        for t, tile in enumerate(tiles):
            first = SPEC_ROWS + (t // 3) * lat_rows
            t_ref[t % 3, pl.ds(first + lat, LATS, stride=ROWS), :] = tile
        return carry

    lax.fori_loop(0, lat_rows, pack, 0)

    def split(b, carry):
        rows = pl.ds(pl.multiple_of(b * lev_rows, lev_rows), lev_rows)
        for piece in range(pieces):
            fetch(b, piece).wait()
        for piece in range(pieces // 2):
            lanes = slice(piece * 128, (piece + 1) * 128)
            for lat in range(lat_rows):
                every = pl.ds(b * block_rows + lat, lev_rows, stride=lat_rows)
                left, right = f_ref[piece, every, :], f_ref[piece + pieces // 2, every, :]
                for parity, u in enumerate((left + right, left - right)):
                    high = u.astype(BF16)
                    uhi[parity, lat, rows, lanes] = high
                    ulo[parity, lat, rows, lanes] = (u - high.astype(F32)).astype(BF16)
        return carry

    lax.fori_loop(0, members, split, 0)
    tab_copy.wait()
    count = LATS // 2 * BLOCKS
    for lat in range(lat_rows):
        for parity in range(2):
            h, l = uhi[parity, lat], ulo[parity, lat]
            th, tl = tab_ref[0, parity], tab_ref[1, parity]
            acc = dot_nt(th, h) + (dot_nt(th, l) + dot_nt(tl, h))
            both = jnp.concatenate([acc[:count], acc[count:]], axis=1)
            for pair in range(LATS // 2):
                start = (2 * pair + parity) * ROWS + lat
                for t in range(3):
                    t_ref[t, pl.ds(start, BLOCKS, stride=lat_rows), :] = both[
                        pair * BLOCKS : (pair + 1) * BLOCKS, t * 128 : (t + 1) * 128
                    ]
    for t in range(3):
        for d in range(LATS):
            rows = slice(d * ROWS, (d + 1) * ROWS)
            out_ref[rows, t * 128 : (t + 1) * 128] = t_ref[t, rows, :].astype(BF16)


def fourier(fields, legendre):
    members, lev_rows, lat_rows, points = fields.shape
    modes = legendre.shape[1]
    columns, pieces = 2 * members * lev_rows, points // 128
    tables = fourier_tables(points, modes)
    split_shape = (2, lat_rows, members * lev_rows, points // 2)
    hbm = pl.BlockSpec(memory_space=pltpu.HBM)
    return pl.pallas_call(
        functools.partial(fourier_kernel, members, lev_rows, lat_rows),
        in_specs=[hbm, hbm, hbm],
        out_specs=pl.BlockSpec(memory_space=VMEM),
        out_shape=jax.ShapeDtypeStruct((LATS * ROWS, columns), BF16),
        scratch_shapes=[
            VMEM((pieces, members * lev_rows * lat_rows, 128), F32),
            VMEM(legendre.shape, BF16),
            VMEM(tables.shape, BF16),
            VMEM(split_shape, BF16),
            VMEM(split_shape, BF16),
            VMEM((3, LATS * ROWS, 128), F32),
            pltpu.SemaphoreType.DMA((members, pieces)),
            pltpu.SemaphoreType.DMA((2,)),
        ],
        compiler_params=pltpu.CompilerParams(vmem_limit_bytes=40 << 20),
        cost_estimate=pl.CostEstimate(flops=5 * 10**9, bytes_accessed=10**7, transcendentals=0),
        name="fourier",
    )(*[pltpu.with_memory_space_constraint(x, pltpu.HBM) for x in (fields.reshape(members, lev_rows * lat_rows, points), legendre, jnp.asarray(tables))])


def place(i, j):
    p = min(j, BLOCKS - 1 - j)
    base = 3 * i if j < BLOCKS // 2 else 3 * (p + 1) + 3 * i
    return [(2 * p + (base + t) // USED_ROWS, (base + t) % USED_ROWS) for t in range(3)]


def legendre_kernel(members, lev_rows, lat_rows, r_ref, out_ref, t_ref):
    columns = r_ref.shape[2]
    lats = LATS * lat_rows

    def rows_of(first, lanes):
        x = r_ref[:, first : first + lat_rows, lanes].astype(F32)
        return x.reshape(lats, -1).astype(BF16)

    def table(t):
        return rows_of(SPEC_ROWS + (t // 3) * lat_rows, slice((t % 3) * 128, (t % 3 + 1) * 128))

    def spectra(i):
        return rows_of(i * lat_rows, slice(0, columns))

    row = lax.broadcasted_iota(jnp.int32, (columns, columns), 0)
    col = lax.broadcasted_iota(jnp.int32, (columns, columns), 1)
    half = members * lev_rows
    same = ((row >= half) == (col >= half)) & (row % lev_rows == col % lev_rows)
    ones = jnp.where(same, 1.0, 0.0).astype(BF16)

    zero = jnp.zeros((LATS, 128), F32)
    for k in range(2 * BLOCKS // 2):
        for r in range(USED_ROWS - (k % 2), SLOT_ROWS):
            t_ref[pl.ds(k * SLOT_ROWS + r, LATS, stride=LEVS * SLOT_ROWS), :] = zero

    def finish(waves, units):
        high = waves.astype(BF16)
        low = (waves - high.astype(F32)).astype(BF16)
        total = dot_nn(high, ones) + dot_nn(low, ones)
        anomaly = waves - total * (1.0 / members)
        for u, (i, j) in enumerate(units):
            for t, (k, r) in enumerate(place(i, j)):
                t_ref[pl.ds(k * SLOT_ROWS + r, LATS, stride=LEVS * SLOT_ROWS), :] = anomaly[
                    u * STRIDE : (u + 1) * STRIDE, t * 128 : (t + 1) * 128
                ]

    for p in range(BLOCKS // 2):
        first, second = table(2 * p), table(2 * p + 1)
        mine = spectra(p)
        lower, upper = dot_tn(first, mine), dot_tn(second, mine)
        units = [(p, j) for j in range(p, BLOCKS)]
        if p:
            other = dot_tn(first, spectra(BLOCKS - p))
            lower = jnp.concatenate([other[: STRIDE * p], lower[STRIDE * p :]], axis=0)
            units = [(BLOCKS - p, BLOCKS - p + g) for g in range(p)] + units
        finish(lower, units[:4])
        finish(upper, units[4:])
    p = BLOCKS // 2
    finish(dot_tn(table(2 * p), spectra(p)), [(p, j) for j in range(p, BLOCKS)])
    step = LEVS * SLOT_ROWS
    for c in range(LATS):
        out_ref[c * step : (c + 1) * step, :] = t_ref[c * step : (c + 1) * step, :].astype(BF16)


def legendre_stage(received, members, lev_rows, lat_rows):
    rows = LATS * LEVS * SLOT_ROWS
    return pl.pallas_call(
        functools.partial(legendre_kernel, members, lev_rows, lat_rows),
        in_specs=[pl.BlockSpec(memory_space=VMEM)],
        out_specs=pl.BlockSpec(memory_space=VMEM),
        out_shape=jax.ShapeDtypeStruct((rows, 128), BF16),
        scratch_shapes=[VMEM((rows, 128), F32)],
        compiler_params=pltpu.CompilerParams(vmem_limit_bytes=40 << 20),
        cost_estimate=pl.CostEstimate(flops=2 * 10**9, bytes_accessed=4 * 10**6, transcendentals=0),
        name="legendre",
    )(received)


def home(lev):
    p, h = lev // 2, lev % 2
    return p, h


def covariance_kernel(members, lev_rows, y_ref, out_ref):
    levels = LEVS * lev_rows
    count = LATS * SLOT_ROWS
    lev, lat = lax.axis_index("lev"), lax.axis_index("lat")
    p, h = home(lev)
    parts = [y_ref[:, v].reshape(count, 128) for v in range(LEVS)]
    lane = lax.broadcasted_iota(jnp.int32, (count, 128), 1)
    for bit in (1, 2, 4):
        shift = bit * lev_rows
        low = (lane // shift) % 2 == 0
        swapped = list(parts)
        for v in range(LEVS):
            if v & bit:
                continue
            a, b = parts[v], parts[v | bit]
            swapped[v] = jnp.where(low, a, pltpu.roll(b, shift, 1))
            swapped[v | bit] = jnp.where(low, pltpu.roll(a, 128 - shift, 1), b)
        parts = swapped
    first_rows = jnp.where(h == 0, 3 * (p + 1), 0)
    slot = lax.broadcasted_iota(jnp.int32, (levels, count), 1) % SLOT_ROWS
    is_first = slot < first_rows
    one = jnp.zeros((levels, levels), F32)
    two = jnp.zeros((levels, levels), F32)
    for part in parts:
        part = part.astype(BF16)
        turned = part.astype(F32).T
        zero = jnp.zeros_like(turned)
        one += dot_nn(jnp.where(is_first, turned, zero).astype(BF16), part)
        two += dot_nn(jnp.where(is_first, zero, turned).astype(BF16), part)
    for s, (total, n) in enumerate(((one, lat + STRIDE * p), (two, lat + STRIDE * (BLOCKS - 1 - p)))):
        divisor = ((members - 1) * (2 * n + 2)).astype(F32)
        scaled = (total / jnp.full((levels, levels), divisor, F32)).astype(BF16)
        for v in range(LEVS):
            out_ref[v, s * lev_rows : (s + 1) * lev_rows, :] = scaled[v * lev_rows : (v + 1) * lev_rows]


def covariance_stage(received, members, lev_rows):
    return pl.pallas_call(
        functools.partial(covariance_kernel, members, lev_rows),
        in_specs=[pl.BlockSpec(memory_space=VMEM)],
        out_specs=pl.BlockSpec(memory_space=VMEM),
        out_shape=jax.ShapeDtypeStruct((LEVS, 2 * lev_rows, 128), BF16),
        compiler_params=pltpu.CompilerParams(vmem_limit_bytes=40 << 20),
        cost_estimate=pl.CostEstimate(flops=10**9, bytes_accessed=2 * 10**6, transcendentals=0),
        name="covariance",
    )(received)


def route_kernel(lev_rows, counts_ref, g_ref, out_ref, f_ref):
    lat = lax.axis_index("lat")
    half = BLOCKS // 2
    for j in range(BLOCKS):
        p, s = min(j, BLOCKS - 1 - j), int(j >= half)
        rows = slice(s * lev_rows, (s + 1) * lev_rows)
        f_ref[j] = (g_ref[2 * p, rows, :].astype(F32) + g_ref[2 * p + 1, rows, :].astype(F32)).astype(BF16)

    def step(owner, start):
        j = jnp.maximum(start - lat + (STRIDE - 1), 0) // STRIDE
        out_ref[owner] = f_ref[jnp.minimum(j, BLOCKS - 1)]
        return start + counts_ref[owner]

    lax.fori_loop(0, LATS, step, jnp.int32(0))


def route_stage(parts, owner_counts, lev_rows):
    return pl.pallas_call(
        functools.partial(route_kernel, lev_rows),
        in_specs=[pl.BlockSpec(memory_space=pltpu.SMEM), pl.BlockSpec(memory_space=VMEM)],
        out_specs=pl.BlockSpec(memory_space=VMEM),
        out_shape=jax.ShapeDtypeStruct((LATS, lev_rows, 128), BF16),
        scratch_shapes=[VMEM((BLOCKS, lev_rows, 128), BF16)],
        compiler_params=pltpu.CompilerParams(vmem_limit_bytes=8 << 20),
        name="route",
    )(owner_counts, parts)


def collect_kernel(counts_ref, r_ref, out_ref):
    lat = lax.axis_index("lat")
    start = lax.fori_loop(0, lat, lambda k, s: s + counts_ref[k], jnp.int32(0))
    count = counts_ref[lat]
    for slot in range(out_ref.shape[0]):
        block = r_ref[(start + slot) % STRIDE].astype(F32)
        out_ref[slot] = jnp.where(slot < count, block, jnp.zeros_like(block))


def collect_stage(routed, owner_counts, capacity, lev_rows):
    return pl.pallas_call(
        collect_kernel,
        in_specs=[pl.BlockSpec(memory_space=pltpu.SMEM), pl.BlockSpec(memory_space=VMEM)],
        out_specs=pl.BlockSpec(memory_space=VMEM),
        out_shape=jax.ShapeDtypeStruct((capacity, lev_rows, 128), F32),
        compiler_params=pltpu.CompilerParams(vmem_limit_bytes=8 << 20),
        name="collect",
    )(owner_counts, routed)


def exchange(x, axis):
    return lax.all_to_all(x, axis, split_axis=0, concat_axis=0, tiled=True)


def on_device(fields, legendre, owner_counts):
    members, lev_rows, lat_rows, _ = fields.shape
    modes = legendre.shape[1]
    capacity = 2 * modes // owner_counts.shape[0]
    first = fourier(fields, legendre)
    first = exchange(first.reshape(LATS, ROWS, -1), "lat")
    second = legendre_stage(first, members, lev_rows, lat_rows)
    second = exchange(second.reshape(LATS * LEVS, SLOT_ROWS, 128), ("lat", "lev"))
    third = covariance_stage(second.reshape(LATS, LEVS, SLOT_ROWS, 128), members, lev_rows)
    third = exchange(third, "lev")
    fourth = route_stage(third, owner_counts, lev_rows)
    fourth = exchange(fourth, "lat")
    return collect_stage(fourth, owner_counts, capacity, lev_rows)


def solution(mesh):
    return jax.shard_map(
        on_device,
        mesh=mesh,
        in_specs=(P(None, "lev", "lat", None), P("lat", None, None), P()),
        out_specs=P("lat", "lev", None),
        check_vma=False,
    )
```

```python
import functools
import math

import jax
import jax.numpy as jnp
import ml_dtypes
import numpy as np
from jax import lax
from jax.experimental import pallas as pl
from jax.experimental.pallas import tpu as pltpu
from jax.sharding import PartitionSpec as P

F32, BF16 = jnp.float32, jnp.bfloat16
LATS, LEVS = 32, 8
STRIDE = 32
BLOCKS = 8
SPEC_ROWS, LEG_ROWS = 64, 24
ROWS = SPEC_ROWS + LEG_ROWS
SLOT_ROWS, USED_ROWS = 14, 14
VMEM = pltpu.VMEM


def fourier_tables(points, modes):
    half = points // 2
    j = np.arange(half)
    tables = []
    for parity in range(2):
        d = 2 * np.arange(LATS // 2) + parity
        m = (d[:, None] + STRIDE * np.arange(BLOCKS)[None, :]).reshape(-1)
        angle = (m[:, None] * j[None, :] % points) * (2.0 * math.pi / points)
        tables.append(np.concatenate([np.cos(angle), -np.sin(angle)]) * points**-0.5)
    table = np.stack(tables)
    high = table.astype(np.float32).astype(ml_dtypes.bfloat16)
    low = (table - high.astype(np.float64)).astype(np.float32).astype(ml_dtypes.bfloat16)
    return np.stack([high, low])


def dot_nt(a, b):
    return lax.dot_general(a, b, (((1,), (1,)), ((), ())), preferred_element_type=F32)


def dot_tn(a, b):
    return lax.dot_general(a, b, (((0,), (0,)), ((), ())), preferred_element_type=F32)


def dot_nn(a, b):
    return lax.dot_general(a, b, (((1,), (0,)), ((), ())), preferred_element_type=F32)


def fourier_kernel(members, lev_rows, lat_rows, f_hbm, leg_hbm, tab_hbm, out_ref, f_ref, leg_ref, tab_ref, uhi, ulo, t_ref, f_sem, sem):
    pieces = f_ref.shape[0]
    block_rows = lev_rows * lat_rows

    def fetch(b, piece):
        rows = pl.ds(pl.multiple_of(b * block_rows, block_rows), block_rows)
        source = f_hbm.at[b, :, piece * 128 : (piece + 1) * 128]
        return pltpu.make_async_copy(source, f_ref.at[piece, rows, :], f_sem.at[b, piece])

    leg_copy = pltpu.make_async_copy(leg_hbm, leg_ref, sem.at[0])
    tab_copy = pltpu.make_async_copy(tab_hbm, tab_ref, sem.at[1])
    leg_copy.start()
    for b in range(members):
        for piece in range(pieces):
            fetch(b, piece).start()
    tab_copy.start()
    leg_copy.wait()

    def pack(lat, carry):
        table = leg_ref[lat].astype(F32)
        lane = lax.broadcasted_iota(jnp.int32, (STRIDE, 2 * 128), 1)

        def block(i):
            return table[STRIDE * i : STRIDE * (i + 1), :]

        tiles = [block(0)[:, :128], block(0)[:, 128:]]
        for p in range(1, BLOCKS // 2):
            other = pltpu.roll(block(BLOCKS - p), STRIDE * p, 1)
            packed = jnp.where(lane >= STRIDE * p, block(p), other)
            tiles += [packed[:, :128], packed[:, 128:]]
        tiles.append(block(BLOCKS // 2)[:, 128:])
        for t, tile in enumerate(tiles):
            first = (t // 3) * lat_rows
            t_ref[t % 3, pl.ds(first + lat, LATS, stride=LEG_ROWS), :] = tile
        return carry

    lax.fori_loop(0, lat_rows, pack, 0)
    for t in range(3):
        for d in range(LATS):
            packed = t_ref[t, d * LEG_ROWS : (d + 1) * LEG_ROWS, :]
            out_ref[d * ROWS + SPEC_ROWS : (d + 1) * ROWS, t * 128 : (t + 1) * 128] = packed.astype(BF16)

    width = members * lev_rows

    def split(b, carry):
        for piece in range(pieces):
            fetch(b, piece).wait()
        for piece in range(pieces // 2):
            lanes = slice(piece * 128, (piece + 1) * 128)
            for lat in range(lat_rows):
                every = pl.ds(b * block_rows + lat, lev_rows, stride=lat_rows)
                rows = pl.ds(pl.multiple_of(lat * width + b * lev_rows, lev_rows), lev_rows)
                left, right = f_ref[piece, every, :], f_ref[piece + pieces // 2, every, :]
                for parity, u in enumerate((left + right, left - right)):
                    high = u.astype(BF16)
                    uhi[parity, rows, lanes] = high
                    ulo[parity, rows, lanes] = (u - high.astype(F32)).astype(BF16)
        return carry

    lax.fori_loop(0, members, split, 0)
    tab_copy.wait()
    count = LATS // 2 * BLOCKS
    group = lat_rows // 2
    for parity in range(2):
        th, tl = tab_ref[0, parity], tab_ref[1, parity]
        for g in range(2):
            columns = slice(g * group * width, (g + 1) * group * width)
            h, l = uhi[parity, columns], ulo[parity, columns]
            acc = dot_nt(th, h) + (dot_nt(th, l) + dot_nt(tl, h))
            for k in range(group):
                part = acc[:, k * width : (k + 1) * width]
                both = jnp.concatenate([part[:count], part[count:]], axis=1).astype(BF16)
                for pair in range(LATS // 2):
                    start = (2 * pair + parity) * ROWS + (g * group + k) * BLOCKS
                    out_ref[start : start + BLOCKS, :] = both[pair * BLOCKS : (pair + 1) * BLOCKS]


def fourier(fields, legendre):
    members, lev_rows, lat_rows, points = fields.shape
    modes = legendre.shape[1]
    columns, pieces = 2 * members * lev_rows, points // 128
    tables = fourier_tables(points, modes)
    split_shape = (2, lat_rows * members * lev_rows, points // 2)
    hbm = pl.BlockSpec(memory_space=pltpu.HBM)
    return pl.pallas_call(
        functools.partial(fourier_kernel, members, lev_rows, lat_rows),
        in_specs=[hbm, hbm, hbm],
        out_specs=pl.BlockSpec(memory_space=VMEM),
        out_shape=jax.ShapeDtypeStruct((LATS * ROWS, columns), BF16),
        scratch_shapes=[
            VMEM((pieces, members * lev_rows * lat_rows, 128), F32),
            VMEM(legendre.shape, BF16),
            VMEM(tables.shape, BF16),
            VMEM(split_shape, BF16),
            VMEM(split_shape, BF16),
            VMEM((3, LATS * LEG_ROWS, 128), F32),
            pltpu.SemaphoreType.DMA((members, pieces)),
            pltpu.SemaphoreType.DMA((2,)),
        ],
        compiler_params=pltpu.CompilerParams(vmem_limit_bytes=40 << 20),
        cost_estimate=pl.CostEstimate(flops=5 * 10**9, bytes_accessed=10**7, transcendentals=0),
        name="fourier",
    )(*[pltpu.with_memory_space_constraint(x, pltpu.HBM) for x in (fields.reshape(members, lev_rows * lat_rows, points), legendre, jnp.asarray(tables))])


def place(i, j):
    p = min(j, BLOCKS - 1 - j)
    base = 3 * i if j < BLOCKS // 2 else 3 * (p + 1) + 3 * i
    return [(2 * p + (base + t) // USED_ROWS, (base + t) % USED_ROWS) for t in range(3)]


def legendre_kernel(members, lev_rows, lat_rows, r_ref, out_ref, t_ref, s_ref):
    columns = r_ref.shape[2]
    lats = LATS * lat_rows
    for t in range(3):
        for s in range(LATS):
            rows = slice(s * SPEC_ROWS, (s + 1) * SPEC_ROWS)
            s_ref[t, rows, :] = r_ref[s, :SPEC_ROWS, t * 128 : (t + 1) * 128].astype(F32)

    def rows_of(first, lanes):
        x = r_ref[:, first : first + lat_rows, lanes].astype(F32)
        return x.reshape(lats, -1).astype(BF16)

    def table(t):
        return rows_of(SPEC_ROWS + (t // 3) * lat_rows, slice((t % 3) * 128, (t % 3 + 1) * 128))

    def spectra(i):
        tiles = [s_ref[t, pl.ds(i, lats, stride=BLOCKS), :] for t in range(3)]
        return jnp.concatenate(tiles, axis=1).astype(BF16)

    row = lax.broadcasted_iota(jnp.int32, (columns, columns), 0)
    col = lax.broadcasted_iota(jnp.int32, (columns, columns), 1)
    half = members * lev_rows
    same = ((row >= half) == (col >= half)) & (row % lev_rows == col % lev_rows)
    ones = jnp.where(same, 1.0, 0.0).astype(BF16)

    zero = jnp.zeros((LATS, 128), F32)
    for k in range(2 * BLOCKS // 2):
        for r in range(USED_ROWS - (k % 2), SLOT_ROWS):
            t_ref[pl.ds(k * SLOT_ROWS + r, LATS, stride=LEVS * SLOT_ROWS), :] = zero

    def finish(waves, units):
        high = waves.astype(BF16)
        low = (waves - high.astype(F32)).astype(BF16)
        total = dot_nn(high, ones) + dot_nn(low, ones)
        anomaly = waves - total * (1.0 / members)
        for u, (i, j) in enumerate(units):
            for t, (k, r) in enumerate(place(i, j)):
                t_ref[pl.ds(k * SLOT_ROWS + r, LATS, stride=LEVS * SLOT_ROWS), :] = anomaly[
                    u * STRIDE : (u + 1) * STRIDE, t * 128 : (t + 1) * 128
                ]

    for p in range(BLOCKS // 2):
        first, second = table(2 * p), table(2 * p + 1)
        mine = spectra(p)
        lower, upper = dot_tn(first, mine), dot_tn(second, mine)
        units = [(p, j) for j in range(p, BLOCKS)]
        if p:
            other = dot_tn(first, spectra(BLOCKS - p))
            lower = jnp.concatenate([other[: STRIDE * p], lower[STRIDE * p :]], axis=0)
            units = [(BLOCKS - p, BLOCKS - p + g) for g in range(p)] + units
        finish(lower, units[:4])
        finish(upper, units[4:])
    p = BLOCKS // 2
    finish(dot_tn(table(2 * p), spectra(p)), [(p, j) for j in range(p, BLOCKS)])
    step = LEVS * SLOT_ROWS
    for c in range(LATS):
        out_ref[c * step : (c + 1) * step, :] = t_ref[c * step : (c + 1) * step, :].astype(BF16)


def legendre_stage(received, members, lev_rows, lat_rows):
    rows = LATS * LEVS * SLOT_ROWS
    return pl.pallas_call(
        functools.partial(legendre_kernel, members, lev_rows, lat_rows),
        in_specs=[pl.BlockSpec(memory_space=VMEM)],
        out_specs=pl.BlockSpec(memory_space=VMEM),
        out_shape=jax.ShapeDtypeStruct((rows, 128), BF16),
        scratch_shapes=[VMEM((rows, 128), F32), VMEM((3, LATS * SPEC_ROWS, 128), F32)],
        compiler_params=pltpu.CompilerParams(vmem_limit_bytes=40 << 20),
        cost_estimate=pl.CostEstimate(flops=2 * 10**9, bytes_accessed=4 * 10**6, transcendentals=0),
        name="legendre",
    )(received)


def home(lev):
    p, h = lev // 2, lev % 2
    return p, h


def covariance_kernel(members, lev_rows, y_ref, out_ref, t_ref):
    levels = LEVS * lev_rows
    count = LATS * SLOT_ROWS
    lev, lat = lax.axis_index("lev"), lax.axis_index("lat")
    p, h = home(lev)
    step = LEVS * SLOT_ROWS
    for d in range(LATS):
        t_ref[d * step : (d + 1) * step, :] = y_ref[d * step : (d + 1) * step, :].astype(F32)
    parts = []
    for v in range(LEVS):
        rows = [t_ref[pl.ds(v * SLOT_ROWS + r, LATS, stride=step), :] for r in range(SLOT_ROWS)]
        parts.append(jnp.concatenate(rows, axis=0).astype(BF16))
    lane = lax.broadcasted_iota(jnp.int32, (count, 128), 1)
    for bit in (1, 2, 4):
        shift = bit * lev_rows
        low = (lane // shift) % 2 == 0
        swapped = list(parts)
        for v in range(LEVS):
            if v & bit:
                continue
            a, b = parts[v], parts[v | bit]
            swapped[v] = jnp.where(low, a, pltpu.roll(b, shift, 1))
            swapped[v | bit] = jnp.where(low, pltpu.roll(a, 128 - shift, 1), b)
        parts = swapped
    first_rows = jnp.where(h == 0, 3 * (p + 1), 0)
    slot = lax.broadcasted_iota(jnp.int32, (levels, count), 1) // LATS
    is_first = slot < first_rows
    one = jnp.zeros((levels, levels), F32)
    two = jnp.zeros((levels, levels), F32)
    for part in parts:
        turned = part.astype(F32).T
        zero = jnp.zeros_like(turned)
        one += dot_nn(jnp.where(is_first, turned, zero).astype(BF16), part)
        two += dot_nn(jnp.where(is_first, zero, turned).astype(BF16), part)
    for s, (total, n) in enumerate(((one, lat + STRIDE * p), (two, lat + STRIDE * (BLOCKS - 1 - p)))):
        divisor = ((members - 1) * (2 * n + 2)).astype(F32)
        scaled = (total / jnp.full((levels, levels), divisor, F32)).astype(BF16)
        for v in range(LEVS):
            out_ref[v, s * lev_rows : (s + 1) * lev_rows, :] = scaled[v * lev_rows : (v + 1) * lev_rows]


def covariance_stage(received, members, lev_rows):
    return pl.pallas_call(
        functools.partial(covariance_kernel, members, lev_rows),
        in_specs=[pl.BlockSpec(memory_space=VMEM)],
        out_specs=pl.BlockSpec(memory_space=VMEM),
        out_shape=jax.ShapeDtypeStruct((LEVS, 2 * lev_rows, 128), BF16),
        scratch_shapes=[VMEM(received.shape, F32)],
        compiler_params=pltpu.CompilerParams(vmem_limit_bytes=40 << 20),
        cost_estimate=pl.CostEstimate(flops=10**9, bytes_accessed=2 * 10**6, transcendentals=0),
        name="covariance",
    )(received)


def route_kernel(lev_rows, counts_ref, g_ref, out_ref, f_ref):
    lat = lax.axis_index("lat")
    half = BLOCKS // 2
    for j in range(BLOCKS):
        p, s = min(j, BLOCKS - 1 - j), int(j >= half)
        rows = slice(s * lev_rows, (s + 1) * lev_rows)
        f_ref[j] = (g_ref[2 * p, rows, :].astype(F32) + g_ref[2 * p + 1, rows, :].astype(F32)).astype(BF16)

    def step(owner, start):
        j = jnp.maximum(start - lat + (STRIDE - 1), 0) // STRIDE
        out_ref[owner] = f_ref[jnp.minimum(j, BLOCKS - 1)]
        return start + counts_ref[owner]

    lax.fori_loop(0, LATS, step, jnp.int32(0))


def route_stage(parts, owner_counts, lev_rows):
    return pl.pallas_call(
        functools.partial(route_kernel, lev_rows),
        in_specs=[pl.BlockSpec(memory_space=pltpu.SMEM), pl.BlockSpec(memory_space=VMEM)],
        out_specs=pl.BlockSpec(memory_space=VMEM),
        out_shape=jax.ShapeDtypeStruct((LATS, lev_rows, 128), BF16),
        scratch_shapes=[VMEM((BLOCKS, lev_rows, 128), BF16)],
        compiler_params=pltpu.CompilerParams(vmem_limit_bytes=8 << 20),
        name="route",
    )(owner_counts, parts)


def collect_kernel(counts_ref, r_ref, out_ref):
    lat = lax.axis_index("lat")
    start = lax.fori_loop(0, lat, lambda k, s: s + counts_ref[k], jnp.int32(0))
    count = counts_ref[lat]
    for slot in range(out_ref.shape[0]):
        block = r_ref[(start + slot) % STRIDE].astype(F32)
        out_ref[slot] = jnp.where(slot < count, block, jnp.zeros_like(block))


def collect_stage(routed, owner_counts, capacity, lev_rows):
    return pl.pallas_call(
        collect_kernel,
        in_specs=[pl.BlockSpec(memory_space=pltpu.SMEM), pl.BlockSpec(memory_space=VMEM)],
        out_specs=pl.BlockSpec(memory_space=VMEM),
        out_shape=jax.ShapeDtypeStruct((capacity, lev_rows, 128), F32),
        compiler_params=pltpu.CompilerParams(vmem_limit_bytes=8 << 20),
        name="collect",
    )(owner_counts, routed)


def exchange(x, axis):
    return lax.all_to_all(x, axis, split_axis=0, concat_axis=0, tiled=True)


def on_device(fields, legendre, owner_counts):
    members, lev_rows, lat_rows, _ = fields.shape
    modes = legendre.shape[1]
    capacity = 2 * modes // owner_counts.shape[0]
    first = fourier(fields, legendre)
    first = exchange(first.reshape(LATS, ROWS, -1), "lat")
    second = legendre_stage(first, members, lev_rows, lat_rows)
    second = exchange(second.reshape(LATS * LEVS, SLOT_ROWS // 2, 2, 128), ("lat", "lev"))
    third = covariance_stage(second.reshape(-1, 128), members, lev_rows)
    third = exchange(third, "lev")
    fourth = route_stage(third, owner_counts, lev_rows)
    fourth = exchange(fourth, "lat")
    return collect_stage(fourth, owner_counts, capacity, lev_rows)


def solution(mesh):
    return jax.shard_map(
        on_device,
        mesh=mesh,
        in_specs=(P(None, "lev", "lat", None), P("lat", None, None), P()),
        out_specs=P("lat", "lev", None),
        check_vma=False,
    )
```

```python
import functools
import math

import jax
import jax.numpy as jnp
import ml_dtypes
import numpy as np
from jax import lax
from jax.experimental import pallas as pl
from jax.experimental.pallas import tpu as pltpu
from jax.sharding import PartitionSpec as P

F32, BF16 = jnp.float32, jnp.bfloat16
LATS, LEVS = 32, 8
STRIDE = 32
BLOCKS = 8
SPEC_ROWS, LEG_ROWS = 64, 24
ROWS = SPEC_ROWS + LEG_ROWS
SLOT_ROWS, USED_ROWS = 14, 14
VMEM = pltpu.VMEM


def fourier_tables(points, modes):
    half = points // 2
    j = np.arange(half)
    tables = []
    for parity in range(2):
        d = 2 * np.arange(LATS // 2) + parity
        m = (d[:, None] + STRIDE * np.arange(BLOCKS)[None, :]).reshape(-1)
        angle = (m[:, None] * j[None, :] % points) * (2.0 * math.pi / points)
        tables.append(np.concatenate([np.cos(angle), -np.sin(angle)]) * points**-0.5)
    table = np.stack(tables)
    high = table.astype(np.float32).astype(ml_dtypes.bfloat16)
    low = (table - high.astype(np.float64)).astype(np.float32).astype(ml_dtypes.bfloat16)
    return np.stack([high, low])


def dot_nt(a, b):
    return lax.dot_general(a, b, (((1,), (1,)), ((), ())), preferred_element_type=F32)


def dot_tn(a, b):
    return lax.dot_general(a, b, (((0,), (0,)), ((), ())), preferred_element_type=F32)


def dot_nn(a, b):
    return lax.dot_general(a, b, (((1,), (0,)), ((), ())), preferred_element_type=F32)


def fourier_kernel(members, lev_rows, lat_rows, f_hbm, leg_hbm, tab_hbm, out_ref, f_ref, leg_ref, tab_ref, uhi, ulo, t_ref, f_sem, sem):
    pieces = f_ref.shape[0]
    block_rows = lev_rows * lat_rows

    def fetch(b, piece):
        rows = pl.ds(pl.multiple_of(b * block_rows, block_rows), block_rows)
        source = f_hbm.at[b, :, piece * 128 : (piece + 1) * 128]
        return pltpu.make_async_copy(source, f_ref.at[piece, rows, :], f_sem.at[b, piece])

    leg_copy = pltpu.make_async_copy(leg_hbm, leg_ref, sem.at[0])
    tab_copy = pltpu.make_async_copy(tab_hbm, tab_ref, sem.at[1])
    for b in range(members):
        for piece in range(pieces):
            fetch(b, piece).start()
    tab_copy.start()
    leg_copy.start()

    def pack(lat):
        table = leg_ref[lat].astype(F32)
        lane = lax.broadcasted_iota(jnp.int32, (STRIDE, 2 * 128), 1)

        def block(i):
            return table[STRIDE * i : STRIDE * (i + 1), :]

        tiles = [block(0)[:, :128], block(0)[:, 128:]]
        for p in range(1, BLOCKS // 2):
            other = pltpu.roll(block(BLOCKS - p), STRIDE * p, 1)
            packed = jnp.where(lane >= STRIDE * p, block(p), other)
            tiles += [packed[:, :128], packed[:, 128:]]
        tiles.append(block(BLOCKS // 2)[:, 128:])
        for t, tile in enumerate(tiles):
            first = (t // 3) * lat_rows
            t_ref[t % 3, pl.ds(first + lat, LATS, stride=LEG_ROWS), :] = tile

    width = members * lev_rows

    def split(b, carry):
        for piece in range(pieces):
            fetch(b, piece).wait()
        for piece in range(pieces // 2):
            lanes = slice(piece * 128, (piece + 1) * 128)
            for lat in range(lat_rows):
                every = pl.ds(b * block_rows + lat, lev_rows, stride=lat_rows)
                rows = pl.ds(pl.multiple_of(lat * width + b * lev_rows, lev_rows), lev_rows)
                left, right = f_ref[piece, every, :], f_ref[piece + pieces // 2, every, :]
                for parity, u in enumerate((left + right, left - right)):
                    high = u.astype(BF16)
                    uhi[parity, rows, lanes] = high
                    ulo[parity, rows, lanes] = (u - high.astype(F32)).astype(BF16)
        return carry

    lax.fori_loop(0, members, split, 0)
    tab_copy.wait()
    leg_copy.wait()
    count = LATS // 2 * BLOCKS
    group = lat_rows // 2
    for parity in range(2):
        th, tl = tab_ref[0, parity], tab_ref[1, parity]
        for g in range(2):
            for k in range(lat_rows // 4):
                pack((2 * parity + g) * (lat_rows // 4) + k)
            columns = slice(g * group * width, (g + 1) * group * width)
            h, l = uhi[parity, columns], ulo[parity, columns]
            acc = dot_nt(th, h) + (dot_nt(th, l) + dot_nt(tl, h))
            for k in range(group):
                part = acc[:, k * width : (k + 1) * width]
                both = jnp.concatenate([part[:count], part[count:]], axis=1).astype(BF16)
                for pair in range(LATS // 2):
                    start = (2 * pair + parity) * ROWS + (g * group + k) * BLOCKS
                    out_ref[start : start + BLOCKS, :] = both[pair * BLOCKS : (pair + 1) * BLOCKS]
    for t in range(3):
        for d in range(LATS):
            packed = t_ref[t, d * LEG_ROWS : (d + 1) * LEG_ROWS, :]
            out_ref[d * ROWS + SPEC_ROWS : (d + 1) * ROWS, t * 128 : (t + 1) * 128] = packed.astype(BF16)


def fourier(fields, legendre):
    members, lev_rows, lat_rows, points = fields.shape
    modes = legendre.shape[1]
    columns, pieces = 2 * members * lev_rows, points // 128
    tables = fourier_tables(points, modes)
    split_shape = (2, lat_rows * members * lev_rows, points // 2)
    hbm = pl.BlockSpec(memory_space=pltpu.HBM)
    return pl.pallas_call(
        functools.partial(fourier_kernel, members, lev_rows, lat_rows),
        in_specs=[hbm, hbm, hbm],
        out_specs=pl.BlockSpec(memory_space=VMEM),
        out_shape=jax.ShapeDtypeStruct((LATS * ROWS, columns), BF16),
        scratch_shapes=[
            VMEM((pieces, members * lev_rows * lat_rows, 128), F32),
            VMEM(legendre.shape, BF16),
            VMEM(tables.shape, BF16),
            VMEM(split_shape, BF16),
            VMEM(split_shape, BF16),
            VMEM((3, LATS * LEG_ROWS, 128), F32),
            pltpu.SemaphoreType.DMA((members, pieces)),
            pltpu.SemaphoreType.DMA((2,)),
        ],
        compiler_params=pltpu.CompilerParams(vmem_limit_bytes=40 << 20),
        cost_estimate=pl.CostEstimate(flops=5 * 10**9, bytes_accessed=10**7, transcendentals=0),
        name="fourier",
    )(*[pltpu.with_memory_space_constraint(x, pltpu.HBM) for x in (fields.reshape(members, lev_rows * lat_rows, points), legendre, jnp.asarray(tables))])


def place(i, j):
    p = min(j, BLOCKS - 1 - j)
    base = 3 * i if j < BLOCKS // 2 else 3 * (p + 1) + 3 * i
    return [(2 * p + (base + t) // USED_ROWS, (base + t) % USED_ROWS) for t in range(3)]


def legendre_kernel(members, lev_rows, lat_rows, r_ref, out_ref, t_ref, s_ref):
    columns = r_ref.shape[2]
    lats = LATS * lat_rows
    for t in range(3):
        for s in range(LATS):
            rows = slice(s * SPEC_ROWS, (s + 1) * SPEC_ROWS)
            s_ref[t, rows, :] = r_ref[s, :SPEC_ROWS, t * 128 : (t + 1) * 128].astype(F32)

    def rows_of(first, lanes):
        x = r_ref[:, first : first + lat_rows, lanes].astype(F32)
        return x.reshape(lats, -1).astype(BF16)

    def table(t):
        return rows_of(SPEC_ROWS + (t // 3) * lat_rows, slice((t % 3) * 128, (t % 3 + 1) * 128))

    def spectra(i):
        tiles = [s_ref[t, pl.ds(i, lats, stride=BLOCKS), :] for t in range(3)]
        return jnp.concatenate(tiles, axis=1).astype(BF16)

    row = lax.broadcasted_iota(jnp.int32, (columns, columns), 0)
    col = lax.broadcasted_iota(jnp.int32, (columns, columns), 1)
    half = members * lev_rows
    same = ((row >= half) == (col >= half)) & (row % lev_rows == col % lev_rows)
    ones = jnp.where(same, 1.0, 0.0).astype(BF16)

    zero = jnp.zeros((LATS, 128), F32)
    for k in range(2 * BLOCKS // 2):
        for r in range(USED_ROWS - (k % 2), SLOT_ROWS):
            t_ref[pl.ds(k * LATS * SLOT_ROWS + r, LATS, stride=SLOT_ROWS), :] = zero

    def finish(waves, units):
        high = waves.astype(BF16)
        low = (waves - high.astype(F32)).astype(BF16)
        total = dot_nn(high, ones) + dot_nn(low, ones)
        anomaly = waves - total * (1.0 / members)
        for u, (i, j) in enumerate(units):
            for t, (k, r) in enumerate(place(i, j)):
                t_ref[pl.ds(k * LATS * SLOT_ROWS + r, LATS, stride=SLOT_ROWS), :] = anomaly[
                    u * STRIDE : (u + 1) * STRIDE, t * 128 : (t + 1) * 128
                ]

    for p in range(BLOCKS // 2):
        first, second = table(2 * p), table(2 * p + 1)
        mine = spectra(p)
        lower, upper = dot_tn(first, mine), dot_tn(second, mine)
        units = [(p, j) for j in range(p, BLOCKS)]
        if p:
            other = dot_tn(first, spectra(BLOCKS - p))
            lower = jnp.concatenate([other[: STRIDE * p], lower[STRIDE * p :]], axis=0)
            units = [(BLOCKS - p, BLOCKS - p + g) for g in range(p)] + units
        finish(lower, units[:4])
        finish(upper, units[4:])
    p = BLOCKS // 2
    finish(dot_tn(table(2 * p), spectra(p)), [(p, j) for j in range(p, BLOCKS)])
    step = LATS * SLOT_ROWS
    for k in range(LEVS):
        out_ref[k * step : (k + 1) * step, :] = t_ref[k * step : (k + 1) * step, :].astype(BF16)


def legendre_stage(received, members, lev_rows, lat_rows):
    rows = LATS * LEVS * SLOT_ROWS
    return pl.pallas_call(
        functools.partial(legendre_kernel, members, lev_rows, lat_rows),
        in_specs=[pl.BlockSpec(memory_space=VMEM)],
        out_specs=pl.BlockSpec(memory_space=VMEM),
        out_shape=jax.ShapeDtypeStruct((rows, 128), BF16),
        scratch_shapes=[VMEM((rows, 128), F32), VMEM((3, LATS * SPEC_ROWS, 128), F32)],
        compiler_params=pltpu.CompilerParams(vmem_limit_bytes=40 << 20),
        cost_estimate=pl.CostEstimate(flops=2 * 10**9, bytes_accessed=4 * 10**6, transcendentals=0),
        name="legendre",
    )(received)


def home(lev):
    p, h = lev // 2, lev % 2
    return p, h


def covariance_kernel(members, lev_rows, y_ref, out_ref):
    levels = LEVS * lev_rows
    count = LATS * SLOT_ROWS
    lev, lat = lax.axis_index("lev"), lax.axis_index("lat")
    p, h = home(lev)
    parts = [y_ref[v * count : (v + 1) * count, :] for v in range(LEVS)]
    lane = lax.broadcasted_iota(jnp.int32, (count, 128), 1)
    for bit in (1, 2, 4):
        shift = bit * lev_rows
        low = (lane // shift) % 2 == 0
        swapped = list(parts)
        for v in range(LEVS):
            if v & bit:
                continue
            a, b = parts[v], parts[v | bit]
            swapped[v] = jnp.where(low, a, pltpu.roll(b, shift, 1))
            swapped[v | bit] = jnp.where(low, pltpu.roll(a, 128 - shift, 1), b)
        parts = swapped
    first_rows = jnp.where(h == 0, 3 * (p + 1), 0)
    slot = lax.broadcasted_iota(jnp.int32, (levels, count), 1) % SLOT_ROWS
    is_first = slot < first_rows
    one = jnp.zeros((levels, levels), F32)
    two = jnp.zeros((levels, levels), F32)
    for part in parts:
        turned = part.astype(F32).T
        zero = jnp.zeros_like(turned)
        one += dot_nn(jnp.where(is_first, turned, zero).astype(BF16), part)
        two += dot_nn(jnp.where(is_first, zero, turned).astype(BF16), part)
    for s, (total, n) in enumerate(((one, lat + STRIDE * p), (two, lat + STRIDE * (BLOCKS - 1 - p)))):
        divisor = ((members - 1) * (2 * n + 2)).astype(F32)
        scaled = (total / jnp.full((levels, levels), divisor, F32)).astype(BF16)
        for v in range(LEVS):
            out_ref[v, s * lev_rows : (s + 1) * lev_rows, :] = scaled[v * lev_rows : (v + 1) * lev_rows]


def covariance_stage(received, members, lev_rows):
    return pl.pallas_call(
        functools.partial(covariance_kernel, members, lev_rows),
        in_specs=[pl.BlockSpec(memory_space=VMEM)],
        out_specs=pl.BlockSpec(memory_space=VMEM),
        out_shape=jax.ShapeDtypeStruct((LEVS, 2 * lev_rows, 128), BF16),
        compiler_params=pltpu.CompilerParams(vmem_limit_bytes=40 << 20),
        cost_estimate=pl.CostEstimate(flops=10**9, bytes_accessed=2 * 10**6, transcendentals=0),
        name="covariance",
    )(received)


def route_kernel(lev_rows, counts_ref, g_ref, out_ref, f_ref):
    lat = lax.axis_index("lat")
    half = BLOCKS // 2
    for j in range(BLOCKS):
        p, s = min(j, BLOCKS - 1 - j), int(j >= half)
        rows = slice(s * lev_rows, (s + 1) * lev_rows)
        f_ref[j] = (g_ref[2 * p, rows, :].astype(F32) + g_ref[2 * p + 1, rows, :].astype(F32)).astype(BF16)

    def step(owner, start):
        j = jnp.maximum(start - lat + (STRIDE - 1), 0) // STRIDE
        out_ref[owner] = f_ref[jnp.minimum(j, BLOCKS - 1)]
        return start + counts_ref[owner]

    lax.fori_loop(0, LATS, step, jnp.int32(0))


def route_stage(parts, owner_counts, lev_rows):
    return pl.pallas_call(
        functools.partial(route_kernel, lev_rows),
        in_specs=[pl.BlockSpec(memory_space=pltpu.SMEM), pl.BlockSpec(memory_space=VMEM)],
        out_specs=pl.BlockSpec(memory_space=VMEM),
        out_shape=jax.ShapeDtypeStruct((LATS, lev_rows, 128), BF16),
        scratch_shapes=[VMEM((BLOCKS, lev_rows, 128), BF16)],
        compiler_params=pltpu.CompilerParams(vmem_limit_bytes=8 << 20),
        name="route",
    )(owner_counts, parts)


def collect_kernel(counts_ref, r_ref, out_ref):
    lat = lax.axis_index("lat")
    start = lax.fori_loop(0, lat, lambda k, s: s + counts_ref[k], jnp.int32(0))
    count = counts_ref[lat]
    for slot in range(out_ref.shape[0]):
        block = r_ref[(start + slot) % STRIDE].astype(F32)
        out_ref[slot] = jnp.where(slot < count, block, jnp.zeros_like(block))


def collect_stage(routed, owner_counts, capacity, lev_rows):
    return pl.pallas_call(
        collect_kernel,
        in_specs=[pl.BlockSpec(memory_space=pltpu.SMEM), pl.BlockSpec(memory_space=VMEM)],
        out_specs=pl.BlockSpec(memory_space=VMEM),
        out_shape=jax.ShapeDtypeStruct((capacity, lev_rows, 128), F32),
        compiler_params=pltpu.CompilerParams(vmem_limit_bytes=8 << 20),
        name="collect",
    )(owner_counts, routed)


def exchange(x, axis):
    return lax.all_to_all(x, axis, split_axis=0, concat_axis=0, tiled=True)


def on_device(fields, legendre, owner_counts):
    members, lev_rows, lat_rows, _ = fields.shape
    modes = legendre.shape[1]
    capacity = 2 * modes // owner_counts.shape[0]
    first = fourier(fields, legendre)
    first = exchange(first.reshape(LATS, ROWS, -1), "lat")
    second = legendre_stage(first, members, lev_rows, lat_rows)
    second = exchange(second.reshape(LATS * LEVS, SLOT_ROWS // 2, 2, 128), ("lev", "lat"))
    third = covariance_stage(second.reshape(-1, 128), members, lev_rows)
    third = exchange(third, "lev")
    fourth = route_stage(third, owner_counts, lev_rows)
    fourth = exchange(fourth, "lat")
    return collect_stage(fourth, owner_counts, capacity, lev_rows)


def solution(mesh):
    return jax.shard_map(
        on_device,
        mesh=mesh,
        in_specs=(P(None, "lev", "lat", None), P("lat", None, None), P()),
        out_specs=P("lat", "lev", None),
        check_vma=False,
    )
```

```python
import functools
import math

import jax
import jax.numpy as jnp
import ml_dtypes
import numpy as np
from jax import lax
from jax.experimental import pallas as pl
from jax.experimental.pallas import tpu as pltpu
from jax.sharding import PartitionSpec as P

F32, BF16 = jnp.float32, jnp.bfloat16
LATS, LEVS = 32, 8
STRIDE = 32
BLOCKS = 8
SPEC_ROWS, LEG_ROWS = 64, 24
ROWS = SPEC_ROWS + LEG_ROWS
SLOT_ROWS, USED_ROWS = 14, 14
CLASSES = ((0, 4, 4), (2, 4, 4), (1, 2, 2))
VMEM = pltpu.VMEM


def fourier_tables(points, modes):
    tables = []
    for first, step, fold in CLASSES:
        j = np.arange(points // fold)
        m = (np.arange(first, LATS, step)[:, None] + STRIDE * np.arange(BLOCKS)[None, :]).reshape(-1)
        angle = (m[:, None] * j[None, :] % points) * (2.0 * math.pi / points)
        table = np.concatenate([np.cos(angle), -np.sin(angle)]) * points**-0.5
        high = table.astype(np.float32).astype(ml_dtypes.bfloat16)
        low = (table - high.astype(np.float64)).astype(np.float32).astype(ml_dtypes.bfloat16)
        tables.append(np.concatenate([high, low]))
    return tables


def dot_nt(a, b):
    return lax.dot_general(a, b, (((1,), (1,)), ((), ())), preferred_element_type=F32)


def dot_tn(a, b):
    return lax.dot_general(a, b, (((0,), (0,)), ((), ())), preferred_element_type=F32)


def dot_nn(a, b):
    return lax.dot_general(a, b, (((1,), (0,)), ((), ())), preferred_element_type=F32)


def fourier_kernel(members, lev_rows, lat_rows, f_hbm, leg_hbm, *refs):
    classes = len(CLASSES)
    tab_hbm, (out_ref, f_ref, leg_ref), refs = refs[:classes], refs[classes : classes + 3], refs[classes + 3 :]
    tab_refs, high_refs, low_refs = refs[:classes], refs[classes : 2 * classes], refs[2 * classes : 3 * classes]
    t_ref, f_sem, sem = refs[3 * classes :]
    pieces = f_ref.shape[0]
    block_rows = lev_rows * lat_rows

    def fetch(b, piece):
        rows = pl.ds(pl.multiple_of(b * block_rows, block_rows), block_rows)
        source = f_hbm.at[b, :, piece * 128 : (piece + 1) * 128]
        return pltpu.make_async_copy(source, f_ref.at[piece, rows, :], f_sem.at[b, piece])

    leg_copy = pltpu.make_async_copy(leg_hbm, leg_ref, sem.at[classes])
    tab_copies = [pltpu.make_async_copy(tab_hbm[c], tab_refs[c], sem.at[c]) for c in range(classes)]
    for b in range(members):
        for piece in range(pieces):
            fetch(b, piece).start()
    for copy in tab_copies:
        copy.start()
    leg_copy.start()

    def pack(lat):
        table = leg_ref[lat].astype(F32)
        lane = lax.broadcasted_iota(jnp.int32, (STRIDE, 2 * 128), 1)

        def block(i):
            return table[STRIDE * i : STRIDE * (i + 1), :]

        tiles = [block(0)[:, :128], block(0)[:, 128:]]
        for p in range(1, BLOCKS // 2):
            other = pltpu.roll(block(BLOCKS - p), STRIDE * p, 1)
            packed = jnp.where(lane >= STRIDE * p, block(p), other)
            tiles += [packed[:, :128], packed[:, 128:]]
        tiles.append(block(BLOCKS // 2)[:, 128:])
        for t, tile in enumerate(tiles):
            first = (t // 3) * lat_rows
            t_ref[t % 3, pl.ds(first + lat, LATS, stride=LEG_ROWS), :] = tile

    group = lat_rows // 2
    main = 128 // lev_rows
    rest = members - main
    width = group * members * lev_rows

    def split(b, carry):
        for piece in range(pieces):
            fetch(b, piece).wait()
        for lat in range(lat_rows):
            every = pl.ds(b * block_rows + lat, lev_rows, stride=lat_rows)
            k = lat % group
            inside = jnp.where(b < main, k * 128 + b * lev_rows, group * 128 + (k * rest + b - main) * lev_rows)
            rows = pl.ds(pl.multiple_of(lat // group * width + inside, lev_rows), lev_rows)

            def store(c, piece, u):
                lanes = slice(piece * 128, (piece + 1) * 128)
                high = u.astype(BF16)
                high_refs[c][rows, lanes] = high
                low_refs[c][rows, lanes] = (u - high.astype(F32)).astype(BF16)

            quarter = pieces // 4
            for piece in range(quarter):
                x0, x1, x2, x3 = [f_ref[piece + q * quarter, every, :] for q in range(4)]
                even, odd = x0 + x2, x1 + x3
                store(0, piece, even + odd)
                store(1, piece, even - odd)
                store(2, piece, x0 - x2)
                store(2, piece + quarter, x1 - x3)
        return carry

    lax.fori_loop(0, members, split, 0)
    for copy in tab_copies:
        copy.wait()
    leg_copy.wait()
    waiting = list(range(lat_rows))
    for g in range(2):
        columns = slice(g * width, (g + 1) * width)
        for c, (first, step, fold) in enumerate(CLASSES):
            for k in range(2 if fold == 2 else 1):
                pack(waiting.pop())
            tab, h, l = tab_refs[c][...], high_refs[c][columns], low_refs[c][columns]
            double = tab.shape[0] // 2
            products = dot_nt(tab, h)
            acc = products[:double] + (products[double:] + dot_nt(tab[:double], l))
            count = double // 2
            lane = lax.broadcasted_iota(jnp.int32, (count, 128), 1)
            for k in range(group):
                here = slice(k * 128, (k + 1) * 128)
                tail = slice((group + k // 2) * 128, (group + k // 2 + 1) * 128)
                cos_tail, sin_tail = acc[:count, tail], acc[count:, tail]
                if k % 2 == 0:
                    sin_tail = pltpu.roll(sin_tail, 64, 1)
                else:
                    cos_tail = pltpu.roll(cos_tail, 64, 1)
                middle = jnp.where(lane < 64, cos_tail, sin_tail)
                for t, tile in enumerate((acc[:count, here], middle, acc[count:, here])):
                    tile = tile.astype(BF16)
                    for n in range(count // BLOCKS):
                        start = (first + step * n) * ROWS + (g * group + k) * BLOCKS
                        out_ref[start : start + BLOCKS, t * 128 : (t + 1) * 128] = tile[n * BLOCKS : (n + 1) * BLOCKS]
    for t in range(3):
        for d in range(LATS):
            packed = t_ref[t, d * LEG_ROWS : (d + 1) * LEG_ROWS, :]
            out_ref[d * ROWS + SPEC_ROWS : (d + 1) * ROWS, t * 128 : (t + 1) * 128] = packed.astype(BF16)


def fourier(fields, legendre):
    members, lev_rows, lat_rows, points = fields.shape
    modes = legendre.shape[1]
    columns, pieces = 2 * members * lev_rows, points // 128
    tables = fourier_tables(points, modes)
    splits = [VMEM((lat_rows * members * lev_rows, table.shape[1]), BF16) for table in tables]
    operands = [fields.reshape(members, lev_rows * lat_rows, points), legendre] + [jnp.asarray(t) for t in tables]
    return pl.pallas_call(
        functools.partial(fourier_kernel, members, lev_rows, lat_rows),
        in_specs=[pl.BlockSpec(memory_space=pltpu.HBM)] * len(operands),
        out_specs=pl.BlockSpec(memory_space=VMEM),
        out_shape=jax.ShapeDtypeStruct((LATS * ROWS, columns), BF16),
        scratch_shapes=[
            VMEM((pieces, members * lev_rows * lat_rows, 128), F32),
            VMEM(legendre.shape, BF16),
            *[VMEM(table.shape, BF16) for table in tables],
            *splits,
            *splits,
            VMEM((3, LATS * LEG_ROWS, 128), F32),
            pltpu.SemaphoreType.DMA((members, pieces)),
            pltpu.SemaphoreType.DMA((len(tables) + 1,)),
        ],
        compiler_params=pltpu.CompilerParams(vmem_limit_bytes=40 << 20),
        cost_estimate=pl.CostEstimate(flops=5 * 10**9, bytes_accessed=10**7, transcendentals=0),
        name="fourier",
    )(*[pltpu.with_memory_space_constraint(x, pltpu.HBM) for x in operands])


def place(i, j):
    p = min(j, BLOCKS - 1 - j)
    base = 3 * i if j < BLOCKS // 2 else 3 * (p + 1) + 3 * i
    return [(2 * p + (base + t) // USED_ROWS, (base + t) % USED_ROWS) for t in range(3)]


def legendre_kernel(members, lev_rows, lat_rows, r_ref, out_ref, t_ref, s_ref):
    columns = r_ref.shape[2]
    lats = LATS * lat_rows
    for t in range(3):
        for s in range(LATS):
            rows = slice(s * SPEC_ROWS, (s + 1) * SPEC_ROWS)
            s_ref[t, rows, :] = r_ref[s, :SPEC_ROWS, t * 128 : (t + 1) * 128].astype(F32)

    def rows_of(first, lanes):
        x = r_ref[:, first : first + lat_rows, lanes].astype(F32)
        return x.reshape(lats, -1).astype(BF16)

    def table(t):
        return rows_of(SPEC_ROWS + (t // 3) * lat_rows, slice((t % 3) * 128, (t % 3 + 1) * 128))

    def spectra(i):
        tiles = [s_ref[t, pl.ds(i, lats, stride=BLOCKS), :] for t in range(3)]
        return jnp.concatenate(tiles, axis=1).astype(BF16)

    row = lax.broadcasted_iota(jnp.int32, (columns, columns), 0)
    col = lax.broadcasted_iota(jnp.int32, (columns, columns), 1)
    half = members * lev_rows
    same = ((row >= half) == (col >= half)) & (row % lev_rows == col % lev_rows)
    ones = jnp.where(same, 1.0, 0.0).astype(BF16)

    zero = jnp.zeros((LATS, 128), F32)
    for k in range(2 * BLOCKS // 2):
        for r in range(USED_ROWS - (k % 2), SLOT_ROWS):
            t_ref[pl.ds(k * LATS * SLOT_ROWS + r, LATS, stride=SLOT_ROWS), :] = zero

    def finish(waves, units):
        high = waves.astype(BF16)
        low = (waves - high.astype(F32)).astype(BF16)
        total = dot_nn(high, ones) + dot_nn(low, ones)
        anomaly = waves - total * (1.0 / members)
        for u, (i, j) in enumerate(units):
            for t, (k, r) in enumerate(place(i, j)):
                t_ref[pl.ds(k * LATS * SLOT_ROWS + r, LATS, stride=SLOT_ROWS), :] = anomaly[
                    u * STRIDE : (u + 1) * STRIDE, t * 128 : (t + 1) * 128
                ]

    for p in range(BLOCKS // 2):
        first, second = table(2 * p), table(2 * p + 1)
        mine = spectra(p)
        lower, upper = dot_tn(first, mine), dot_tn(second, mine)
        units = [(p, j) for j in range(p, BLOCKS)]
        if p:
            other = dot_tn(first, spectra(BLOCKS - p))
            lower = jnp.concatenate([other[: STRIDE * p], lower[STRIDE * p :]], axis=0)
            units = [(BLOCKS - p, BLOCKS - p + g) for g in range(p)] + units
        finish(lower, units[:4])
        finish(upper, units[4:])
    p = BLOCKS // 2
    finish(dot_tn(table(2 * p), spectra(p)), [(p, j) for j in range(p, BLOCKS)])
    step = LATS * SLOT_ROWS
    for k in range(LEVS):
        out_ref[k * step : (k + 1) * step, :] = t_ref[k * step : (k + 1) * step, :].astype(BF16)


def legendre_stage(received, members, lev_rows, lat_rows):
    rows = LATS * LEVS * SLOT_ROWS
    return pl.pallas_call(
        functools.partial(legendre_kernel, members, lev_rows, lat_rows),
        in_specs=[pl.BlockSpec(memory_space=VMEM)],
        out_specs=pl.BlockSpec(memory_space=VMEM),
        out_shape=jax.ShapeDtypeStruct((rows, 128), BF16),
        scratch_shapes=[VMEM((rows, 128), F32), VMEM((3, LATS * SPEC_ROWS, 128), F32)],
        compiler_params=pltpu.CompilerParams(vmem_limit_bytes=40 << 20),
        cost_estimate=pl.CostEstimate(flops=2 * 10**9, bytes_accessed=4 * 10**6, transcendentals=0),
        name="legendre",
    )(received)


def home(lev):
    p, h = lev // 2, lev % 2
    return p, h


def covariance_kernel(members, lev_rows, y_ref, out_ref):
    levels = LEVS * lev_rows
    count = LATS * SLOT_ROWS
    lev, lat = lax.axis_index("lev"), lax.axis_index("lat")
    p, h = home(lev)
    parts = [y_ref[v * count : (v + 1) * count, :] for v in range(LEVS)]
    lane = lax.broadcasted_iota(jnp.int32, (count, 128), 1)
    for bit in (1, 2, 4):
        shift = bit * lev_rows
        low = (lane // shift) % 2 == 0
        swapped = list(parts)
        for v in range(LEVS):
            if v & bit:
                continue
            a, b = parts[v], parts[v | bit]
            swapped[v] = jnp.where(low, a, pltpu.roll(b, shift, 1))
            swapped[v | bit] = jnp.where(low, pltpu.roll(a, 128 - shift, 1), b)
        parts = swapped
    first_rows = jnp.where(h == 0, 3 * (p + 1), 0)
    slot = lax.broadcasted_iota(jnp.int32, (levels, count), 1) % SLOT_ROWS
    is_first = slot < first_rows
    one = jnp.zeros((levels, levels), F32)
    two = jnp.zeros((levels, levels), F32)
    for part in parts:
        turned = part.astype(F32).T
        zero = jnp.zeros_like(turned)
        one += dot_nn(jnp.where(is_first, turned, zero).astype(BF16), part)
        two += dot_nn(jnp.where(is_first, zero, turned).astype(BF16), part)
    for s, (total, n) in enumerate(((one, lat + STRIDE * p), (two, lat + STRIDE * (BLOCKS - 1 - p)))):
        divisor = ((members - 1) * (2 * n + 2)).astype(F32)
        scaled = (total / jnp.full((levels, levels), divisor, F32)).astype(BF16)
        for v in range(LEVS):
            out_ref[v, s * lev_rows : (s + 1) * lev_rows, :] = scaled[v * lev_rows : (v + 1) * lev_rows]


def covariance_stage(received, members, lev_rows):
    return pl.pallas_call(
        functools.partial(covariance_kernel, members, lev_rows),
        in_specs=[pl.BlockSpec(memory_space=VMEM)],
        out_specs=pl.BlockSpec(memory_space=VMEM),
        out_shape=jax.ShapeDtypeStruct((LEVS, 2 * lev_rows, 128), BF16),
        compiler_params=pltpu.CompilerParams(vmem_limit_bytes=40 << 20),
        cost_estimate=pl.CostEstimate(flops=10**9, bytes_accessed=2 * 10**6, transcendentals=0),
        name="covariance",
    )(received)


def route_kernel(lev_rows, counts_ref, g_ref, out_ref, f_ref):
    lat = lax.axis_index("lat")
    half = BLOCKS // 2
    for j in range(BLOCKS):
        p, s = min(j, BLOCKS - 1 - j), int(j >= half)
        rows = slice(s * lev_rows, (s + 1) * lev_rows)
        f_ref[j] = (g_ref[2 * p, rows, :].astype(F32) + g_ref[2 * p + 1, rows, :].astype(F32)).astype(BF16)

    def step(owner, start):
        j = jnp.maximum(start - lat + (STRIDE - 1), 0) // STRIDE
        out_ref[owner] = f_ref[jnp.minimum(j, BLOCKS - 1)]
        return start + counts_ref[owner]

    lax.fori_loop(0, LATS, step, jnp.int32(0))


def route_stage(parts, owner_counts, lev_rows):
    return pl.pallas_call(
        functools.partial(route_kernel, lev_rows),
        in_specs=[pl.BlockSpec(memory_space=pltpu.SMEM), pl.BlockSpec(memory_space=VMEM)],
        out_specs=pl.BlockSpec(memory_space=VMEM),
        out_shape=jax.ShapeDtypeStruct((LATS, lev_rows, 128), BF16),
        scratch_shapes=[VMEM((BLOCKS, lev_rows, 128), BF16)],
        compiler_params=pltpu.CompilerParams(vmem_limit_bytes=8 << 20),
        name="route",
    )(owner_counts, parts)


def collect_kernel(counts_ref, r_ref, out_ref):
    lat = lax.axis_index("lat")
    start = lax.fori_loop(0, lat, lambda k, s: s + counts_ref[k], jnp.int32(0))
    count = counts_ref[lat]
    for slot in range(out_ref.shape[0]):
        block = r_ref[(start + slot) % STRIDE].astype(F32)
        out_ref[slot] = jnp.where(slot < count, block, jnp.zeros_like(block))


def collect_stage(routed, owner_counts, capacity, lev_rows):
    return pl.pallas_call(
        collect_kernel,
        in_specs=[pl.BlockSpec(memory_space=pltpu.SMEM), pl.BlockSpec(memory_space=VMEM)],
        out_specs=pl.BlockSpec(memory_space=VMEM),
        out_shape=jax.ShapeDtypeStruct((capacity, lev_rows, 128), F32),
        compiler_params=pltpu.CompilerParams(vmem_limit_bytes=8 << 20),
        name="collect",
    )(owner_counts, routed)


def exchange(x, axis):
    return lax.all_to_all(x, axis, split_axis=0, concat_axis=0, tiled=True)


def on_device(fields, legendre, owner_counts):
    members, lev_rows, lat_rows, _ = fields.shape
    modes = legendre.shape[1]
    capacity = 2 * modes // owner_counts.shape[0]
    first = fourier(fields, legendre)
    first = exchange(first.reshape(LATS, ROWS, -1), "lat")
    second = legendre_stage(first, members, lev_rows, lat_rows)
    second = exchange(second.reshape(LATS * LEVS, SLOT_ROWS // 2, 2, 128), ("lev", "lat"))
    third = covariance_stage(second.reshape(-1, 128), members, lev_rows)
    third = exchange(third, "lev")
    fourth = route_stage(third, owner_counts, lev_rows)
    fourth = exchange(fourth, "lat")
    return collect_stage(fourth, owner_counts, capacity, lev_rows)


def solution(mesh):
    return jax.shard_map(
        on_device,
        mesh=mesh,
        in_specs=(P(None, "lev", "lat", None), P("lat", None, None), P()),
        out_specs=P("lat", "lev", None),
        check_vma=False,
    )
```

```python
import functools
import math

import jax
import jax.numpy as jnp
import ml_dtypes
import numpy as np
from jax import lax
from jax.experimental import pallas as pl
from jax.experimental.pallas import tpu as pltpu
from jax.sharding import PartitionSpec as P

F32, BF16 = jnp.float32, jnp.bfloat16
LATS, LEVS = 32, 8
STRIDE = 32
BLOCKS = 8
SPEC_ROWS, LEG_ROWS = 64, 24
ROWS = SPEC_ROWS + LEG_ROWS
SLOT_ROWS, USED_ROWS = 14, 14
CLASSES = ((0, 4, 4), (2, 4, 4), (1, 2, 2))
VMEM = pltpu.VMEM


def fourier_tables(points, modes):
    tables = []
    for first, step, fold in CLASSES:
        j = np.arange(points // fold)
        m = (np.arange(first, LATS, step)[:, None] + STRIDE * np.arange(BLOCKS)[None, :]).reshape(-1)
        angle = (m[:, None] * j[None, :] % points) * (2.0 * math.pi / points)
        table = np.concatenate([np.cos(angle), -np.sin(angle)]) * points**-0.5
        high = table.astype(np.float32).astype(ml_dtypes.bfloat16)
        low = (table - high.astype(np.float64)).astype(np.float32).astype(ml_dtypes.bfloat16)
        tables.append(np.concatenate([high, low]))
    return tables


def dot_nt(a, b):
    return lax.dot_general(a, b, (((1,), (1,)), ((), ())), preferred_element_type=F32)


def dot_tn(a, b):
    return lax.dot_general(a, b, (((0,), (0,)), ((), ())), preferred_element_type=F32)


def dot_nn(a, b):
    return lax.dot_general(a, b, (((1,), (0,)), ((), ())), preferred_element_type=F32)


def fourier_kernel(members, lev_rows, lat_rows, f_hbm, leg_hbm, *refs):
    classes = len(CLASSES)
    tab_hbm, (out_ref, f_ref, leg_ref), refs = refs[:classes], refs[classes : classes + 3], refs[classes + 3 :]
    tab_refs, high_refs, low_refs = refs[:classes], refs[classes : 2 * classes], refs[2 * classes : 3 * classes]
    t_ref, f_sem, sem = refs[3 * classes :]
    pieces = f_ref.shape[0]
    block_rows = lev_rows * lat_rows

    def fetch(b, piece):
        rows = pl.ds(pl.multiple_of(b * block_rows, block_rows), block_rows)
        source = f_hbm.at[b, :, piece * 128 : (piece + 1) * 128]
        return pltpu.make_async_copy(source, f_ref.at[piece, rows, :], f_sem.at[b, piece])

    leg_copy = pltpu.make_async_copy(leg_hbm, leg_ref, sem.at[classes])
    tab_copies = [pltpu.make_async_copy(tab_hbm[c], tab_refs[c], sem.at[c]) for c in range(classes)]
    for b in range(members):
        for piece in range(pieces):
            fetch(b, piece).start()
    for copy in tab_copies:
        copy.start()
    leg_copy.start()

    def pack(lat):
        table = leg_ref[lat].astype(F32)
        lane = lax.broadcasted_iota(jnp.int32, (STRIDE, 2 * 128), 1)

        def block(i):
            return table[STRIDE * i : STRIDE * (i + 1), :]

        tiles = [block(0)[:, :128], block(0)[:, 128:]]
        for p in range(1, BLOCKS // 2):
            other = pltpu.roll(block(BLOCKS - p), STRIDE * p, 1)
            packed = jnp.where(lane >= STRIDE * p, block(p), other)
            tiles += [packed[:, :128], packed[:, 128:]]
        tiles.append(block(BLOCKS // 2)[:, 128:])
        for t, tile in enumerate(tiles):
            first = (t // 3) * lat_rows
            t_ref[t % 3, pl.ds(first + lat, LATS, stride=LEG_ROWS), :] = tile

    group = lat_rows // 2
    main = 128 // lev_rows
    rest = members - main
    width = group * members * lev_rows

    def split(b, carry):
        for piece in range(pieces):
            fetch(b, piece).wait()
        for lat in range(lat_rows):
            every = pl.ds(b * block_rows + lat, lev_rows, stride=lat_rows)
            k = lat % group
            inside = jnp.where(b < main, k * 128 + b * lev_rows, group * 128 + (k * rest + b - main) * lev_rows)
            rows = pl.ds(pl.multiple_of(lat // group * width + inside, lev_rows), lev_rows)

            def store(c, piece, u):
                lanes = slice(piece * 128, (piece + 1) * 128)
                high = u.astype(BF16)
                high_refs[c][rows, lanes] = high
                low_refs[c][rows, lanes] = (u - high.astype(F32)).astype(BF16)

            quarter = pieces // 4
            for piece in range(quarter):
                x0, x1, x2, x3 = [f_ref[piece + q * quarter, every, :] for q in range(4)]
                even, odd = x0 + x2, x1 + x3
                store(0, piece, even + odd)
                store(1, piece, even - odd)
                store(2, piece, x0 - x2)
                store(2, piece + quarter, x1 - x3)
        return carry

    lax.fori_loop(0, members, split, 0)
    for copy in tab_copies:
        copy.wait()
    leg_copy.wait()
    waiting = list(range(lat_rows))
    for g in range(2):
        columns = slice(g * width, (g + 1) * width)
        for c, (first, step, fold) in enumerate(CLASSES):
            for k in range(2 if fold == 2 else 1):
                pack(waiting.pop())
            tab, h, l = tab_refs[c][...], high_refs[c][columns], low_refs[c][columns]
            double = tab.shape[0] // 2
            products = dot_nt(tab, h)
            acc = products[:double] + (products[double:] + dot_nt(tab[:double], l))
            count = double // 2
            lane = lax.broadcasted_iota(jnp.int32, (count, 128), 1)
            for k in range(group):
                here = slice(k * 128, (k + 1) * 128)
                tail = slice((group + k // 2) * 128, (group + k // 2 + 1) * 128)
                cos_tail, sin_tail = acc[:count, tail], acc[count:, tail]
                if k % 2 == 0:
                    sin_tail = pltpu.roll(sin_tail, 64, 1)
                else:
                    cos_tail = pltpu.roll(cos_tail, 64, 1)
                middle = jnp.where(lane < 64, cos_tail, sin_tail)
                for t, tile in enumerate((acc[:count, here], middle, acc[count:, here])):
                    tile = tile.astype(BF16)
                    for n in range(count // BLOCKS):
                        start = (first + step * n) * ROWS + (g * group + k) * BLOCKS
                        out_ref[start : start + BLOCKS, t * 128 : (t + 1) * 128] = tile[n * BLOCKS : (n + 1) * BLOCKS]
    for t in range(3):
        for d in range(LATS):
            packed = t_ref[t, d * LEG_ROWS : (d + 1) * LEG_ROWS, :]
            out_ref[d * ROWS + SPEC_ROWS : (d + 1) * ROWS, t * 128 : (t + 1) * 128] = packed.astype(BF16)


def fourier(fields, legendre):
    members, lev_rows, lat_rows, points = fields.shape
    modes = legendre.shape[1]
    columns, pieces = 2 * members * lev_rows, points // 128
    tables = fourier_tables(points, modes)
    splits = [VMEM((lat_rows * members * lev_rows, table.shape[1]), BF16) for table in tables]
    operands = [fields.reshape(members, lev_rows * lat_rows, points), legendre] + [jnp.asarray(t) for t in tables]
    return pl.pallas_call(
        functools.partial(fourier_kernel, members, lev_rows, lat_rows),
        in_specs=[pl.BlockSpec(memory_space=pltpu.HBM)] * len(operands),
        out_specs=pl.BlockSpec(memory_space=VMEM),
        out_shape=jax.ShapeDtypeStruct((LATS * ROWS, columns), BF16),
        scratch_shapes=[
            VMEM((pieces, members * lev_rows * lat_rows, 128), F32),
            VMEM(legendre.shape, BF16),
            *[VMEM(table.shape, BF16) for table in tables],
            *splits,
            *splits,
            VMEM((3, LATS * LEG_ROWS, 128), F32),
            pltpu.SemaphoreType.DMA((members, pieces)),
            pltpu.SemaphoreType.DMA((len(tables) + 1,)),
        ],
        compiler_params=pltpu.CompilerParams(vmem_limit_bytes=40 << 20),
        cost_estimate=pl.CostEstimate(flops=5 * 10**9, bytes_accessed=10**7, transcendentals=0),
        name="fourier",
    )(*[pltpu.with_memory_space_constraint(x, pltpu.HBM) for x in operands])


def place(i, j):
    p = min(j, BLOCKS - 1 - j)
    base = 3 * i if j < BLOCKS // 2 else 3 * (p + 1) + 3 * i
    return [(2 * p + (base + t) // USED_ROWS, (base + t) % USED_ROWS) for t in range(3)]


def legendre_kernel(members, lev_rows, lat_rows, r_ref, out_ref, t_ref, s_ref):
    columns = r_ref.shape[2]
    lats = LATS * lat_rows
    for t in range(3):
        for s in range(LATS):
            rows = slice(s * SPEC_ROWS, (s + 1) * SPEC_ROWS)
            s_ref[t, rows, :] = r_ref[s, :SPEC_ROWS, t * 128 : (t + 1) * 128].astype(F32)

    def rows_of(first, lanes):
        x = r_ref[:, first : first + lat_rows, lanes].astype(F32)
        return x.reshape(lats, -1).astype(BF16)

    def table(t):
        return rows_of(SPEC_ROWS + (t // 3) * lat_rows, slice((t % 3) * 128, (t % 3 + 1) * 128))

    def spectra(i):
        tiles = [s_ref[t, pl.ds(i, lats, stride=BLOCKS), :] for t in range(3)]
        return jnp.concatenate(tiles, axis=1).astype(BF16)

    row = lax.broadcasted_iota(jnp.int32, (256, 256), 0)
    col = lax.broadcasted_iota(jnp.int32, (256, 256), 1)
    same = ((row >= 128) == (col >= 128)) & (row % lev_rows == col % lev_rows)
    ones = jnp.where(same, 1.0, 0.0).astype(BF16)

    zero = jnp.zeros((LATS, 128), F32)
    for k in range(2 * BLOCKS // 2):
        for r in range(USED_ROWS - (k % 2), SLOT_ROWS):
            t_ref[pl.ds(k * LATS * SLOT_ROWS + r, LATS, stride=SLOT_ROWS), :] = zero

    def finish(waves, units):
        tiles = [waves[:, t * 128 : (t + 1) * 128] for t in range(3)]
        lane = lax.broadcasted_iota(jnp.int32, tiles[1].shape, 1)
        zeros = jnp.zeros_like(tiles[1])
        folded = jnp.concatenate(
            [tiles[0] + jnp.where(lane < 64, tiles[1], zeros), tiles[2] + jnp.where(lane < 64, zeros, tiles[1])], axis=1
        )
        high = folded.astype(BF16)
        low = (folded - high.astype(F32)).astype(BF16)
        mean = (dot_nn(high, ones) + dot_nn(low, ones)) * (1.0 / members)
        middle = jnp.where(lane < 64, mean[:, :128], mean[:, 128:])
        anomaly = waves - jnp.concatenate([mean[:, :128], middle, mean[:, 128:]], axis=1)
        for u, (i, j) in enumerate(units):
            for t, (k, r) in enumerate(place(i, j)):
                t_ref[pl.ds(k * LATS * SLOT_ROWS + r, LATS, stride=SLOT_ROWS), :] = anomaly[
                    u * STRIDE : (u + 1) * STRIDE, t * 128 : (t + 1) * 128
                ]

    for p in range(BLOCKS // 2):
        first, second = table(2 * p), table(2 * p + 1)
        mine = spectra(p)
        lower, upper = dot_tn(first, mine), dot_tn(second, mine)
        units = [(p, j) for j in range(p, BLOCKS)]
        if p:
            other = dot_tn(first, spectra(BLOCKS - p))
            lower = jnp.concatenate([other[: STRIDE * p], lower[STRIDE * p :]], axis=0)
            units = [(BLOCKS - p, BLOCKS - p + g) for g in range(p)] + units
        finish(lower, units[:4])
        finish(upper, units[4:])
    p = BLOCKS // 2
    finish(dot_tn(table(2 * p), spectra(p)), [(p, j) for j in range(p, BLOCKS)])
    step = LATS * SLOT_ROWS
    for k in range(LEVS):
        out_ref[k * step : (k + 1) * step, :] = t_ref[k * step : (k + 1) * step, :].astype(BF16)


def legendre_stage(received, members, lev_rows, lat_rows):
    rows = LATS * LEVS * SLOT_ROWS
    return pl.pallas_call(
        functools.partial(legendre_kernel, members, lev_rows, lat_rows),
        in_specs=[pl.BlockSpec(memory_space=VMEM)],
        out_specs=pl.BlockSpec(memory_space=VMEM),
        out_shape=jax.ShapeDtypeStruct((rows, 128), BF16),
        scratch_shapes=[VMEM((rows, 128), F32), VMEM((3, LATS * SPEC_ROWS, 128), F32)],
        compiler_params=pltpu.CompilerParams(vmem_limit_bytes=40 << 20),
        cost_estimate=pl.CostEstimate(flops=2 * 10**9, bytes_accessed=4 * 10**6, transcendentals=0),
        name="legendre",
    )(received)


def home(lev):
    p, h = lev // 2, lev % 2
    return p, h


def covariance_kernel(members, lev_rows, y_ref, out_ref):
    levels = LEVS * lev_rows
    count = LATS * SLOT_ROWS
    lev, lat = lax.axis_index("lev"), lax.axis_index("lat")
    p, h = home(lev)
    parts = [y_ref[v * count : (v + 1) * count, :] for v in range(LEVS)]
    lane = lax.broadcasted_iota(jnp.int32, (count, 128), 1)
    for bit in (1, 2, 4):
        shift = bit * lev_rows
        low = (lane // shift) % 2 == 0
        swapped = list(parts)
        for v in range(LEVS):
            if v & bit:
                continue
            a, b = parts[v], parts[v | bit]
            swapped[v] = jnp.where(low, a, pltpu.roll(b, shift, 1))
            swapped[v | bit] = jnp.where(low, pltpu.roll(a, 128 - shift, 1), b)
        parts = swapped
    first_rows = jnp.where(h == 0, 3 * (p + 1), 0)
    slot = lax.broadcasted_iota(jnp.int32, (levels, count), 1) % SLOT_ROWS
    is_first = slot < first_rows
    one = jnp.zeros((levels, levels), F32)
    two = jnp.zeros((levels, levels), F32)
    for part in parts:
        turned = part.astype(F32).T
        zero = jnp.zeros_like(turned)
        one += dot_nn(jnp.where(is_first, turned, zero).astype(BF16), part)
        two += dot_nn(jnp.where(is_first, zero, turned).astype(BF16), part)
    for s, (total, n) in enumerate(((one, lat + STRIDE * p), (two, lat + STRIDE * (BLOCKS - 1 - p)))):
        divisor = ((members - 1) * (2 * n + 2)).astype(F32)
        scaled = (total / jnp.full((levels, levels), divisor, F32)).astype(BF16)
        for v in range(LEVS):
            out_ref[v, s * lev_rows : (s + 1) * lev_rows, :] = scaled[v * lev_rows : (v + 1) * lev_rows]


def covariance_stage(received, members, lev_rows):
    return pl.pallas_call(
        functools.partial(covariance_kernel, members, lev_rows),
        in_specs=[pl.BlockSpec(memory_space=VMEM)],
        out_specs=pl.BlockSpec(memory_space=VMEM),
        out_shape=jax.ShapeDtypeStruct((LEVS, 2 * lev_rows, 128), BF16),
        compiler_params=pltpu.CompilerParams(vmem_limit_bytes=40 << 20),
        cost_estimate=pl.CostEstimate(flops=10**9, bytes_accessed=2 * 10**6, transcendentals=0),
        name="covariance",
    )(received)


def route_kernel(lev_rows, counts_ref, g_ref, out_ref, f_ref):
    lat = lax.axis_index("lat")
    half = BLOCKS // 2
    for j in range(BLOCKS):
        p, s = min(j, BLOCKS - 1 - j), int(j >= half)
        rows = slice(s * lev_rows, (s + 1) * lev_rows)
        f_ref[j] = (g_ref[2 * p, rows, :].astype(F32) + g_ref[2 * p + 1, rows, :].astype(F32)).astype(BF16)

    def step(owner, start):
        j = jnp.maximum(start - lat + (STRIDE - 1), 0) // STRIDE
        out_ref[owner] = f_ref[jnp.minimum(j, BLOCKS - 1)]
        return start + counts_ref[owner]

    lax.fori_loop(0, LATS, step, jnp.int32(0))


def route_stage(parts, owner_counts, lev_rows):
    return pl.pallas_call(
        functools.partial(route_kernel, lev_rows),
        in_specs=[pl.BlockSpec(memory_space=pltpu.SMEM), pl.BlockSpec(memory_space=VMEM)],
        out_specs=pl.BlockSpec(memory_space=VMEM),
        out_shape=jax.ShapeDtypeStruct((LATS, lev_rows, 128), BF16),
        scratch_shapes=[VMEM((BLOCKS, lev_rows, 128), BF16)],
        compiler_params=pltpu.CompilerParams(vmem_limit_bytes=8 << 20),
        name="route",
    )(owner_counts, parts)


def collect_kernel(counts_ref, r_ref, out_ref):
    lat = lax.axis_index("lat")
    start = lax.fori_loop(0, lat, lambda k, s: s + counts_ref[k], jnp.int32(0))
    count = counts_ref[lat]
    for slot in range(out_ref.shape[0]):
        block = r_ref[(start + slot) % STRIDE].astype(F32)
        out_ref[slot] = jnp.where(slot < count, block, jnp.zeros_like(block))


def collect_stage(routed, owner_counts, capacity, lev_rows):
    return pl.pallas_call(
        collect_kernel,
        in_specs=[pl.BlockSpec(memory_space=pltpu.SMEM), pl.BlockSpec(memory_space=VMEM)],
        out_specs=pl.BlockSpec(memory_space=VMEM),
        out_shape=jax.ShapeDtypeStruct((capacity, lev_rows, 128), F32),
        compiler_params=pltpu.CompilerParams(vmem_limit_bytes=8 << 20),
        name="collect",
    )(owner_counts, routed)


def exchange(x, axis):
    return lax.all_to_all(x, axis, split_axis=0, concat_axis=0, tiled=True)


def on_device(fields, legendre, owner_counts):
    members, lev_rows, lat_rows, _ = fields.shape
    modes = legendre.shape[1]
    capacity = 2 * modes // owner_counts.shape[0]
    first = fourier(fields, legendre)
    first = exchange(first.reshape(LATS, ROWS, -1), "lat")
    second = legendre_stage(first, members, lev_rows, lat_rows)
    second = exchange(second.reshape(LATS * LEVS, SLOT_ROWS // 2, 2, 128), ("lev", "lat"))
    third = covariance_stage(second.reshape(-1, 128), members, lev_rows)
    third = exchange(third, "lev")
    fourth = route_stage(third, owner_counts, lev_rows)
    fourth = exchange(fourth, "lat")
    return collect_stage(fourth, owner_counts, capacity, lev_rows)


def solution(mesh):
    return jax.shard_map(
        on_device,
        mesh=mesh,
        in_specs=(P(None, "lev", "lat", None), P("lat", None, None), P()),
        out_specs=P("lat", "lev", None),
        check_vma=False,
    )
```

```python
import functools
import math

import jax
import jax.numpy as jnp
import ml_dtypes
import numpy as np
from jax import lax
from jax.experimental import pallas as pl
from jax.experimental.pallas import tpu as pltpu
from jax.sharding import PartitionSpec as P

F32, BF16 = jnp.float32, jnp.bfloat16
LATS, LEVS = 32, 8
STRIDE = 32
BLOCKS = 8
SPEC_ROWS, LEG_ROWS = 64, 24
ROWS = SPEC_ROWS + LEG_ROWS
SLOT_ROWS, USED_ROWS = 14, 14
CLASSES = ((0, 4, 4), (2, 4, 4), (1, 2, 2))
VMEM = pltpu.VMEM


def fourier_tables(points, modes):
    tables = []
    for first, step, fold in CLASSES:
        j = np.arange(points // fold)
        m = (np.arange(first, LATS, step)[:, None] + STRIDE * np.arange(BLOCKS)[None, :]).reshape(-1)
        angle = (m[:, None] * j[None, :] % points) * (2.0 * math.pi / points)
        table = np.concatenate([np.cos(angle), -np.sin(angle)]) * points**-0.5
        high = table.astype(np.float32).astype(ml_dtypes.bfloat16)
        low = (table - high.astype(np.float64)).astype(np.float32).astype(ml_dtypes.bfloat16)
        tables.append(np.concatenate([high, low]))
    return tables


def dot_nt(a, b):
    return lax.dot_general(a, b, (((1,), (1,)), ((), ())), preferred_element_type=F32)


def dot_tn(a, b):
    return lax.dot_general(a, b, (((0,), (0,)), ((), ())), preferred_element_type=F32)


def dot_nn(a, b):
    return lax.dot_general(a, b, (((1,), (0,)), ((), ())), preferred_element_type=F32)


def fourier_kernel(members, lev_rows, lat_rows, f_hbm, *refs):
    classes = len(CLASSES)
    tab_hbm, (out_ref, f_ref), refs = refs[:classes], refs[classes : classes + 2], refs[classes + 2 :]
    tab_refs, high_refs, low_refs = refs[:classes], refs[classes : 2 * classes], refs[2 * classes : 3 * classes]
    f_sem, sem = refs[3 * classes :]
    pieces = f_ref.shape[0]
    block_rows = lev_rows * lat_rows

    def fetch(b, piece):
        rows = pl.ds(pl.multiple_of(b * block_rows, block_rows), block_rows)
        source = f_hbm.at[b, :, piece * 128 : (piece + 1) * 128]
        return pltpu.make_async_copy(source, f_ref.at[piece, rows, :], f_sem.at[b, piece])

    tab_copies = [pltpu.make_async_copy(tab_hbm[c], tab_refs[c], sem.at[c]) for c in range(classes)]
    for b in range(members):
        for piece in range(pieces):
            fetch(b, piece).start()
    for copy in tab_copies:
        copy.start()

    group = lat_rows // 2
    main = 128 // lev_rows
    rest = members - main
    width = group * members * lev_rows

    def split(b, carry):
        for piece in range(pieces):
            fetch(b, piece).wait()
        for lat in range(lat_rows):
            every = pl.ds(b * block_rows + lat, lev_rows, stride=lat_rows)
            k = lat % group
            inside = jnp.where(b < main, k * 128 + b * lev_rows, group * 128 + (k * rest + b - main) * lev_rows)
            rows = pl.ds(pl.multiple_of(lat // group * width + inside, lev_rows), lev_rows)

            def store(c, piece, u):
                lanes = slice(piece * 128, (piece + 1) * 128)
                high = u.astype(BF16)
                high_refs[c][rows, lanes] = high
                low_refs[c][rows, lanes] = (u - high.astype(F32)).astype(BF16)

            quarter = pieces // 4
            for piece in range(quarter):
                x0, x1, x2, x3 = [f_ref[piece + q * quarter, every, :] for q in range(4)]
                even, odd = x0 + x2, x1 + x3
                store(0, piece, even + odd)
                store(1, piece, even - odd)
                store(2, piece, x0 - x2)
                store(2, piece + quarter, x1 - x3)
        return carry

    lax.fori_loop(0, members, split, 0)
    for copy in tab_copies:
        copy.wait()
    for g in range(2):
        columns = slice(g * width, (g + 1) * width)
        for c, (first, step, fold) in enumerate(CLASSES):
            tab, h, l = tab_refs[c][...], high_refs[c][columns], low_refs[c][columns]
            double = tab.shape[0] // 2
            products = dot_nt(tab, h)
            acc = products[:double] + (products[double:] + dot_nt(tab[:double], l))
            count = double // 2
            lane = lax.broadcasted_iota(jnp.int32, (count, 128), 1)
            for k in range(group):
                here = slice(k * 128, (k + 1) * 128)
                tail = slice((group + k // 2) * 128, (group + k // 2 + 1) * 128)
                cos_tail, sin_tail = acc[:count, tail], acc[count:, tail]
                if k % 2 == 0:
                    sin_tail = pltpu.roll(sin_tail, 64, 1)
                else:
                    cos_tail = pltpu.roll(cos_tail, 64, 1)
                middle = jnp.where(lane < 64, cos_tail, sin_tail)
                for t, tile in enumerate((acc[:count, here], middle, acc[count:, here])):
                    tile = tile.astype(BF16)
                    for n in range(count // BLOCKS):
                        start = (first + step * n) * SPEC_ROWS + (g * group + k) * BLOCKS
                        out_ref[start : start + BLOCKS, t * 128 : (t + 1) * 128] = tile[n * BLOCKS : (n + 1) * BLOCKS]


def pack_kernel(lat_rows, leg_ref, out_ref, t_ref):
    def pack(lat):
        table = leg_ref[lat].astype(F32)
        lane = lax.broadcasted_iota(jnp.int32, (STRIDE, 2 * 128), 1)

        def block(i):
            return table[STRIDE * i : STRIDE * (i + 1), :]

        tiles = [block(0)[:, :128], block(0)[:, 128:]]
        for p in range(1, BLOCKS // 2):
            other = pltpu.roll(block(BLOCKS - p), STRIDE * p, 1)
            packed = jnp.where(lane >= STRIDE * p, block(p), other)
            tiles += [packed[:, :128], packed[:, 128:]]
        tiles.append(block(BLOCKS // 2)[:, 128:])
        for t, tile in enumerate(tiles):
            first = (t // 3) * lat_rows
            t_ref[t % 3, pl.ds(first + lat, LATS, stride=LEG_ROWS), :] = tile

    for lat in range(lat_rows):
        pack(lat)
    for t in range(3):
        for d in range(LATS):
            packed = t_ref[t, d * LEG_ROWS : (d + 1) * LEG_ROWS, :]
            out_ref[d * LEG_ROWS : (d + 1) * LEG_ROWS, t * 128 : (t + 1) * 128] = packed.astype(BF16)


def pack_stage(legendre):
    return pl.pallas_call(
        functools.partial(pack_kernel, legendre.shape[0]),
        in_specs=[pl.BlockSpec(memory_space=VMEM)],
        out_specs=pl.BlockSpec(memory_space=VMEM),
        out_shape=jax.ShapeDtypeStruct((LATS * LEG_ROWS, 3 * 128), BF16),
        scratch_shapes=[VMEM((3, LATS * LEG_ROWS, 128), F32)],
        compiler_params=pltpu.CompilerParams(vmem_limit_bytes=40 << 20),
        cost_estimate=pl.CostEstimate(flops=10**8, bytes_accessed=2 * 10**6, transcendentals=0),
        name="pack",
    )(legendre)


def fourier(fields):
    members, lev_rows, lat_rows, points = fields.shape
    modes = LATS * BLOCKS
    columns, pieces = 2 * members * lev_rows, points // 128
    tables = fourier_tables(points, modes)
    splits = [VMEM((lat_rows * members * lev_rows, table.shape[1]), BF16) for table in tables]
    operands = [fields.reshape(members, lev_rows * lat_rows, points)] + [jnp.asarray(t) for t in tables]
    return pl.pallas_call(
        functools.partial(fourier_kernel, members, lev_rows, lat_rows),
        in_specs=[pl.BlockSpec(memory_space=pltpu.HBM)] * len(operands),
        out_specs=pl.BlockSpec(memory_space=VMEM),
        out_shape=jax.ShapeDtypeStruct((LATS * SPEC_ROWS, columns), BF16),
        scratch_shapes=[
            VMEM((pieces, members * lev_rows * lat_rows, 128), F32),
            *[VMEM(table.shape, BF16) for table in tables],
            *splits,
            *splits,
            pltpu.SemaphoreType.DMA((members, pieces)),
            pltpu.SemaphoreType.DMA((len(tables),)),
        ],
        compiler_params=pltpu.CompilerParams(vmem_limit_bytes=40 << 20),
        cost_estimate=pl.CostEstimate(flops=5 * 10**9, bytes_accessed=10**7, transcendentals=0),
        name="fourier",
    )(*[pltpu.with_memory_space_constraint(x, pltpu.HBM) for x in operands])


def place(i, j):
    p = min(j, BLOCKS - 1 - j)
    base = 3 * i if j < BLOCKS // 2 else 3 * (p + 1) + 3 * i
    return [(2 * p + (base + t) // USED_ROWS, (base + t) % USED_ROWS) for t in range(3)]


def legendre_kernel(members, lev_rows, lat_rows, r_ref, leg_ref, out_ref, t_ref, s_ref):
    columns = r_ref.shape[2]
    lats = LATS * lat_rows
    for t in range(3):
        for s in range(LATS):
            rows = slice(s * SPEC_ROWS, (s + 1) * SPEC_ROWS)
            s_ref[t, rows, :] = r_ref[s, :, t * 128 : (t + 1) * 128].astype(F32)

    def rows_of(first, lanes):
        x = leg_ref[:, first : first + lat_rows, lanes].astype(F32)
        return x.reshape(lats, -1).astype(BF16)

    def table(t):
        return rows_of((t // 3) * lat_rows, slice((t % 3) * 128, (t % 3 + 1) * 128))

    def spectra(i):
        tiles = [s_ref[t, pl.ds(i, lats, stride=BLOCKS), :] for t in range(3)]
        return jnp.concatenate(tiles, axis=1).astype(BF16)

    row = lax.broadcasted_iota(jnp.int32, (256, 256), 0)
    col = lax.broadcasted_iota(jnp.int32, (256, 256), 1)
    same = ((row >= 128) == (col >= 128)) & (row % lev_rows == col % lev_rows)
    ones = jnp.where(same, 1.0, 0.0).astype(BF16)

    zero = jnp.zeros((LATS, 128), F32)
    for k in range(2 * BLOCKS // 2):
        for r in range(USED_ROWS - (k % 2), SLOT_ROWS):
            t_ref[pl.ds(k * LATS * SLOT_ROWS + r, LATS, stride=SLOT_ROWS), :] = zero

    def finish(waves, units):
        tiles = [waves[:, t * 128 : (t + 1) * 128] for t in range(3)]
        lane = lax.broadcasted_iota(jnp.int32, tiles[1].shape, 1)
        zeros = jnp.zeros_like(tiles[1])
        folded = jnp.concatenate(
            [tiles[0] + jnp.where(lane < 64, tiles[1], zeros), tiles[2] + jnp.where(lane < 64, zeros, tiles[1])], axis=1
        )
        high = folded.astype(BF16)
        low = (folded - high.astype(F32)).astype(BF16)
        mean = (dot_nn(high, ones) + dot_nn(low, ones)) * (1.0 / members)
        middle = jnp.where(lane < 64, mean[:, :128], mean[:, 128:])
        anomaly = waves - jnp.concatenate([mean[:, :128], middle, mean[:, 128:]], axis=1)
        for u, (i, j) in enumerate(units):
            for t, (k, r) in enumerate(place(i, j)):
                t_ref[pl.ds(k * LATS * SLOT_ROWS + r, LATS, stride=SLOT_ROWS), :] = anomaly[
                    u * STRIDE : (u + 1) * STRIDE, t * 128 : (t + 1) * 128
                ]

    for p in range(BLOCKS // 2):
        first, second = table(2 * p), table(2 * p + 1)
        mine = spectra(p)
        lower, upper = dot_tn(first, mine), dot_tn(second, mine)
        units = [(p, j) for j in range(p, BLOCKS)]
        if p:
            other = dot_tn(first, spectra(BLOCKS - p))
            lower = jnp.concatenate([other[: STRIDE * p], lower[STRIDE * p :]], axis=0)
            units = [(BLOCKS - p, BLOCKS - p + g) for g in range(p)] + units
        finish(lower, units[:4])
        finish(upper, units[4:])
    p = BLOCKS // 2
    finish(dot_tn(table(2 * p), spectra(p)), [(p, j) for j in range(p, BLOCKS)])
    step = LATS * SLOT_ROWS
    for k in range(LEVS):
        out_ref[k * step : (k + 1) * step, :] = t_ref[k * step : (k + 1) * step, :].astype(BF16)


def legendre_stage(received, table, members, lev_rows, lat_rows):
    rows = LATS * LEVS * SLOT_ROWS
    return pl.pallas_call(
        functools.partial(legendre_kernel, members, lev_rows, lat_rows),
        in_specs=[pl.BlockSpec(memory_space=VMEM)] * 2,
        out_specs=pl.BlockSpec(memory_space=VMEM),
        out_shape=jax.ShapeDtypeStruct((rows, 128), BF16),
        scratch_shapes=[VMEM((rows, 128), F32), VMEM((3, LATS * SPEC_ROWS, 128), F32)],
        compiler_params=pltpu.CompilerParams(vmem_limit_bytes=40 << 20),
        cost_estimate=pl.CostEstimate(flops=2 * 10**9, bytes_accessed=4 * 10**6, transcendentals=0),
        name="legendre",
    )(received, table)


def home(lev):
    p, h = lev // 2, lev % 2
    return p, h


def covariance_kernel(members, lev_rows, y_ref, out_ref):
    levels = LEVS * lev_rows
    count = LATS * SLOT_ROWS
    lev, lat = lax.axis_index("lev"), lax.axis_index("lat")
    p, h = home(lev)
    parts = [y_ref[v * count : (v + 1) * count, :] for v in range(LEVS)]
    lane = lax.broadcasted_iota(jnp.int32, (count, 128), 1)
    for bit in (1, 2, 4):
        shift = bit * lev_rows
        low = (lane // shift) % 2 == 0
        swapped = list(parts)
        for v in range(LEVS):
            if v & bit:
                continue
            a, b = parts[v], parts[v | bit]
            swapped[v] = jnp.where(low, a, pltpu.roll(b, shift, 1))
            swapped[v | bit] = jnp.where(low, pltpu.roll(a, 128 - shift, 1), b)
        parts = swapped
    first_rows = jnp.where(h == 0, 3 * (p + 1), 0)
    slot = lax.broadcasted_iota(jnp.int32, (levels, count), 1) % SLOT_ROWS
    is_first = slot < first_rows
    one = jnp.zeros((levels, levels), F32)
    two = jnp.zeros((levels, levels), F32)
    for part in parts:
        turned = part.astype(F32).T
        zero = jnp.zeros_like(turned)
        one += dot_nn(jnp.where(is_first, turned, zero).astype(BF16), part)
        two += dot_nn(jnp.where(is_first, zero, turned).astype(BF16), part)
    for s, (total, n) in enumerate(((one, lat + STRIDE * p), (two, lat + STRIDE * (BLOCKS - 1 - p)))):
        divisor = ((members - 1) * (2 * n + 2)).astype(F32)
        scaled = (total / jnp.full((levels, levels), divisor, F32)).astype(BF16)
        for v in range(LEVS):
            out_ref[v, s * lev_rows : (s + 1) * lev_rows, :] = scaled[v * lev_rows : (v + 1) * lev_rows]


def covariance_stage(received, members, lev_rows):
    return pl.pallas_call(
        functools.partial(covariance_kernel, members, lev_rows),
        in_specs=[pl.BlockSpec(memory_space=VMEM)],
        out_specs=pl.BlockSpec(memory_space=VMEM),
        out_shape=jax.ShapeDtypeStruct((LEVS, 2 * lev_rows, 128), BF16),
        compiler_params=pltpu.CompilerParams(vmem_limit_bytes=40 << 20),
        cost_estimate=pl.CostEstimate(flops=10**9, bytes_accessed=2 * 10**6, transcendentals=0),
        name="covariance",
    )(received)


def route_kernel(lev_rows, counts_ref, g_ref, out_ref, f_ref):
    lat = lax.axis_index("lat")
    half = BLOCKS // 2
    for j in range(BLOCKS):
        p, s = min(j, BLOCKS - 1 - j), int(j >= half)
        rows = slice(s * lev_rows, (s + 1) * lev_rows)
        f_ref[j] = (g_ref[2 * p, rows, :].astype(F32) + g_ref[2 * p + 1, rows, :].astype(F32)).astype(BF16)

    def step(owner, start):
        j = jnp.maximum(start - lat + (STRIDE - 1), 0) // STRIDE
        out_ref[owner] = f_ref[jnp.minimum(j, BLOCKS - 1)]
        return start + counts_ref[owner]

    lax.fori_loop(0, LATS, step, jnp.int32(0))


def route_stage(parts, owner_counts, lev_rows):
    return pl.pallas_call(
        functools.partial(route_kernel, lev_rows),
        in_specs=[pl.BlockSpec(memory_space=pltpu.SMEM), pl.BlockSpec(memory_space=VMEM)],
        out_specs=pl.BlockSpec(memory_space=VMEM),
        out_shape=jax.ShapeDtypeStruct((LATS, lev_rows, 128), BF16),
        scratch_shapes=[VMEM((BLOCKS, lev_rows, 128), BF16)],
        compiler_params=pltpu.CompilerParams(vmem_limit_bytes=8 << 20),
        name="route",
    )(owner_counts, parts)


def collect_kernel(counts_ref, r_ref, out_ref):
    lat = lax.axis_index("lat")
    start = lax.fori_loop(0, lat, lambda k, s: s + counts_ref[k], jnp.int32(0))
    count = counts_ref[lat]
    for slot in range(out_ref.shape[0]):
        block = r_ref[(start + slot) % STRIDE].astype(F32)
        out_ref[slot] = jnp.where(slot < count, block, jnp.zeros_like(block))


def collect_stage(routed, owner_counts, capacity, lev_rows):
    return pl.pallas_call(
        collect_kernel,
        in_specs=[pl.BlockSpec(memory_space=pltpu.SMEM), pl.BlockSpec(memory_space=VMEM)],
        out_specs=pl.BlockSpec(memory_space=VMEM),
        out_shape=jax.ShapeDtypeStruct((capacity, lev_rows, 128), F32),
        compiler_params=pltpu.CompilerParams(vmem_limit_bytes=8 << 20),
        name="collect",
    )(owner_counts, routed)


def exchange(x, axis):
    return lax.all_to_all(x, axis, split_axis=0, concat_axis=0, tiled=True)


def on_device(fields, legendre, owner_counts):
    members, lev_rows, lat_rows, _ = fields.shape
    modes = legendre.shape[1]
    capacity = 2 * modes // owner_counts.shape[0]
    table = exchange(pack_stage(legendre).reshape(LATS, LEG_ROWS, -1), "lat")
    first = exchange(fourier(fields).reshape(LATS, SPEC_ROWS, -1), "lat")
    second = legendre_stage(first, table, members, lev_rows, lat_rows)
    second = exchange(second.reshape(LATS * LEVS, SLOT_ROWS // 2, 2, 128), ("lev", "lat"))
    third = covariance_stage(second.reshape(-1, 128), members, lev_rows)
    third = exchange(third, "lev")
    fourth = route_stage(third, owner_counts, lev_rows)
    fourth = exchange(fourth, "lat")
    return collect_stage(fourth, owner_counts, capacity, lev_rows)


def solution(mesh):
    return jax.shard_map(
        on_device,
        mesh=mesh,
        in_specs=(P(None, "lev", "lat", None), P("lat", None, None), P()),
        out_specs=P("lat", "lev", None),
        check_vma=False,
    )
```

```python
import functools
import math

import jax
import jax.numpy as jnp
import ml_dtypes
import numpy as np
from jax import lax
from jax.experimental import pallas as pl
from jax.experimental.pallas import tpu as pltpu
from jax.sharding import PartitionSpec as P

F32, BF16 = jnp.float32, jnp.bfloat16
LATS, LEVS = 32, 8
STRIDE = 32
BLOCKS = 8
SPEC_ROWS, LEG_ROWS = 64, 24
ROWS = SPEC_ROWS + LEG_ROWS
SLOT_ROWS, USED_ROWS = 14, 14
CLASSES = ((0, 4, 4), (2, 4, 4), (1, 2, 2))
VMEM = pltpu.VMEM


def fourier_tables(points, modes):
    tables = []
    for first, step, fold in CLASSES:
        j = np.arange(points // fold)
        m = (np.arange(first, LATS, step)[:, None] + STRIDE * np.arange(BLOCKS)[None, :]).reshape(-1)
        angle = (m[:, None] * j[None, :] % points) * (2.0 * math.pi / points)
        table = np.concatenate([np.cos(angle), -np.sin(angle)]) * points**-0.5
        high = table.astype(np.float32).astype(ml_dtypes.bfloat16)
        low = (table - high.astype(np.float64)).astype(np.float32).astype(ml_dtypes.bfloat16)
        tables.append(np.concatenate([high, low]))
    return tables


def dot_nt(a, b):
    return lax.dot_general(a, b, (((1,), (1,)), ((), ())), preferred_element_type=F32)


def dot_tn(a, b):
    return lax.dot_general(a, b, (((0,), (0,)), ((), ())), preferred_element_type=F32)


def dot_nn(a, b):
    return lax.dot_general(a, b, (((1,), (0,)), ((), ())), preferred_element_type=F32)


def fourier_kernel(members, lev_rows, lat_rows, f_hbm, leg_hbm, *refs):
    classes = len(CLASSES)
    tab_hbm, (out_ref, f_ref, leg_ref), refs = refs[:classes], refs[classes : classes + 3], refs[classes + 3 :]
    tab_refs, high_refs, low_refs = refs[:classes], refs[classes : 2 * classes], refs[2 * classes : 3 * classes]
    t_ref, f_sem, sem = refs[3 * classes :]
    unit, pitch = f_hbm.shape[1], f_ref.shape[1]
    pieces = unit // lat_rows
    flat = f_ref.reshape(f_ref.shape[0] * pitch, 128)

    def fetch(b):
        rows = pl.ds(b * lev_rows, lev_rows)
        return pltpu.make_async_copy(f_hbm.at[rows], f_ref.at[rows, pl.ds(0, unit), :], f_sem.at[b])

    leg_copy = pltpu.make_async_copy(leg_hbm, leg_ref, sem.at[classes])
    tab_copies = [pltpu.make_async_copy(tab_hbm[c], tab_refs[c], sem.at[c]) for c in range(classes)]
    for b in range(members):
        fetch(b).start()
    for copy in tab_copies:
        copy.start()
    leg_copy.start()

    def pack(lat):
        table = leg_ref[lat].astype(F32)
        lane = lax.broadcasted_iota(jnp.int32, (STRIDE, 2 * 128), 1)

        def block(i):
            return table[STRIDE * i : STRIDE * (i + 1), :]

        tiles = [block(0)[:, :128], block(0)[:, 128:]]
        for p in range(1, BLOCKS // 2):
            other = pltpu.roll(block(BLOCKS - p), STRIDE * p, 1)
            packed = jnp.where(lane >= STRIDE * p, block(p), other)
            tiles += [packed[:, :128], packed[:, 128:]]
        tiles.append(block(BLOCKS // 2)[:, 128:])
        for t, tile in enumerate(tiles):
            first = (t // 3) * lat_rows
            t_ref[t % 3, pl.ds(first + lat, LATS, stride=LEG_ROWS), :] = tile

    group = lat_rows // 2
    main = 128 // lev_rows
    rest = members - main
    width = group * members * lev_rows

    def split(b, carry):
        fetch(b).wait()
        for lat in range(lat_rows):
            k = lat % group
            inside = jnp.where(b < main, k * 128 + b * lev_rows, group * 128 + (k * rest + b - main) * lev_rows)
            rows = pl.ds(pl.multiple_of(lat // group * width + inside, lev_rows), lev_rows)

            def store(c, piece, u):
                lanes = slice(piece * 128, (piece + 1) * 128)
                high = u.astype(BF16)
                high_refs[c][rows, lanes] = high
                low_refs[c][rows, lanes] = (u - high.astype(F32)).astype(BF16)

            quarter = pieces // 4
            for piece in range(quarter):
                x0, x1, x2, x3 = [
                    flat[pl.ds((b * lev_rows) * pitch + (piece + q * quarter) * lat_rows + lat, lev_rows, stride=pitch), :]
                    for q in range(4)
                ]
                even, odd = x0 + x2, x1 + x3
                store(0, piece, even + odd)
                store(1, piece, even - odd)
                store(2, piece, x0 - x2)
                store(2, piece + quarter, x1 - x3)
        return carry

    lax.fori_loop(0, members, split, 0)
    for copy in tab_copies:
        copy.wait()
    leg_copy.wait()
    waiting = list(range(lat_rows))
    for g in range(2):
        columns = slice(g * width, (g + 1) * width)
        for c, (first, step, fold) in enumerate(CLASSES):
            for k in range(2 if fold == 2 else 1):
                pack(waiting.pop())
            tab, h, l = tab_refs[c][...], high_refs[c][columns], low_refs[c][columns]
            double = tab.shape[0] // 2
            products = dot_nt(tab, h)
            acc = products[:double] + (products[double:] + dot_nt(tab[:double], l))
            count = double // 2
            lane = lax.broadcasted_iota(jnp.int32, (count, 128), 1)
            for k in range(group):
                here = slice(k * 128, (k + 1) * 128)
                tail = slice((group + k // 2) * 128, (group + k // 2 + 1) * 128)
                cos_tail, sin_tail = acc[:count, tail], acc[count:, tail]
                if k % 2 == 0:
                    sin_tail = pltpu.roll(sin_tail, 64, 1)
                else:
                    cos_tail = pltpu.roll(cos_tail, 64, 1)
                middle = jnp.where(lane < 64, cos_tail, sin_tail)
                for t, tile in enumerate((acc[:count, here], middle, acc[count:, here])):
                    tile = tile.astype(BF16)
                    for n in range(count // BLOCKS):
                        start = (first + step * n) * ROWS + (g * group + k) * BLOCKS
                        out_ref[start : start + BLOCKS, t * 128 : (t + 1) * 128] = tile[n * BLOCKS : (n + 1) * BLOCKS]
    for t in range(3):
        for d in range(LATS):
            packed = t_ref[t, d * LEG_ROWS : (d + 1) * LEG_ROWS, :]
            out_ref[d * ROWS + SPEC_ROWS : (d + 1) * ROWS, t * 128 : (t + 1) * 128] = packed.astype(BF16)


def fourier(fields, legendre):
    members, lev_rows, lat_rows, points = fields.shape
    modes = legendre.shape[1]
    columns, pieces = 2 * members * lev_rows, points // 128
    tables = fourier_tables(points, modes)
    splits = [VMEM((lat_rows * members * lev_rows, table.shape[1]), BF16) for table in tables]
    rows = fields.reshape(members, lev_rows, lat_rows, pieces, 128).swapaxes(2, 3).reshape(members * lev_rows, pieces * lat_rows, 128)
    operands = [rows, legendre] + [jnp.asarray(t) for t in tables]
    return pl.pallas_call(
        functools.partial(fourier_kernel, members, lev_rows, lat_rows),
        in_specs=[pl.BlockSpec(memory_space=pltpu.HBM)] * len(operands),
        out_specs=pl.BlockSpec(memory_space=VMEM),
        out_shape=jax.ShapeDtypeStruct((LATS * ROWS, columns), BF16),
        scratch_shapes=[
            VMEM((members * lev_rows, pieces * lat_rows + 8, 128), F32),
            VMEM(legendre.shape, BF16),
            *[VMEM(table.shape, BF16) for table in tables],
            *splits,
            *splits,
            VMEM((3, LATS * LEG_ROWS, 128), F32),
            pltpu.SemaphoreType.DMA((members,)),
            pltpu.SemaphoreType.DMA((len(tables) + 1,)),
        ],
        compiler_params=pltpu.CompilerParams(vmem_limit_bytes=40 << 20),
        cost_estimate=pl.CostEstimate(flops=5 * 10**9, bytes_accessed=10**7, transcendentals=0),
        name="fourier",
    )(*[pltpu.with_memory_space_constraint(x, pltpu.HBM) for x in operands])


def place(i, j):
    p = min(j, BLOCKS - 1 - j)
    base = 3 * i if j < BLOCKS // 2 else 3 * (p + 1) + 3 * i
    return [(2 * p + (base + t) // USED_ROWS, (base + t) % USED_ROWS) for t in range(3)]


def legendre_kernel(members, lev_rows, lat_rows, r_ref, out_ref, t_ref, s_ref):
    columns = r_ref.shape[2]
    lats = LATS * lat_rows
    for t in range(3):
        for s in range(LATS):
            rows = slice(s * SPEC_ROWS, (s + 1) * SPEC_ROWS)
            s_ref[t, rows, :] = r_ref[s, :SPEC_ROWS, t * 128 : (t + 1) * 128].astype(F32)

    def rows_of(first, lanes):
        x = r_ref[:, first : first + lat_rows, lanes].astype(F32)
        return x.reshape(lats, -1).astype(BF16)

    def table(t):
        return rows_of(SPEC_ROWS + (t // 3) * lat_rows, slice((t % 3) * 128, (t % 3 + 1) * 128))

    def spectra(i):
        tiles = [s_ref[t, pl.ds(i, lats, stride=BLOCKS), :] for t in range(3)]
        return jnp.concatenate(tiles, axis=1).astype(BF16)

    row = lax.broadcasted_iota(jnp.int32, (256, 256), 0)
    col = lax.broadcasted_iota(jnp.int32, (256, 256), 1)
    same = ((row >= 128) == (col >= 128)) & (row % lev_rows == col % lev_rows)
    ones = jnp.where(same, 1.0, 0.0).astype(BF16)

    zero = jnp.zeros((LATS, 128), F32)
    for k in range(2 * BLOCKS // 2):
        for r in range(USED_ROWS - (k % 2), SLOT_ROWS):
            t_ref[pl.ds(k * LATS * SLOT_ROWS + r, LATS, stride=SLOT_ROWS), :] = zero

    def finish(waves, units):
        tiles = [waves[:, t * 128 : (t + 1) * 128] for t in range(3)]
        lane = lax.broadcasted_iota(jnp.int32, tiles[1].shape, 1)
        zeros = jnp.zeros_like(tiles[1])
        folded = jnp.concatenate(
            [tiles[0] + jnp.where(lane < 64, tiles[1], zeros), tiles[2] + jnp.where(lane < 64, zeros, tiles[1])], axis=1
        )
        high = folded.astype(BF16)
        low = (folded - high.astype(F32)).astype(BF16)
        mean = (dot_nn(high, ones) + dot_nn(low, ones)) * (1.0 / members)
        middle = jnp.where(lane < 64, mean[:, :128], mean[:, 128:])
        anomaly = waves - jnp.concatenate([mean[:, :128], middle, mean[:, 128:]], axis=1)
        for u, (i, j) in enumerate(units):
            for t, (k, r) in enumerate(place(i, j)):
                t_ref[pl.ds(k * LATS * SLOT_ROWS + r, LATS, stride=SLOT_ROWS), :] = anomaly[
                    u * STRIDE : (u + 1) * STRIDE, t * 128 : (t + 1) * 128
                ]

    for p in range(BLOCKS // 2):
        first, second = table(2 * p), table(2 * p + 1)
        mine = spectra(p)
        lower, upper = dot_tn(first, mine), dot_tn(second, mine)
        units = [(p, j) for j in range(p, BLOCKS)]
        if p:
            other = dot_tn(first, spectra(BLOCKS - p))
            lower = jnp.concatenate([other[: STRIDE * p], lower[STRIDE * p :]], axis=0)
            units = [(BLOCKS - p, BLOCKS - p + g) for g in range(p)] + units
        finish(lower, units[:4])
        finish(upper, units[4:])
    p = BLOCKS // 2
    finish(dot_tn(table(2 * p), spectra(p)), [(p, j) for j in range(p, BLOCKS)])
    step = LATS * SLOT_ROWS
    for k in range(LEVS):
        out_ref[k * step : (k + 1) * step, :] = t_ref[k * step : (k + 1) * step, :].astype(BF16)


def legendre_stage(received, members, lev_rows, lat_rows):
    rows = LATS * LEVS * SLOT_ROWS
    return pl.pallas_call(
        functools.partial(legendre_kernel, members, lev_rows, lat_rows),
        in_specs=[pl.BlockSpec(memory_space=VMEM)],
        out_specs=pl.BlockSpec(memory_space=VMEM),
        out_shape=jax.ShapeDtypeStruct((rows, 128), BF16),
        scratch_shapes=[VMEM((rows, 128), F32), VMEM((3, LATS * SPEC_ROWS, 128), F32)],
        compiler_params=pltpu.CompilerParams(vmem_limit_bytes=40 << 20),
        cost_estimate=pl.CostEstimate(flops=2 * 10**9, bytes_accessed=4 * 10**6, transcendentals=0),
        name="legendre",
    )(received)


def home(lev):
    p, h = lev // 2, lev % 2
    return p, h


def covariance_kernel(members, lev_rows, y_ref, out_ref):
    levels = LEVS * lev_rows
    count = LATS * SLOT_ROWS
    lev, lat = lax.axis_index("lev"), lax.axis_index("lat")
    p, h = home(lev)
    parts = [y_ref[v * count : (v + 1) * count, :] for v in range(LEVS)]
    lane = lax.broadcasted_iota(jnp.int32, (count, 128), 1)
    for bit in (1, 2, 4):
        shift = bit * lev_rows
        low = (lane // shift) % 2 == 0
        swapped = list(parts)
        for v in range(LEVS):
            if v & bit:
                continue
            a, b = parts[v], parts[v | bit]
            swapped[v] = jnp.where(low, a, pltpu.roll(b, shift, 1))
            swapped[v | bit] = jnp.where(low, pltpu.roll(a, 128 - shift, 1), b)
        parts = swapped
    first_rows = jnp.where(h == 0, 3 * (p + 1), 0)
    slot = lax.broadcasted_iota(jnp.int32, (levels, count), 1) % SLOT_ROWS
    is_first = slot < first_rows
    one = jnp.zeros((levels, levels), F32)
    two = jnp.zeros((levels, levels), F32)
    for part in parts:
        turned = part.astype(F32).T
        zero = jnp.zeros_like(turned)
        one += dot_nn(jnp.where(is_first, turned, zero).astype(BF16), part)
        two += dot_nn(jnp.where(is_first, zero, turned).astype(BF16), part)
    for s, (total, n) in enumerate(((one, lat + STRIDE * p), (two, lat + STRIDE * (BLOCKS - 1 - p)))):
        divisor = ((members - 1) * (2 * n + 2)).astype(F32)
        scaled = (total / jnp.full((levels, levels), divisor, F32)).astype(BF16)
        for v in range(LEVS):
            out_ref[v, s * lev_rows : (s + 1) * lev_rows, :] = scaled[v * lev_rows : (v + 1) * lev_rows]


def covariance_stage(received, members, lev_rows):
    return pl.pallas_call(
        functools.partial(covariance_kernel, members, lev_rows),
        in_specs=[pl.BlockSpec(memory_space=VMEM)],
        out_specs=pl.BlockSpec(memory_space=VMEM),
        out_shape=jax.ShapeDtypeStruct((LEVS, 2 * lev_rows, 128), BF16),
        compiler_params=pltpu.CompilerParams(vmem_limit_bytes=40 << 20),
        cost_estimate=pl.CostEstimate(flops=10**9, bytes_accessed=2 * 10**6, transcendentals=0),
        name="covariance",
    )(received)


def route_kernel(lev_rows, counts_ref, g_ref, out_ref, f_ref):
    lat = lax.axis_index("lat")
    half = BLOCKS // 2
    for j in range(BLOCKS):
        p, s = min(j, BLOCKS - 1 - j), int(j >= half)
        rows = slice(s * lev_rows, (s + 1) * lev_rows)
        f_ref[j] = (g_ref[2 * p, rows, :].astype(F32) + g_ref[2 * p + 1, rows, :].astype(F32)).astype(BF16)

    def step(owner, start):
        j = jnp.maximum(start - lat + (STRIDE - 1), 0) // STRIDE
        out_ref[owner] = f_ref[jnp.minimum(j, BLOCKS - 1)]
        return start + counts_ref[owner]

    lax.fori_loop(0, LATS, step, jnp.int32(0))


def route_stage(parts, owner_counts, lev_rows):
    return pl.pallas_call(
        functools.partial(route_kernel, lev_rows),
        in_specs=[pl.BlockSpec(memory_space=pltpu.SMEM), pl.BlockSpec(memory_space=VMEM)],
        out_specs=pl.BlockSpec(memory_space=VMEM),
        out_shape=jax.ShapeDtypeStruct((LATS, lev_rows, 128), BF16),
        scratch_shapes=[VMEM((BLOCKS, lev_rows, 128), BF16)],
        compiler_params=pltpu.CompilerParams(vmem_limit_bytes=8 << 20),
        name="route",
    )(owner_counts, parts)


def collect_kernel(counts_ref, r_ref, out_ref):
    lat = lax.axis_index("lat")
    start = lax.fori_loop(0, lat, lambda k, s: s + counts_ref[k], jnp.int32(0))
    count = counts_ref[lat]
    for slot in range(out_ref.shape[0]):
        block = r_ref[(start + slot) % STRIDE].astype(F32)
        out_ref[slot] = jnp.where(slot < count, block, jnp.zeros_like(block))


def collect_stage(routed, owner_counts, capacity, lev_rows):
    return pl.pallas_call(
        collect_kernel,
        in_specs=[pl.BlockSpec(memory_space=pltpu.SMEM), pl.BlockSpec(memory_space=VMEM)],
        out_specs=pl.BlockSpec(memory_space=VMEM),
        out_shape=jax.ShapeDtypeStruct((capacity, lev_rows, 128), F32),
        compiler_params=pltpu.CompilerParams(vmem_limit_bytes=8 << 20),
        name="collect",
    )(owner_counts, routed)


def exchange(x, axis):
    return lax.all_to_all(x, axis, split_axis=0, concat_axis=0, tiled=True)


def on_device(fields, legendre, owner_counts):
    members, lev_rows, lat_rows, _ = fields.shape
    modes = legendre.shape[1]
    capacity = 2 * modes // owner_counts.shape[0]
    first = fourier(fields, legendre)
    first = exchange(first.reshape(LATS, ROWS, -1), "lat")
    second = legendre_stage(first, members, lev_rows, lat_rows)
    second = exchange(second.reshape(LATS * LEVS, SLOT_ROWS // 2, 2, 128), ("lev", "lat"))
    third = covariance_stage(second.reshape(-1, 128), members, lev_rows)
    third = exchange(third, "lev")
    fourth = route_stage(third, owner_counts, lev_rows)
    fourth = exchange(fourth, "lat")
    return collect_stage(fourth, owner_counts, capacity, lev_rows)


def solution(mesh):
    return jax.shard_map(
        on_device,
        mesh=mesh,
        in_specs=(P(None, "lev", "lat", None), P("lat", None, None), P()),
        out_specs=P("lat", "lev", None),
        check_vma=False,
    )
```

```python
import functools
import math

import jax
import jax.numpy as jnp
import ml_dtypes
import numpy as np
from jax import lax
from jax.experimental import pallas as pl
from jax.experimental.pallas import tpu as pltpu
from jax.sharding import PartitionSpec as P

F32, BF16 = jnp.float32, jnp.bfloat16
LATS, LEVS = 32, 8
STRIDE = 32
BLOCKS = 8
SPEC_ROWS, LEG_ROWS = 64, 24
ROWS = SPEC_ROWS + LEG_ROWS
SLOT_ROWS, USED_ROWS = 14, 14
CLASSES = ((0, 4, 4), (2, 4, 4), (1, 2, 2))
VMEM = pltpu.VMEM


def fourier_tables(points, modes):
    tables = []
    for first, step, fold in CLASSES:
        j = np.arange(points // fold)
        m = (np.arange(first, LATS, step)[:, None] + STRIDE * np.arange(BLOCKS)[None, :]).reshape(-1)
        angle = (m[:, None] * j[None, :] % points) * (2.0 * math.pi / points)
        table = np.concatenate([np.cos(angle), -np.sin(angle)]) * points**-0.5
        high = table.astype(np.float32).astype(ml_dtypes.bfloat16)
        low = (table - high.astype(np.float64)).astype(np.float32).astype(ml_dtypes.bfloat16)
        tables.append(np.concatenate([high, low]))
    return tables


def dot_nt(a, b):
    return lax.dot_general(a, b, (((1,), (1,)), ((), ())), preferred_element_type=F32)


def dot_tn(a, b):
    return lax.dot_general(a, b, (((0,), (0,)), ((), ())), preferred_element_type=F32)


def dot_nn(a, b):
    return lax.dot_general(a, b, (((1,), (0,)), ((), ())), preferred_element_type=F32)


def fourier_kernel(members, lev_rows, lat_rows, f_hbm, leg_hbm, *refs):
    classes = len(CLASSES)
    tab_hbm, (out_ref, f_ref, leg_ref), refs = refs[:classes], refs[classes : classes + 3], refs[classes + 3 :]
    tab_refs, high_refs, low_refs = refs[:classes], refs[classes : 2 * classes], refs[2 * classes : 3 * classes]
    t_ref, f_sem, sem = refs[3 * classes :]
    unit, pitch = f_hbm.shape[1], f_ref.shape[1]
    pieces = unit // lat_rows
    flat = f_ref.reshape(f_ref.shape[0] * pitch, 128)

    def fetch(b):
        rows = pl.ds(b * lev_rows, lev_rows)
        return pltpu.make_async_copy(f_hbm.at[rows], f_ref.at[rows, pl.ds(0, unit), :], f_sem.at[b])

    leg_copy = pltpu.make_async_copy(leg_hbm, leg_ref, sem.at[classes])
    tab_copies = [pltpu.make_async_copy(tab_hbm[c], tab_refs[c], sem.at[c]) for c in range(classes)]
    for b in range(members):
        fetch(b).start()
    for copy in tab_copies:
        copy.start()
    leg_copy.start()

    def pack(lat):
        table = leg_ref[lat].astype(F32)
        lane = lax.broadcasted_iota(jnp.int32, (STRIDE, 2 * 128), 1)

        def block(i):
            return table[STRIDE * i : STRIDE * (i + 1), :]

        tiles = [block(0)[:, :128], block(0)[:, 128:]]
        for p in range(1, BLOCKS // 2):
            other = pltpu.roll(block(BLOCKS - p), STRIDE * p, 1)
            packed = jnp.where(lane >= STRIDE * p, block(p), other)
            tiles += [packed[:, :128], packed[:, 128:]]
        tiles.append(block(BLOCKS // 2)[:, 128:])
        for t, tile in enumerate(tiles):
            first = (t // 3) * lat_rows
            t_ref[t % 3, pl.ds(first + lat, LATS, stride=LEG_ROWS), :] = tile

    group = lat_rows // 2
    main = 128 // lev_rows
    rest = members - main
    width = group * members * lev_rows

    def split(b, carry):
        fetch(b).wait()
        for lat in range(lat_rows):
            k = lat % group
            inside = jnp.where(b < main, k * 128 + b * lev_rows, group * 128 + (k * rest + b - main) * lev_rows)
            rows = pl.ds(pl.multiple_of(lat // group * width + inside, lev_rows), lev_rows)

            def store(c, piece, u):
                lanes = slice(piece * 128, (piece + 1) * 128)
                high = u.astype(BF16)
                high_refs[c][rows, lanes] = high
                low_refs[c][rows, lanes] = (u - high.astype(F32)).astype(BF16)

            quarter = pieces // 4
            for piece in range(quarter):
                x0, x1, x2, x3 = [
                    flat[pl.ds((b * lev_rows) * pitch + (piece + q * quarter) * lat_rows + lat, lev_rows, stride=pitch), :]
                    for q in range(4)
                ]
                even, odd = x0 + x2, x1 + x3
                store(0, piece, even + odd)
                store(1, piece, even - odd)
                store(2, piece, x0 - x2)
                store(2, piece + quarter, x1 - x3)
        return carry

    lax.fori_loop(0, members, split, 0)
    for copy in tab_copies:
        copy.wait()
    leg_copy.wait()
    waiting = list(range(lat_rows))
    for g in range(2):
        columns = slice(g * width, (g + 1) * width)
        for c, (first, step, fold) in enumerate(CLASSES):
            for k in range(2 if fold == 2 else 1):
                pack(waiting.pop())
            tab, h, l = tab_refs[c][...], high_refs[c][columns], low_refs[c][columns]
            double = tab.shape[0] // 2
            products = dot_nt(tab, h)
            acc = products[:double] + (products[double:] + dot_nt(tab[:double], l))
            count = double // 2
            lane = lax.broadcasted_iota(jnp.int32, (count, 128), 1)
            for k in range(group):
                here = slice(k * 128, (k + 1) * 128)
                tail = slice((group + k // 2) * 128, (group + k // 2 + 1) * 128)
                cos_tail, sin_tail = acc[:count, tail], acc[count:, tail]
                if k % 2 == 0:
                    sin_tail = pltpu.roll(sin_tail, 64, 1)
                else:
                    cos_tail = pltpu.roll(cos_tail, 64, 1)
                middle = jnp.where(lane < 64, cos_tail, sin_tail)
                for t, tile in enumerate((acc[:count, here], middle, acc[count:, here])):
                    tile = tile.astype(BF16)
                    for n in range(count // BLOCKS):
                        start = (first + step * n) * ROWS + (g * group + k) * BLOCKS
                        out_ref[start : start + BLOCKS, t * 128 : (t + 1) * 128] = tile[n * BLOCKS : (n + 1) * BLOCKS]
    for t in range(3):
        for d in range(LATS):
            packed = t_ref[t, d * LEG_ROWS : (d + 1) * LEG_ROWS, :]
            out_ref[d * ROWS + SPEC_ROWS : (d + 1) * ROWS, t * 128 : (t + 1) * 128] = packed.astype(BF16)


def fourier(fields, legendre):
    members, lev_rows, lat_rows, points = fields.shape
    modes = legendre.shape[1]
    columns, pieces = 2 * members * lev_rows, points // 128
    tables = fourier_tables(points, modes)
    splits = [VMEM((lat_rows * members * lev_rows, table.shape[1]), BF16) for table in tables]
    rows = fields.reshape(members, lev_rows, lat_rows, pieces, 128).swapaxes(2, 3).reshape(members * lev_rows, pieces * lat_rows, 128)
    operands = [rows, legendre] + [jnp.asarray(t) for t in tables]
    return pl.pallas_call(
        functools.partial(fourier_kernel, members, lev_rows, lat_rows),
        in_specs=[pl.BlockSpec(memory_space=pltpu.HBM)] * len(operands),
        out_specs=pl.BlockSpec(memory_space=VMEM),
        out_shape=jax.ShapeDtypeStruct((LATS * ROWS, columns), BF16),
        scratch_shapes=[
            VMEM((members * lev_rows, pieces * lat_rows + 8, 128), F32),
            VMEM(legendre.shape, BF16),
            *[VMEM(table.shape, BF16) for table in tables],
            *splits,
            *splits,
            VMEM((3, LATS * LEG_ROWS, 128), F32),
            pltpu.SemaphoreType.DMA((members,)),
            pltpu.SemaphoreType.DMA((len(tables) + 1,)),
        ],
        compiler_params=pltpu.CompilerParams(vmem_limit_bytes=40 << 20),
        cost_estimate=pl.CostEstimate(flops=5 * 10**9, bytes_accessed=10**7, transcendentals=0),
        name="fourier",
    )(*[pltpu.with_memory_space_constraint(x, pltpu.HBM) for x in operands])


def place(i, j):
    p = min(j, BLOCKS - 1 - j)
    base = 3 * i if j < BLOCKS // 2 else 3 * (p + 1) + 3 * i
    return [(2 * p + (base + t) // USED_ROWS, (base + t) % USED_ROWS) for t in range(3)]


def legendre_kernel(members, lev_rows, lat_rows, r_ref, out_ref, t_ref, s_ref):
    columns = r_ref.shape[2]
    lats = LATS * lat_rows
    for t in range(3):
        for s in range(LATS):
            rows = slice(s * SPEC_ROWS, (s + 1) * SPEC_ROWS)
            s_ref[t, rows, :] = r_ref[s, :SPEC_ROWS, t * 128 : (t + 1) * 128].astype(F32)

    def rows_of(first, lanes):
        x = r_ref[:, first : first + lat_rows, lanes].astype(F32)
        return x.reshape(lats, -1).astype(BF16)

    def table(t):
        return rows_of(SPEC_ROWS + (t // 3) * lat_rows, slice((t % 3) * 128, (t % 3 + 1) * 128))

    def spectra(i):
        tiles = [s_ref[t, pl.ds(i, lats, stride=BLOCKS), :] for t in range(3)]
        return jnp.concatenate(tiles, axis=1).astype(BF16)

    row = lax.broadcasted_iota(jnp.int32, (256, 256), 0)
    col = lax.broadcasted_iota(jnp.int32, (256, 256), 1)
    same = ((row >= 128) == (col >= 128)) & (row % lev_rows == col % lev_rows)
    ones = jnp.where(same, 1.0, 0.0).astype(BF16)

    zero = jnp.zeros((LATS, 128), F32)
    for k in range(2 * BLOCKS // 2):
        for r in range(USED_ROWS - (k % 2), SLOT_ROWS):
            t_ref[pl.ds(k * LATS * SLOT_ROWS + r, LATS, stride=SLOT_ROWS), :] = zero

    def finish(waves, units):
        tiles = [waves[:, t * 128 : (t + 1) * 128] for t in range(3)]
        lane = lax.broadcasted_iota(jnp.int32, tiles[1].shape, 1)
        zeros = jnp.zeros_like(tiles[1])
        folded = jnp.concatenate(
            [tiles[0] + jnp.where(lane < 64, tiles[1], zeros), tiles[2] + jnp.where(lane < 64, zeros, tiles[1])], axis=1
        )
        high = folded.astype(BF16)
        low = (folded - high.astype(F32)).astype(BF16)
        mean = (dot_nn(high, ones) + dot_nn(low, ones)) * (1.0 / members)
        middle = jnp.where(lane < 64, mean[:, :128], mean[:, 128:])
        anomaly = waves - jnp.concatenate([mean[:, :128], middle, mean[:, 128:]], axis=1)
        for u, (i, j) in enumerate(units):
            for t, (k, r) in enumerate(place(i, j)):
                t_ref[pl.ds(k * LATS * SLOT_ROWS + r, LATS, stride=SLOT_ROWS), :] = anomaly[
                    u * STRIDE : (u + 1) * STRIDE, t * 128 : (t + 1) * 128
                ]

    for p in range(BLOCKS // 2):
        first, second = table(2 * p), table(2 * p + 1)
        mine = spectra(p)
        lower, upper = dot_tn(first, mine), dot_tn(second, mine)
        units = [(p, j) for j in range(p, BLOCKS)]
        if p:
            other = dot_tn(first, spectra(BLOCKS - p))
            lower = jnp.concatenate([other[: STRIDE * p], lower[STRIDE * p :]], axis=0)
            units = [(BLOCKS - p, BLOCKS - p + g) for g in range(p)] + units
        finish(lower, units[:4])
        finish(upper, units[4:])
    p = BLOCKS // 2
    finish(dot_tn(table(2 * p), spectra(p)), [(p, j) for j in range(p, BLOCKS)])
    step = LATS * SLOT_ROWS
    for k in range(LEVS):
        out_ref[k * step : (k + 1) * step, :] = t_ref[k * step : (k + 1) * step, :].astype(BF16)


def legendre_stage(received, members, lev_rows, lat_rows):
    rows = LATS * LEVS * SLOT_ROWS
    return pl.pallas_call(
        functools.partial(legendre_kernel, members, lev_rows, lat_rows),
        in_specs=[pl.BlockSpec(memory_space=VMEM)],
        out_specs=pl.BlockSpec(memory_space=VMEM),
        out_shape=jax.ShapeDtypeStruct((rows, 128), BF16),
        scratch_shapes=[VMEM((rows, 128), F32), VMEM((3, LATS * SPEC_ROWS, 128), F32)],
        compiler_params=pltpu.CompilerParams(vmem_limit_bytes=40 << 20),
        cost_estimate=pl.CostEstimate(flops=2 * 10**9, bytes_accessed=4 * 10**6, transcendentals=0),
        name="legendre",
    )(received)


def home(lev):
    p, h = lev // 2, lev % 2
    return p, h


def covariance_kernel(members, lev_rows, y_ref, out_ref):
    levels = LEVS * lev_rows
    count = LATS * SLOT_ROWS
    lev, lat = lax.axis_index("lev"), lax.axis_index("lat")
    p, h = home(lev)
    turned = [y_ref[v * count : (v + 1) * count, :].T for v in range(LEVS)]
    first_rows = jnp.where(h == 0, 3 * (p + 1), 0)
    slot = lax.broadcasted_iota(jnp.int32, (levels, count), 1) % SLOT_ROWS
    is_first = slot < first_rows
    zero = jnp.zeros((levels, count), BF16)
    one = jnp.zeros((levels, levels), F32)
    two = jnp.zeros((levels, levels), F32)
    for b in range(128 // lev_rows):
        part = jnp.concatenate([t[b * lev_rows : (b + 1) * lev_rows] for t in turned], axis=0)
        one += dot_nt(jnp.where(is_first, part, zero), part)
        two += dot_nt(jnp.where(is_first, zero, part), part)
    for s, (total, n) in enumerate(((one, lat + STRIDE * p), (two, lat + STRIDE * (BLOCKS - 1 - p)))):
        divisor = ((members - 1) * (2 * n + 2)).astype(F32)
        scaled = (total / jnp.full((levels, levels), divisor, F32)).astype(BF16)
        for v in range(LEVS):
            out_ref[v, s * lev_rows : (s + 1) * lev_rows, :] = scaled[v * lev_rows : (v + 1) * lev_rows]


def covariance_stage(received, members, lev_rows):
    return pl.pallas_call(
        functools.partial(covariance_kernel, members, lev_rows),
        in_specs=[pl.BlockSpec(memory_space=VMEM)],
        out_specs=pl.BlockSpec(memory_space=VMEM),
        out_shape=jax.ShapeDtypeStruct((LEVS, 2 * lev_rows, 128), BF16),
        compiler_params=pltpu.CompilerParams(vmem_limit_bytes=40 << 20),
        cost_estimate=pl.CostEstimate(flops=10**9, bytes_accessed=2 * 10**6, transcendentals=0),
        name="covariance",
    )(received)


def route_kernel(lev_rows, counts_ref, g_ref, out_ref, f_ref):
    lat = lax.axis_index("lat")
    half = BLOCKS // 2
    for j in range(BLOCKS):
        p, s = min(j, BLOCKS - 1 - j), int(j >= half)
        rows = slice(s * lev_rows, (s + 1) * lev_rows)
        f_ref[j] = (g_ref[2 * p, rows, :].astype(F32) + g_ref[2 * p + 1, rows, :].astype(F32)).astype(BF16)

    def step(owner, start):
        j = jnp.maximum(start - lat + (STRIDE - 1), 0) // STRIDE
        out_ref[owner] = f_ref[jnp.minimum(j, BLOCKS - 1)]
        return start + counts_ref[owner]

    lax.fori_loop(0, LATS, step, jnp.int32(0))


def route_stage(parts, owner_counts, lev_rows):
    return pl.pallas_call(
        functools.partial(route_kernel, lev_rows),
        in_specs=[pl.BlockSpec(memory_space=pltpu.SMEM), pl.BlockSpec(memory_space=VMEM)],
        out_specs=pl.BlockSpec(memory_space=VMEM),
        out_shape=jax.ShapeDtypeStruct((LATS, lev_rows, 128), BF16),
        scratch_shapes=[VMEM((BLOCKS, lev_rows, 128), BF16)],
        compiler_params=pltpu.CompilerParams(vmem_limit_bytes=8 << 20),
        name="route",
    )(owner_counts, parts)


def collect_kernel(counts_ref, r_ref, out_ref):
    lat = lax.axis_index("lat")
    start = lax.fori_loop(0, lat, lambda k, s: s + counts_ref[k], jnp.int32(0))
    count = counts_ref[lat]
    for slot in range(out_ref.shape[0]):
        block = r_ref[(start + slot) % STRIDE].astype(F32)
        out_ref[slot] = jnp.where(slot < count, block, jnp.zeros_like(block))


def collect_stage(routed, owner_counts, capacity, lev_rows):
    return pl.pallas_call(
        collect_kernel,
        in_specs=[pl.BlockSpec(memory_space=pltpu.SMEM), pl.BlockSpec(memory_space=VMEM)],
        out_specs=pl.BlockSpec(memory_space=VMEM),
        out_shape=jax.ShapeDtypeStruct((capacity, lev_rows, 128), F32),
        compiler_params=pltpu.CompilerParams(vmem_limit_bytes=8 << 20),
        name="collect",
    )(owner_counts, routed)


def exchange(x, axis):
    return lax.all_to_all(x, axis, split_axis=0, concat_axis=0, tiled=True)


def on_device(fields, legendre, owner_counts):
    members, lev_rows, lat_rows, _ = fields.shape
    modes = legendre.shape[1]
    capacity = 2 * modes // owner_counts.shape[0]
    first = fourier(fields, legendre)
    first = exchange(first.reshape(LATS, ROWS, -1), "lat")
    second = legendre_stage(first, members, lev_rows, lat_rows)
    second = exchange(second.reshape(LATS * LEVS, SLOT_ROWS // 2, 2, 128), ("lev", "lat"))
    third = covariance_stage(second.reshape(-1, 128), members, lev_rows)
    third = exchange(third, "lev")
    fourth = route_stage(third, owner_counts, lev_rows)
    fourth = exchange(fourth, "lat")
    return collect_stage(fourth, owner_counts, capacity, lev_rows)


def solution(mesh):
    return jax.shard_map(
        on_device,
        mesh=mesh,
        in_specs=(P(None, "lev", "lat", None), P("lat", None, None), P()),
        out_specs=P("lat", "lev", None),
        check_vma=False,
    )
```

```python
import functools
import math

import jax
import jax.numpy as jnp
import ml_dtypes
import numpy as np
from jax import lax
from jax.experimental import pallas as pl
from jax.experimental.pallas import tpu as pltpu
from jax.sharding import PartitionSpec as P

F32, BF16 = jnp.float32, jnp.bfloat16
LATS, LEVS = 32, 8
CHIPS = LATS // 2
LAT = ("y", "x", "core")
STRIDE = 32
BLOCKS = 8
SPEC_ROWS, LEG_ROWS = 64, 24
ROWS = SPEC_ROWS + LEG_ROWS
SLOT_ROWS, USED_ROWS = 14, 14
CLASSES = ((0, 4, 4), (2, 4, 4), (1, 2, 2))
VMEM = pltpu.VMEM


def fourier_tables(points, modes):
    tables = []
    for first, step, fold in CLASSES:
        j = np.arange(points // fold)
        m = (np.arange(first, LATS, step)[:, None] + STRIDE * np.arange(BLOCKS)[None, :]).reshape(-1)
        angle = (m[:, None] * j[None, :] % points) * (2.0 * math.pi / points)
        table = np.concatenate([np.cos(angle), -np.sin(angle)]) * points**-0.5
        high = table.astype(np.float32).astype(ml_dtypes.bfloat16)
        low = (table - high.astype(np.float64)).astype(np.float32).astype(ml_dtypes.bfloat16)
        tables.append(np.concatenate([high, low]))
    return tables


def dot_nt(a, b):
    return lax.dot_general(a, b, (((1,), (1,)), ((), ())), preferred_element_type=F32)


def dot_tn(a, b):
    return lax.dot_general(a, b, (((0,), (0,)), ((), ())), preferred_element_type=F32)


def dot_nn(a, b):
    return lax.dot_general(a, b, (((1,), (0,)), ((), ())), preferred_element_type=F32)


def fourier_kernel(members, lev_rows, lat_rows, f_hbm, leg_hbm, *refs):
    classes = len(CLASSES)
    tab_hbm, (out_ref, f_ref, leg_ref), refs = refs[:classes], refs[classes : classes + 3], refs[classes + 3 :]
    tab_refs, high_refs, low_refs = refs[:classes], refs[classes : 2 * classes], refs[2 * classes : 3 * classes]
    t_ref, f_sem, sem = refs[3 * classes :]
    unit, pitch = f_hbm.shape[1], f_ref.shape[1]
    pieces = unit // lat_rows
    flat = f_ref.reshape(f_ref.shape[0] * pitch, 128)

    def fetch(b):
        rows = pl.ds(b * lev_rows, lev_rows)
        return pltpu.make_async_copy(f_hbm.at[rows], f_ref.at[rows, pl.ds(0, unit), :], f_sem.at[b])

    leg_copy = pltpu.make_async_copy(leg_hbm, leg_ref, sem.at[classes])
    tab_copies = [pltpu.make_async_copy(tab_hbm[c], tab_refs[c], sem.at[c]) for c in range(classes)]
    for b in range(members):
        fetch(b).start()
    for copy in tab_copies:
        copy.start()
    leg_copy.start()

    def pack(lat):
        table = leg_ref[lat].astype(F32)
        lane = lax.broadcasted_iota(jnp.int32, (STRIDE, 2 * 128), 1)

        def block(i):
            return table[STRIDE * i : STRIDE * (i + 1), :]

        tiles = [block(0)[:, :128], block(0)[:, 128:]]
        for p in range(1, BLOCKS // 2):
            other = pltpu.roll(block(BLOCKS - p), STRIDE * p, 1)
            packed = jnp.where(lane >= STRIDE * p, block(p), other)
            tiles += [packed[:, :128], packed[:, 128:]]
        tiles.append(block(BLOCKS // 2)[:, 128:])
        for t, tile in enumerate(tiles):
            first = (t // 3) * lat_rows
            t_ref[t % 3, pl.ds(first + lat, LATS, stride=LEG_ROWS), :] = tile

    group = lat_rows // 2
    main = 128 // lev_rows
    rest = members - main
    width = group * members * lev_rows

    def split(b, carry):
        fetch(b).wait()
        for lat in range(lat_rows):
            k = lat % group
            inside = jnp.where(b < main, k * 128 + b * lev_rows, group * 128 + (k * rest + b - main) * lev_rows)
            rows = pl.ds(pl.multiple_of(lat // group * width + inside, lev_rows), lev_rows)

            def store(c, piece, u):
                lanes = slice(piece * 128, (piece + 1) * 128)
                high = u.astype(BF16)
                high_refs[c][rows, lanes] = high
                low_refs[c][rows, lanes] = (u - high.astype(F32)).astype(BF16)

            quarter = pieces // 4
            for piece in range(quarter):
                x0, x1, x2, x3 = [
                    flat[pl.ds((b * lev_rows) * pitch + (piece + q * quarter) * lat_rows + lat, lev_rows, stride=pitch), :]
                    for q in range(4)
                ]
                even, odd = x0 + x2, x1 + x3
                store(0, piece, even + odd)
                store(1, piece, even - odd)
                store(2, piece, x0 - x2)
                store(2, piece + quarter, x1 - x3)
        return carry

    lax.fori_loop(0, members, split, 0)
    for copy in tab_copies:
        copy.wait()
    leg_copy.wait()
    waiting = list(range(lat_rows))
    for g in range(2):
        columns = slice(g * width, (g + 1) * width)
        for c, (first, step, fold) in enumerate(CLASSES):
            for k in range(2 if fold == 2 else 1):
                pack(waiting.pop())
            tab, h, l = tab_refs[c][...], high_refs[c][columns], low_refs[c][columns]
            double = tab.shape[0] // 2
            products = dot_nt(tab, h)
            acc = products[:double] + (products[double:] + dot_nt(tab[:double], l))
            count = double // 2
            lane = lax.broadcasted_iota(jnp.int32, (count, 128), 1)
            for k in range(group):
                here = slice(k * 128, (k + 1) * 128)
                tail = slice((group + k // 2) * 128, (group + k // 2 + 1) * 128)
                cos_tail, sin_tail = acc[:count, tail], acc[count:, tail]
                if k % 2 == 0:
                    sin_tail = pltpu.roll(sin_tail, 64, 1)
                else:
                    cos_tail = pltpu.roll(cos_tail, 64, 1)
                middle = jnp.where(lane < 64, cos_tail, sin_tail)
                for t, tile in enumerate((acc[:count, here], middle, acc[count:, here])):
                    tile = tile.astype(BF16)
                    for n in range(count // BLOCKS):
                        start = (first + step * n) * ROWS + (g * group + k) * BLOCKS
                        out_ref[start : start + BLOCKS, t * 128 : (t + 1) * 128] = tile[n * BLOCKS : (n + 1) * BLOCKS]
    for t in range(3):
        for d in range(LATS):
            packed = t_ref[t, d * LEG_ROWS : (d + 1) * LEG_ROWS, :]
            out_ref[d * ROWS + SPEC_ROWS : (d + 1) * ROWS, t * 128 : (t + 1) * 128] = packed.astype(BF16)


def fourier(fields, legendre):
    members, lev_rows, lat_rows, points = fields.shape
    modes = legendre.shape[1]
    columns, pieces = 2 * members * lev_rows, points // 128
    tables = fourier_tables(points, modes)
    splits = [VMEM((lat_rows * members * lev_rows, table.shape[1]), BF16) for table in tables]
    rows = fields.reshape(members, lev_rows, lat_rows, pieces, 128).swapaxes(2, 3).reshape(members * lev_rows, pieces * lat_rows, 128)
    operands = [rows, legendre] + [jnp.asarray(t) for t in tables]
    return pl.pallas_call(
        functools.partial(fourier_kernel, members, lev_rows, lat_rows),
        in_specs=[pl.BlockSpec(memory_space=pltpu.HBM)] * len(operands),
        out_specs=pl.BlockSpec(memory_space=VMEM),
        out_shape=jax.ShapeDtypeStruct((LATS * ROWS, columns), BF16),
        scratch_shapes=[
            VMEM((members * lev_rows, pieces * lat_rows + 8, 128), F32),
            VMEM(legendre.shape, BF16),
            *[VMEM(table.shape, BF16) for table in tables],
            *splits,
            *splits,
            VMEM((3, LATS * LEG_ROWS, 128), F32),
            pltpu.SemaphoreType.DMA((members,)),
            pltpu.SemaphoreType.DMA((len(tables) + 1,)),
        ],
        compiler_params=pltpu.CompilerParams(vmem_limit_bytes=40 << 20),
        cost_estimate=pl.CostEstimate(flops=5 * 10**9, bytes_accessed=10**7, transcendentals=0),
        name="fourier",
    )(*[pltpu.with_memory_space_constraint(x, pltpu.HBM) for x in operands])


def place(i, j):
    p = min(j, BLOCKS - 1 - j)
    base = 3 * i if j < BLOCKS // 2 else 3 * (p + 1) + 3 * i
    return [(2 * p + (base + t) // USED_ROWS, (base + t) % USED_ROWS) for t in range(3)]


def legendre_kernel(members, lev_rows, lat_rows, r_ref, out_ref, t_ref, s_ref):
    columns = r_ref.shape[2]
    lats = LATS * lat_rows
    for t in range(3):
        for s in range(LATS):
            rows = slice(s * SPEC_ROWS, (s + 1) * SPEC_ROWS)
            s_ref[t, rows, :] = r_ref[s, :SPEC_ROWS, t * 128 : (t + 1) * 128].astype(F32)

    def rows_of(first, lanes):
        x = r_ref[:, first : first + lat_rows, lanes].astype(F32)
        return x.reshape(lats, -1).astype(BF16)

    def table(t):
        return rows_of(SPEC_ROWS + (t // 3) * lat_rows, slice((t % 3) * 128, (t % 3 + 1) * 128))

    def spectra(i):
        tiles = [s_ref[t, pl.ds(i, lats, stride=BLOCKS), :] for t in range(3)]
        return jnp.concatenate(tiles, axis=1).astype(BF16)

    row = lax.broadcasted_iota(jnp.int32, (256, 256), 0)
    col = lax.broadcasted_iota(jnp.int32, (256, 256), 1)
    same = ((row >= 128) == (col >= 128)) & (row % lev_rows == col % lev_rows)
    ones = jnp.where(same, 1.0, 0.0).astype(BF16)

    zero = jnp.zeros((LATS, 128), F32)
    for k in range(2 * BLOCKS // 2):
        for r in range(USED_ROWS - (k % 2), SLOT_ROWS):
            t_ref[pl.ds(k * LATS * SLOT_ROWS + r, LATS, stride=SLOT_ROWS), :] = zero

    def finish(waves, units):
        tiles = [waves[:, t * 128 : (t + 1) * 128] for t in range(3)]
        lane = lax.broadcasted_iota(jnp.int32, tiles[1].shape, 1)
        zeros = jnp.zeros_like(tiles[1])
        folded = jnp.concatenate(
            [tiles[0] + jnp.where(lane < 64, tiles[1], zeros), tiles[2] + jnp.where(lane < 64, zeros, tiles[1])], axis=1
        )
        high = folded.astype(BF16)
        low = (folded - high.astype(F32)).astype(BF16)
        mean = (dot_nn(high, ones) + dot_nn(low, ones)) * (1.0 / members)
        middle = jnp.where(lane < 64, mean[:, :128], mean[:, 128:])
        anomaly = waves - jnp.concatenate([mean[:, :128], middle, mean[:, 128:]], axis=1)
        for u, (i, j) in enumerate(units):
            for t, (k, r) in enumerate(place(i, j)):
                t_ref[pl.ds(k * LATS * SLOT_ROWS + r, LATS, stride=SLOT_ROWS), :] = anomaly[
                    u * STRIDE : (u + 1) * STRIDE, t * 128 : (t + 1) * 128
                ]

    for p in range(BLOCKS // 2):
        first, second = table(2 * p), table(2 * p + 1)
        mine = spectra(p)
        lower, upper = dot_tn(first, mine), dot_tn(second, mine)
        units = [(p, j) for j in range(p, BLOCKS)]
        if p:
            other = dot_tn(first, spectra(BLOCKS - p))
            lower = jnp.concatenate([other[: STRIDE * p], lower[STRIDE * p :]], axis=0)
            units = [(BLOCKS - p, BLOCKS - p + g) for g in range(p)] + units
        finish(lower, units[:4])
        finish(upper, units[4:])
    p = BLOCKS // 2
    finish(dot_tn(table(2 * p), spectra(p)), [(p, j) for j in range(p, BLOCKS)])
    step = LATS * SLOT_ROWS
    for k in range(LEVS):
        out_ref[k * step : (k + 1) * step, :] = t_ref[k * step : (k + 1) * step, :].astype(BF16)


def legendre_stage(received, members, lev_rows, lat_rows):
    rows = LATS * LEVS * SLOT_ROWS
    return pl.pallas_call(
        functools.partial(legendre_kernel, members, lev_rows, lat_rows),
        in_specs=[pl.BlockSpec(memory_space=VMEM)],
        out_specs=pl.BlockSpec(memory_space=VMEM),
        out_shape=jax.ShapeDtypeStruct((rows, 128), BF16),
        scratch_shapes=[VMEM((rows, 128), F32), VMEM((3, LATS * SPEC_ROWS, 128), F32)],
        compiler_params=pltpu.CompilerParams(vmem_limit_bytes=40 << 20),
        cost_estimate=pl.CostEstimate(flops=2 * 10**9, bytes_accessed=4 * 10**6, transcendentals=0),
        name="legendre",
    )(received)


def chip_index():
    return lax.axis_index("y") * (CHIPS // 4) + lax.axis_index("x")


def residue():
    return lax.axis_index("core") * CHIPS + chip_index()


def home(lev):
    p, h = lev // 2, lev % 2
    return p, h


def covariance_kernel(members, lev_rows, y_ref, out_ref):
    levels = LEVS * lev_rows
    count = LATS * SLOT_ROWS
    lev, lat = lax.axis_index("lev"), residue()
    p, h = home(lev)
    turned = [y_ref[v * count : (v + 1) * count, :].T for v in range(LEVS)]
    first_rows = jnp.where(h == 0, 3 * (p + 1), 0)
    slot = lax.broadcasted_iota(jnp.int32, (levels, count), 1) % SLOT_ROWS
    is_first = slot < first_rows
    zero = jnp.zeros((levels, count), BF16)
    one = jnp.zeros((levels, levels), F32)
    two = jnp.zeros((levels, levels), F32)
    for b in range(128 // lev_rows):
        part = jnp.concatenate([t[b * lev_rows : (b + 1) * lev_rows] for t in turned], axis=0)
        one += dot_nt(jnp.where(is_first, part, zero), part)
        two += dot_nt(jnp.where(is_first, zero, part), part)
    for s, (total, n) in enumerate(((one, lat + STRIDE * p), (two, lat + STRIDE * (BLOCKS - 1 - p)))):
        divisor = ((members - 1) * (2 * n + 2)).astype(F32)
        scaled = (total / jnp.full((levels, levels), divisor, F32)).astype(BF16)
        for v in range(LEVS):
            out_ref[v, s * lev_rows : (s + 1) * lev_rows, :] = scaled[v * lev_rows : (v + 1) * lev_rows]


def covariance_stage(received, members, lev_rows):
    return pl.pallas_call(
        functools.partial(covariance_kernel, members, lev_rows),
        in_specs=[pl.BlockSpec(memory_space=VMEM)],
        out_specs=pl.BlockSpec(memory_space=VMEM),
        out_shape=jax.ShapeDtypeStruct((LEVS, 2 * lev_rows, 128), BF16),
        compiler_params=pltpu.CompilerParams(vmem_limit_bytes=40 << 20),
        cost_estimate=pl.CostEstimate(flops=10**9, bytes_accessed=2 * 10**6, transcendentals=0),
        name="covariance",
    )(received)


def route_kernel(lev_rows, counts_ref, g_ref, out_ref, f_ref):
    lat = residue()
    half = BLOCKS // 2
    for j in range(BLOCKS):
        p, s = min(j, BLOCKS - 1 - j), int(j >= half)
        rows = slice(s * lev_rows, (s + 1) * lev_rows)
        f_ref[j] = (g_ref[2 * p, rows, :].astype(F32) + g_ref[2 * p + 1, rows, :].astype(F32)).astype(BF16)

    def step(owner, start):
        j = jnp.maximum(start - lat + (STRIDE - 1), 0) // STRIDE
        out_ref[owner] = f_ref[jnp.minimum(j, BLOCKS - 1)]
        return start + counts_ref[owner]

    lax.fori_loop(0, LATS, step, jnp.int32(0))


def route_stage(parts, owner_counts, lev_rows):
    return pl.pallas_call(
        functools.partial(route_kernel, lev_rows),
        in_specs=[pl.BlockSpec(memory_space=pltpu.SMEM), pl.BlockSpec(memory_space=VMEM)],
        out_specs=pl.BlockSpec(memory_space=VMEM),
        out_shape=jax.ShapeDtypeStruct((LATS, lev_rows, 128), BF16),
        scratch_shapes=[VMEM((BLOCKS, lev_rows, 128), BF16)],
        compiler_params=pltpu.CompilerParams(vmem_limit_bytes=8 << 20),
        name="route",
    )(owner_counts, parts)


def collect_kernel(counts_ref, r_ref, out_ref):
    chip, core = chip_index(), lax.axis_index("core")
    lat = 2 * chip + core
    start = lax.fori_loop(0, lat, lambda k, s: s + counts_ref[k], jnp.int32(0))
    count = counts_ref[lat]
    for slot in range(out_ref.shape[0]):
        c = (start + slot) % STRIDE
        block = r_ref[(c % CHIPS) * 2 + c // CHIPS].astype(F32)
        out_ref[slot] = jnp.where(slot < count, block, jnp.zeros_like(block))


def collect_stage(routed, owner_counts, capacity, lev_rows):
    return pl.pallas_call(
        collect_kernel,
        in_specs=[pl.BlockSpec(memory_space=pltpu.SMEM), pl.BlockSpec(memory_space=VMEM)],
        out_specs=pl.BlockSpec(memory_space=VMEM),
        out_shape=jax.ShapeDtypeStruct((capacity, lev_rows, 128), F32),
        compiler_params=pltpu.CompilerParams(vmem_limit_bytes=8 << 20),
        name="collect",
    )(owner_counts, routed)


def exchange(x, axis):
    return lax.all_to_all(x, axis, split_axis=0, concat_axis=0, tiled=True)


def on_device(fields, legendre, owner_counts):
    members, lev_rows, lat_rows, _ = fields.shape
    modes = legendre.shape[1]
    capacity = 2 * modes // owner_counts.shape[0]
    first = fourier(fields, legendre)
    first = exchange(first.reshape(LATS, ROWS, -1), LAT)
    second = legendre_stage(first, members, lev_rows, lat_rows)
    second = exchange(second.reshape(LATS * LEVS, SLOT_ROWS // 2, 2, 128), ("lev", "core", "y", "x"))
    third = covariance_stage(second.reshape(-1, 128), members, lev_rows)
    third = exchange(third, "lev")
    fourth = route_stage(third, owner_counts, lev_rows)
    fourth = exchange(fourth, LAT)
    return collect_stage(fourth, owner_counts, capacity, lev_rows)


def solution(mesh):
    parts = jax.sharding.Mesh(mesh.devices.reshape(4, CHIPS // 4, 2, LEVS), (*LAT, "lev"))
    return jax.shard_map(
        on_device,
        mesh=parts,
        in_specs=(P(None, "lev", LAT, None), P(LAT, None, None), P()),
        out_specs=P(LAT, "lev", None),
        check_vma=False,
    )
```

```python
import functools
import math

import jax
import jax.numpy as jnp
import ml_dtypes
import numpy as np
from jax import lax
from jax.experimental import pallas as pl
from jax.experimental.pallas import tpu as pltpu
from jax.sharding import PartitionSpec as P

F32, BF16 = jnp.float32, jnp.bfloat16
LATS, LEVS = 32, 8
STRIDE = 32
BLOCKS = 8
SPEC_ROWS, LEG_ROWS = 64, 24
ROWS = SPEC_ROWS + LEG_ROWS
SLOT_ROWS, USED_ROWS = 14, 14
CLASSES = ((0, 4, 4), (2, 4, 4), (1, 2, 2))
VMEM = pltpu.VMEM


def fourier_tables(points, modes):
    tables = []
    for first, step, fold in CLASSES:
        j = np.arange(points // fold)
        m = (np.arange(first, LATS, step)[:, None] + STRIDE * np.arange(BLOCKS)[None, :]).reshape(-1)
        angle = (m[:, None] * j[None, :] % points) * (2.0 * math.pi / points)
        table = np.concatenate([np.cos(angle), -np.sin(angle)]) * points**-0.5
        high = table.astype(np.float32).astype(ml_dtypes.bfloat16)
        low = (table - high.astype(np.float64)).astype(np.float32).astype(ml_dtypes.bfloat16)
        tables.append(np.concatenate([high, low]))
    return tables


def dot_nt(a, b):
    return lax.dot_general(a, b, (((1,), (1,)), ((), ())), preferred_element_type=F32)


def dot_tn(a, b):
    return lax.dot_general(a, b, (((0,), (0,)), ((), ())), preferred_element_type=F32)


def dot_nn(a, b):
    return lax.dot_general(a, b, (((1,), (0,)), ((), ())), preferred_element_type=F32)


def fourier_kernel(members, lev_rows, lat_rows, f_hbm, leg_hbm, *refs):
    classes = len(CLASSES)
    tab_hbm, (out_ref, f_ref, leg_ref), refs = refs[:classes], refs[classes : classes + 3], refs[classes + 3 :]
    tab_refs, high_refs, low_refs = refs[:classes], refs[classes : 2 * classes], refs[2 * classes : 3 * classes]
    t_ref, f_sem, sem = refs[3 * classes :]
    unit, pitch = f_hbm.shape[1], f_ref.shape[1]
    pieces = unit // lat_rows
    flat = f_ref.reshape(f_ref.shape[0] * pitch, 128)

    def fetch(b):
        rows = pl.ds(b * lev_rows, lev_rows)
        return pltpu.make_async_copy(f_hbm.at[rows], f_ref.at[rows, pl.ds(0, unit), :], f_sem.at[b])

    leg_copy = pltpu.make_async_copy(leg_hbm, leg_ref, sem.at[classes])
    tab_copies = [pltpu.make_async_copy(tab_hbm[c], tab_refs[c], sem.at[c]) for c in range(classes)]
    for b in range(members):
        fetch(b).start()
    for copy in tab_copies:
        copy.start()
    leg_copy.start()

    def pack(lat):
        table = leg_ref[lat].astype(F32)
        lane = lax.broadcasted_iota(jnp.int32, (STRIDE, 2 * 128), 1)

        def block(i):
            return table[STRIDE * i : STRIDE * (i + 1), :]

        tiles = [block(0)[:, :128], block(0)[:, 128:]]
        for p in range(1, BLOCKS // 2):
            other = pltpu.roll(block(BLOCKS - p), STRIDE * p, 1)
            packed = jnp.where(lane >= STRIDE * p, block(p), other)
            tiles += [packed[:, :128], packed[:, 128:]]
        tiles.append(block(BLOCKS // 2)[:, 128:])
        for t, tile in enumerate(tiles):
            first = (t // 3) * lat_rows
            t_ref[t % 3, pl.ds(first + lat, LATS, stride=LEG_ROWS), :] = tile

    group = lat_rows // 2
    main = 128 // lev_rows
    rest = members - main
    width = group * members * lev_rows

    def split(b, carry):
        fetch(b).wait()
        for lat in range(lat_rows):
            k = lat % group
            inside = jnp.where(b < main, k * 128 + b * lev_rows, group * 128 + (k * rest + b - main) * lev_rows)
            rows = pl.ds(pl.multiple_of(lat // group * width + inside, lev_rows), lev_rows)

            def store(c, piece, u):
                lanes = slice(piece * 128, (piece + 1) * 128)
                high = u.astype(BF16)
                high_refs[c][rows, lanes] = high
                low_refs[c][rows, lanes] = (u - high.astype(F32)).astype(BF16)

            quarter = pieces // 4
            for piece in range(quarter):
                x0, x1, x2, x3 = [
                    flat[pl.ds((b * lev_rows) * pitch + (piece + q * quarter) * lat_rows + lat, lev_rows, stride=pitch), :]
                    for q in range(4)
                ]
                even, odd = x0 + x2, x1 + x3
                store(0, piece, even + odd)
                store(1, piece, even - odd)
                store(2, piece, x0 - x2)
                store(2, piece + quarter, x1 - x3)
        return carry

    lax.fori_loop(0, members, split, 0)
    for copy in tab_copies:
        copy.wait()
    leg_copy.wait()
    waiting = list(range(lat_rows))
    for g in range(2):
        columns = slice(g * width, (g + 1) * width)
        for c, (first, step, fold) in enumerate(CLASSES):
            for k in range(2 if fold == 2 else 1):
                pack(waiting.pop())
            tab, h, l = tab_refs[c][...], high_refs[c][columns], low_refs[c][columns]
            double = tab.shape[0] // 2
            products = dot_nt(tab, h)
            acc = products[:double] + (products[double:] + dot_nt(tab[:double], l))
            count = double // 2
            lane = lax.broadcasted_iota(jnp.int32, (count, 128), 1)
            for k in range(group):
                here = slice(k * 128, (k + 1) * 128)
                tail = slice((group + k // 2) * 128, (group + k // 2 + 1) * 128)
                cos_tail, sin_tail = acc[:count, tail], acc[count:, tail]
                if k % 2 == 0:
                    sin_tail = pltpu.roll(sin_tail, 64, 1)
                else:
                    cos_tail = pltpu.roll(cos_tail, 64, 1)
                middle = jnp.where(lane < 64, cos_tail, sin_tail)
                for t, tile in enumerate((acc[:count, here], middle, acc[count:, here])):
                    tile = tile.astype(BF16)
                    for n in range(count // BLOCKS):
                        start = (first + step * n) * ROWS + (g * group + k) * BLOCKS
                        out_ref[start : start + BLOCKS, t * 128 : (t + 1) * 128] = tile[n * BLOCKS : (n + 1) * BLOCKS]
    for t in range(3):
        for d in range(LATS):
            packed = t_ref[t, d * LEG_ROWS : (d + 1) * LEG_ROWS, :]
            out_ref[d * ROWS + SPEC_ROWS : (d + 1) * ROWS, t * 128 : (t + 1) * 128] = packed.astype(BF16)


def fourier(fields, legendre):
    members, lev_rows, lat_rows, points = fields.shape
    modes = legendre.shape[1]
    columns, pieces = 2 * members * lev_rows, points // 128
    tables = fourier_tables(points, modes)
    splits = [VMEM((lat_rows * members * lev_rows, table.shape[1]), BF16) for table in tables]
    rows = fields.reshape(members, lev_rows, lat_rows, pieces, 128).swapaxes(2, 3).reshape(members * lev_rows, pieces * lat_rows, 128)
    operands = [rows, legendre] + [jnp.asarray(t) for t in tables]
    return pl.pallas_call(
        functools.partial(fourier_kernel, members, lev_rows, lat_rows),
        in_specs=[pl.BlockSpec(memory_space=pltpu.HBM)] * len(operands),
        out_specs=pl.BlockSpec(memory_space=VMEM),
        out_shape=jax.ShapeDtypeStruct((LATS * ROWS, columns), BF16),
        scratch_shapes=[
            VMEM((members * lev_rows, pieces * lat_rows + 8, 128), F32),
            VMEM(legendre.shape, BF16),
            *[VMEM(table.shape, BF16) for table in tables],
            *splits,
            *splits,
            VMEM((3, LATS * LEG_ROWS, 128), F32),
            pltpu.SemaphoreType.DMA((members,)),
            pltpu.SemaphoreType.DMA((len(tables) + 1,)),
        ],
        compiler_params=pltpu.CompilerParams(vmem_limit_bytes=40 << 20),
        cost_estimate=pl.CostEstimate(flops=5 * 10**9, bytes_accessed=10**7, transcendentals=0),
        name="fourier",
    )(*[pltpu.with_memory_space_constraint(x, pltpu.HBM) for x in operands])


def place(i, j):
    p = min(j, BLOCKS - 1 - j)
    base = 3 * i if j < BLOCKS // 2 else 3 * (p + 1) + 3 * i
    return [(2 * p + (base + t) // USED_ROWS, (base + t) % USED_ROWS) for t in range(3)]


def legendre_kernel(members, lev_rows, lat_rows, r_ref, out_ref, t_ref, s_ref):
    columns = r_ref.shape[2]
    lats = LATS * lat_rows
    for t in range(3):
        for s in range(LATS):
            rows = slice(s * SPEC_ROWS, (s + 1) * SPEC_ROWS)
            s_ref[t, rows, :] = r_ref[s, :SPEC_ROWS, t * 128 : (t + 1) * 128].astype(F32)

    def rows_of(first, lanes):
        x = r_ref[:, first : first + lat_rows, lanes].astype(F32)
        return x.reshape(lats, -1).astype(BF16)

    def table(t):
        return rows_of(SPEC_ROWS + (t // 3) * lat_rows, slice((t % 3) * 128, (t % 3 + 1) * 128))

    def spectra(i):
        tiles = [s_ref[t, pl.ds(i, lats, stride=BLOCKS), :] for t in range(3)]
        return jnp.concatenate(tiles, axis=1).astype(BF16)

    row = lax.broadcasted_iota(jnp.int32, (256, 256), 0)
    col = lax.broadcasted_iota(jnp.int32, (256, 256), 1)
    same = ((row >= 128) == (col >= 128)) & (row % lev_rows == col % lev_rows)
    ones = jnp.where(same, 1.0, 0.0).astype(BF16)

    zero = jnp.zeros((LATS, 128), F32)
    for k in range(2 * BLOCKS // 2):
        for r in range(USED_ROWS - (k % 2), SLOT_ROWS):
            t_ref[pl.ds(k * LATS * SLOT_ROWS + r, LATS, stride=SLOT_ROWS), :] = zero

    def finish(waves, units):
        tiles = [waves[:, t * 128 : (t + 1) * 128] for t in range(3)]
        lane = lax.broadcasted_iota(jnp.int32, tiles[1].shape, 1)
        zeros = jnp.zeros_like(tiles[1])
        folded = jnp.concatenate(
            [tiles[0] + jnp.where(lane < 64, tiles[1], zeros), tiles[2] + jnp.where(lane < 64, zeros, tiles[1])], axis=1
        )
        high = folded.astype(BF16)
        low = (folded - high.astype(F32)).astype(BF16)
        mean = (dot_nn(high, ones) + dot_nn(low, ones)) * (1.0 / members)
        middle = jnp.where(lane < 64, mean[:, :128], mean[:, 128:])
        anomaly = waves - jnp.concatenate([mean[:, :128], middle, mean[:, 128:]], axis=1)
        for u, (i, j) in enumerate(units):
            for t, (k, r) in enumerate(place(i, j)):
                t_ref[pl.ds(k * LATS * SLOT_ROWS + r, LATS, stride=SLOT_ROWS), :] = anomaly[
                    u * STRIDE : (u + 1) * STRIDE, t * 128 : (t + 1) * 128
                ]

    for p in range(BLOCKS // 2):
        first, second = table(2 * p), table(2 * p + 1)
        mine = spectra(p)
        lower, upper = dot_tn(first, mine), dot_tn(second, mine)
        units = [(p, j) for j in range(p, BLOCKS)]
        if p:
            other = dot_tn(first, spectra(BLOCKS - p))
            lower = jnp.concatenate([other[: STRIDE * p], lower[STRIDE * p :]], axis=0)
            units = [(BLOCKS - p, BLOCKS - p + g) for g in range(p)] + units
        finish(lower, units[:4])
        finish(upper, units[4:])
    p = BLOCKS // 2
    finish(dot_tn(table(2 * p), spectra(p)), [(p, j) for j in range(p, BLOCKS)])
    step = LATS * SLOT_ROWS
    for k in range(LEVS):
        out_ref[k * step : (k + 1) * step, :] = t_ref[k * step : (k + 1) * step, :].astype(BF16)


def legendre_stage(received, members, lev_rows, lat_rows):
    rows = LATS * LEVS * SLOT_ROWS
    return pl.pallas_call(
        functools.partial(legendre_kernel, members, lev_rows, lat_rows),
        in_specs=[pl.BlockSpec(memory_space=VMEM)],
        out_specs=pl.BlockSpec(memory_space=VMEM),
        out_shape=jax.ShapeDtypeStruct((rows, 128), BF16),
        scratch_shapes=[VMEM((rows, 128), F32), VMEM((3, LATS * SPEC_ROWS, 128), F32)],
        compiler_params=pltpu.CompilerParams(vmem_limit_bytes=40 << 20),
        cost_estimate=pl.CostEstimate(flops=2 * 10**9, bytes_accessed=4 * 10**6, transcendentals=0),
        name="legendre",
    )(received)


def home(lev):
    p, h = lev // 2, lev % 2
    return p, h


def covariance_kernel(members, lev_rows, y_ref, out_ref):
    levels = LEVS * lev_rows
    count = LATS * SLOT_ROWS
    lev, lat = lax.axis_index("lev"), lax.axis_index("lat")
    p, h = home(lev)
    turned = [y_ref[v * count : (v + 1) * count, :].T for v in range(LEVS)]
    first_rows = jnp.where(h == 0, 3 * (p + 1), 0)
    slot = lax.broadcasted_iota(jnp.int32, (levels, count), 1) % SLOT_ROWS
    is_first = slot < first_rows
    zero = jnp.zeros((levels, count), BF16)
    one = jnp.zeros((levels, levels), F32)
    two = jnp.zeros((levels, levels), F32)
    for b in range(128 // lev_rows):
        part = jnp.concatenate([t[b * lev_rows : (b + 1) * lev_rows] for t in turned], axis=0)
        one += dot_nt(jnp.where(is_first, part, zero), part)
        two += dot_nt(jnp.where(is_first, zero, part), part)
    for s, (total, n) in enumerate(((one, lat + STRIDE * p), (two, lat + STRIDE * (BLOCKS - 1 - p)))):
        divisor = ((members - 1) * (2 * n + 2)).astype(F32)
        scaled = (total / jnp.full((levels, levels), divisor, F32)).astype(BF16)
        for v in range(LEVS):
            out_ref[v, s * lev_rows : (s + 1) * lev_rows, :] = scaled[v * lev_rows : (v + 1) * lev_rows]


def covariance_stage(received, members, lev_rows):
    return pl.pallas_call(
        functools.partial(covariance_kernel, members, lev_rows),
        in_specs=[pl.BlockSpec(memory_space=VMEM)],
        out_specs=pl.BlockSpec(memory_space=VMEM),
        out_shape=jax.ShapeDtypeStruct((LEVS, 2 * lev_rows, 128), BF16),
        compiler_params=pltpu.CompilerParams(vmem_limit_bytes=40 << 20),
        cost_estimate=pl.CostEstimate(flops=10**9, bytes_accessed=2 * 10**6, transcendentals=0),
        name="covariance",
    )(received)


def route_kernel(lev_rows, counts_ref, g_ref, out_ref, f_ref):
    lat = lax.axis_index("lat")
    half = BLOCKS // 2
    for j in range(BLOCKS):
        p, s = min(j, BLOCKS - 1 - j), int(j >= half)
        rows = slice(s * lev_rows, (s + 1) * lev_rows)
        f_ref[j] = (g_ref[2 * p, rows, :].astype(F32) + g_ref[2 * p + 1, rows, :].astype(F32)).astype(BF16)

    start = jnp.int32(0)
    for owner in range(LATS):
        j = lax.shift_right_logical(start - lat + (STRIDE - 1), 5)
        out_ref[owner] = f_ref[jnp.minimum(j, BLOCKS - 1)]
        start += counts_ref[owner]


def route_stage(parts, owner_counts, lev_rows):
    return pl.pallas_call(
        functools.partial(route_kernel, lev_rows),
        in_specs=[pl.BlockSpec(memory_space=pltpu.SMEM), pl.BlockSpec(memory_space=VMEM)],
        out_specs=pl.BlockSpec(memory_space=VMEM),
        out_shape=jax.ShapeDtypeStruct((LATS, lev_rows, 128), BF16),
        scratch_shapes=[VMEM((BLOCKS, lev_rows, 128), BF16)],
        compiler_params=pltpu.CompilerParams(vmem_limit_bytes=8 << 20),
        name="route",
    )(owner_counts, parts)


def collect_kernel(counts_ref, r_ref, out_ref):
    lat = lax.axis_index("lat")
    start = jnp.int32(0)
    for k in range(LATS - 1):
        start += jnp.where(k < lat, counts_ref[k], 0)
    count = counts_ref[lat]
    for slot in range(out_ref.shape[0]):
        block = r_ref[jnp.bitwise_and(start + slot, STRIDE - 1)].astype(F32)
        out_ref[slot] = jnp.where(slot < count, block, jnp.zeros_like(block))


def collect_stage(routed, owner_counts, capacity, lev_rows):
    return pl.pallas_call(
        collect_kernel,
        in_specs=[pl.BlockSpec(memory_space=pltpu.SMEM), pl.BlockSpec(memory_space=VMEM)],
        out_specs=pl.BlockSpec(memory_space=VMEM),
        out_shape=jax.ShapeDtypeStruct((capacity, lev_rows, 128), F32),
        compiler_params=pltpu.CompilerParams(vmem_limit_bytes=8 << 20),
        name="collect",
    )(owner_counts, routed)


def exchange(x, axis):
    return lax.all_to_all(x, axis, split_axis=0, concat_axis=0, tiled=True)


def on_device(fields, legendre, owner_counts):
    members, lev_rows, lat_rows, _ = fields.shape
    modes = legendre.shape[1]
    capacity = 2 * modes // owner_counts.shape[0]
    first = fourier(fields, legendre)
    first = exchange(first.reshape(LATS, ROWS, -1), "lat")
    second = legendre_stage(first, members, lev_rows, lat_rows)
    second = exchange(second.reshape(LATS * LEVS, SLOT_ROWS // 2, 2, 128), ("lev", "lat"))
    third = covariance_stage(second.reshape(-1, 128), members, lev_rows)
    third = exchange(third, "lev")
    fourth = route_stage(third, owner_counts, lev_rows)
    fourth = exchange(fourth, "lat")
    return collect_stage(fourth, owner_counts, capacity, lev_rows)


def solution(mesh):
    return jax.shard_map(
        on_device,
        mesh=mesh,
        in_specs=(P(None, "lev", "lat", None), P("lat", None, None), P()),
        out_specs=P("lat", "lev", None),
        check_vma=False,
    )
```
